128 devices in a mesh: ang: 8 (over z_lo, x), rad: 16 (over y, z_hi, core).
Axes of the slice: x: 4, y: 4, z: 4 (z_hi: 2, z_lo: 2; z = z_hi * 2 + z_lo), core: 2. Of those that a mesh axis runs over, the one named last changes fastest.
Arguments:
- right_side: float32 [2048, 8192], P('rad', 'ang'), may hold values from -6 to 7
- guess: float32 [2048, 8192], P('rad', 'ang'), may hold values from -6 to 6
Outputs:
- solution: float32 [2048, 8192], P('rad', 'ang')
- residual: float32 [2048, 8192], P('rad', 'ang')
The draws below stay inside these ranges and needn't reach their ends.
All inputs are finite; a program needn't handle non-finite values.
Results may differ from the reference program's by a relative error of at most 0.007.
Values sent between devices are 32-bit elements; how exact they have to be, the bound alone decides.
A program may use at most 128 MiB of HBM per device.

```python
import math
import jax
import jax.numpy as jnp

LEVELS = 8
PRE = 2
POST = 2
COARSE_SWEEPS = 8
NR = 2048
NT = 8192


def draw_right_side(key, part):
    rough_part = jnp.clip(jax.random.normal(key, (NR, NT), jnp.float32), -6.0, 6.0)
    return rough_part


def levels(key, dims, cuts, low, top_value):
    gain, own = 1.0, jax.random.fold_in(key, 6)
    for position, blocks in cuts:
        steps = jnp.exp(jax.random.uniform(jax.random.fold_in(own, position), (blocks,), jnp.float32, low / len(cuts), top_value / len(cuts)))
        gain = gain * jnp.repeat(steps, dims[position] // blocks).reshape([-1 if axis == position else 1 for axis in range(len(dims))])
    return gain


def normal_values(rng, extent, width, most, pieces=(), kind=jnp.bfloat16):
    gain = levels(rng, extent, pieces, -0.22, 0.18) if pieces else 1.0
    array = jax.random.normal(rng, extent, jnp.float32) * width * gain
    return jnp.minimum(jnp.maximum(array, -most), most).astype(kind)


def setup_inputs(seed: int = 0) -> dict:
    seeds = jax.random.split(jax.random.key(seed), 3)
    return {
        "right_side": draw_right_side(jax.random.fold_in(seeds[2], 71), 0),
        "guess": normal_values(seeds[1], (NR, NT), 1.0, 6.0, ((0, 16), (1, 8)), jnp.float32),
    }


def coefficients(row_float, spacing):
    radius = 1.0 + (row_float + 0.5) * spacing
    offset_ratio = 0.5 * spacing / radius
    outward = 1.0 + offset_ratio
    inward = 1.0 - offset_ratio
    angular = 1.0 / (radius * radius)
    centre = 2.0 + 2.0 * angular
    return outward, inward, angular, centre


def relax_cells(padded, source, stencil, chosen):
    outward, inward, angular, centre = stencil
    middle = padded[1:-1, 1:-1]
    updated = (source + outward * padded[2:, 1:-1] + inward * padded[:-2, 1:-1]
               + angular * (padded[1:-1, 2:] + padded[1:-1, :-2])) / centre
    return jnp.where(chosen, updated, middle)


def apply_operator(padded, stencil):
    outward, inward, angular, centre = stencil
    middle = padded[1:-1, 1:-1]
    return (centre * middle - outward * padded[2:, 1:-1] - inward * padded[:-2, 1:-1]
            - angular * (padded[1:-1, 2:] + padded[1:-1, :-2]))


def restrict_grid(padded):
    height = padded.shape[0] - 2
    breadth = padded.shape[1] - 2
    row_sum = (padded[0:height:2] + 3.0 * padded[1:height + 1:2] + 3.0 * padded[2:height + 2:2]
               + padded[3:height + 3:2]) * 0.125
    col_sum = (row_sum[:, 0:breadth:2] + 3.0 * row_sum[:, 1:breadth + 1:2] + 3.0 * row_sum[:, 2:breadth + 2:2]
               + row_sum[:, 3:breadth + 3:2]) * 0.125
    return 4.0 * col_sum


def prolong_grid(padded):
    centre_rep = jnp.repeat(padded[1:-1], 2, axis=0)
    below_rep = jnp.repeat(padded[:-2], 2, axis=0)
    above_rep = jnp.repeat(padded[2:], 2, axis=0)
    row_ids = jnp.arange(centre_rep.shape[0], dtype=jnp.int32)[:, None]
    stretched = 0.75 * centre_rep + 0.25 * jnp.where(row_ids % 2 == 0, below_rep, above_rep)
    mid_cols = jnp.repeat(stretched[:, 1:-1], 2, axis=1)
    left_cols = jnp.repeat(stretched[:, :-2], 2, axis=1)
    right_cols = jnp.repeat(stretched[:, 2:], 2, axis=1)
    col_ids = jnp.arange(mid_cols.shape[1], dtype=jnp.int32)[None, :]
    return 0.75 * mid_cols + 0.25 * jnp.where(col_ids % 2 == 0, left_cols, right_cols)


def wrap_pad(values, margin):
    values = jnp.pad(values, ((0, 0), (margin, margin)), mode="wrap")
    return jnp.pad(values, ((margin, margin), (0, 0)))


def cycle_local(level_at, iterate, source):
    height, breadth = source.shape
    spacing = 2.0 * math.pi / breadth
    row_ids = jnp.arange(height, dtype=jnp.int32)[:, None]
    col_ids = jnp.arange(breadth, dtype=jnp.int32)[None, :]
    stencil = coefficients(row_ids.astype(jnp.float32), spacing)
    red_cells = (row_ids + col_ids) % 2 == 0
    black_cells = jnp.logical_not(red_cells)

    def colour_sweep(values):
        values = relax_cells(wrap_pad(values, 1), source, stencil, red_cells)
        return relax_cells(wrap_pad(values, 1), source, stencil, black_cells)

    if level_at == LEVELS - 1:
        for _ in range(COARSE_SWEEPS):
            iterate = colour_sweep(iterate)
        return iterate
    for _ in range(PRE):
        iterate = colour_sweep(iterate)
    remainder = source - apply_operator(wrap_pad(iterate, 1), stencil)
    coarse_source = restrict_grid(wrap_pad(remainder, 1))
    correction = cycle_local(level_at + 1, jnp.zeros_like(coarse_source), coarse_source)
    iterate = iterate + prolong_grid(wrap_pad(correction, 1))
    for _ in range(POST):
        iterate = colour_sweep(iterate)
    return iterate


def reference(right_side, guess):
    solution = cycle_local(0, guess, right_side)
    height, breadth = right_side.shape
    row_ids = jnp.arange(height, dtype=jnp.int32)[:, None]
    stencil = coefficients(row_ids.astype(jnp.float32), 2.0 * math.pi / breadth)
    residual = right_side - apply_operator(wrap_pad(solution, 1), stencil)
    return solution, residual
```

```python
import math

import jax
import jax.numpy as jnp
from jax import lax
from jax.experimental import pallas as pl
from jax.experimental.pallas import tpu as pltpu
from jax.sharding import PartitionSpec as P

MESH = pl.DeviceIdType.MESH
F32 = jnp.float32
NR, NT = 2048, 8192
NA, NB = 8, 16
OWN = ((128, 8), (64, 4), (32, 2), (16, 1))
HALO = (8, 40, 16, 16)
BASE = tuple(h + 8 for h in HALO)
ROWS = tuple(o[0] + 2 * b for o, b in zip(OWN, BASE))
WHOLE = ((128, 4), (64, 2), (32, 1), (16, 1))
WB = 8
DIRS = tuple((dr, da) for dr in (-1, 0, 1) for da in (-1, 0, 1) if dr or da)
SIDES = tuple(d for d in DIRS if not d[0])
ENDS = tuple(d for d in DIRS if not d[1])
CORNERS = tuple(d for d in DIRS if d[0] and d[1])
PER = (9, 9, 8, 8)


def blocks(start, count, per, step):
    if count <= per:
        for k in range(count):
            step(start + 8 * k)
        return
    assert count % per == 0

    def body(i, carry):
        for k in range(per):
            step(pl.multiple_of(start + 8 * k + i * (8 * per), 8))
        return carry

    lax.fori_loop(0, count // per, body, 0)


def ids():
    sub = lax.broadcasted_iota(jnp.int32, (8, 128), 0)
    lane = lax.broadcasted_iota(jnp.int32, (8, 128), 1)
    return sub, lane


def ring_shift(tiles, lane):
    n = len(tiles)
    one = [pltpu.roll(x, 1, 1) for x in tiles]
    back = [pltpu.roll(x, 127, 1) for x in tiles]
    if n == 1:
        return one, back
    left = [jnp.where(lane == 0, one[t - 1], one[t]) for t in range(n)]
    right = [jnp.where(lane == 127, back[(t + 1) % n], back[t]) for t in range(n)]
    return left, right


def pick(x, index):
    return jnp.take_along_axis(x, index, axis=1, mode="promise_in_bounds")


def fill_coefficients(c_ref, count, base, first_row, total_rows, cells):
    h = 2.0 * math.pi / cells
    sub, _ = ids()

    def step(p):
        row = first_row + (p - base) + sub
        inside = jnp.logical_and(row >= 0, row < total_rows)
        r = 1.0 + (row.astype(F32) + 0.5) * h
        rr = r * r
        q = jnp.where(inside, 0.5 / (rr + 1.0), 0.0)
        half = (0.5 * h) * r
        at = pl.ds(p, 8)
        c_ref[0, at, :] = (rr + half) * q
        c_ref[1, at, :] = (rr - half) * q
        c_ref[2, at, :] = q
        c_ref[3, at, :] = rr * q
        c_ref[4, at, :] = 2.0 + 2.0 / rr

    blocks(0, count, 4 if count % 4 == 0 else count if count < 4 else 2, step)


def relaxed(src, g, c_ref, p, n, lane):
    at, above, below = pl.ds(p, 8), pl.ds(p + 1, 8), pl.ds(p - 1, 8)
    x = [src[t, at, :] for t in range(n)]
    left, right = ring_shift(x, lane)
    oc, ic, ac = c_ref[0, at, :], c_ref[1, at, :], c_ref[2, at, :]
    new = [
        (g[t, at, :] + oc * src[t, above, :]) + (ic * src[t, below, :] + ac * (left[t] + right[t]))
        for t in range(n)
    ]
    return x, new


def half_sweep(src, dst, g, c_ref, start, count, n, colour, per):
    sub, lane = ids()
    chosen = (sub + lane) % 2 == colour

    def step(p):
        x, new = relaxed(src, g, c_ref, p, n, lane)
        for t in range(n):
            dst[t, pl.ds(p, 8), :] = jnp.where(chosen, new[t], x[t])

    blocks(start, count, per, step)


def residual_pass(src, dst, g, c_ref, start, count, n, per, out_tiles=None):
    _, lane = ids()

    def step(p):
        x, new = relaxed(src, g, c_ref, p, n, lane)
        c = c_ref[4, pl.ds(p, 8), :]
        for t in range(out_tiles or n):
            dst[t, pl.ds(p, 8), :] = c * (new[t] - x[t])

    blocks(start, count, per, step)


def restrict_pass(s, fine_base, n, dst, coarse_base, c_ref, start, count, pairs, per):
    sub, lane = ids()
    even = lane % 2 == 0
    perm = jnp.where(lane < 64, 2 * lane, 2 * lane - 127)
    lo, hi = start // 8, start // 8 + count

    def step(p):
        f = 2 * (p - coarse_base) + fine_base
        r = [
            (s[t, pl.ds(f - 1, 8, stride=2), :] + s[t, pl.ds(f + 2, 8, stride=2), :])
            + 3.0 * (s[t, pl.ds(f, 8, stride=2), :] + s[t, pl.ds(f + 1, 8, stride=2), :])
            for t in range(n)
        ]
        left, right = ring_shift(r, lane)
        m = [3.0 * r[t] + jnp.where(even, left[t], right[t]) for t in range(n)]
        scale = c_ref[3, pl.ds(p, 8), :] * 0.0625
        for k, (a, b) in enumerate(pairs):
            joined = jnp.where(even, m[a] + pltpu.roll(m[a], 127, 1), m[b] + pltpu.roll(m[b], 1, 1))
            dst[k, pl.ds(p, 8), :] = pick(joined, perm) * scale

    del lo, hi
    blocks(coarse_base + start, count, per, step)


def prolong_pass(e, coarse_base, nc, f, start, count, fine, fine_base, plan, per, sealed):
    sub, lane = ids()
    even = lane % 2 == 0
    half = lane // 2
    kinds = (half, half + 64, jnp.where(lane < 64, half, half + 64))

    def across(p):
        x = [e[t, pl.ds(p, 8), :] for t in range(nc)]
        left, right = ring_shift(x, lane)
        a = [0.75 * x[t] + 0.25 * left[t] for t in range(nc)]
        b = [0.75 * x[t] + 0.25 * right[t] for t in range(nc)]
        for t, (source, kind) in enumerate(plan):
            f[t, pl.ds(p - (coarse_base + start) + 8, 8), :] = jnp.where(
                even, pick(a[source], kinds[kind]), pick(b[source], kinds[kind])
            )

    blocks(coarse_base + start, count, per, across)
    if sealed:
        for t in range(len(plan)):
            f[t, pl.ds(0, 8), :] = jnp.zeros((8, 128), F32)
            f[t, pl.ds(8 + 8 * count, 8), :] = jnp.zeros((8, 128), F32)

    def along(p):
        q = 2 * (p - 8 + start) + fine_base
        for t in range(len(plan)):
            mid = 0.75 * f[t, pl.ds(p, 8), :]
            first, second = pl.ds(q, 8, stride=2), pl.ds(q + 1, 8, stride=2)
            fine[t, first, :] = fine[t, first, :] + (mid + 0.25 * f[t, pl.ds(p - 1, 8), :])
            fine[t, second, :] = fine[t, second, :] + (mid + 0.25 * f[t, pl.ds(p + 1, 8), :])

    blocks(8, count, per, along)


def zero_rows(ref, n, start, count):
    for t in range(n):
        for k in range(count):
            ref[t, pl.ds(start + 8 * k, 8), :] = jnp.zeros((8, 128), F32)


def kernel(
    right_hbm, guess_hbm, sol_hbm, res_hbm,
    s0, g0, b0, g1, a1, b1, g2, a2, b2, s3, b3,
    g4, a4, b4, g5, a5, b5, g6, a6, b6, g7, a7, b7,
    win, f_ref, c0, c1, c2, c3, c4, c5, c6, c7,
    pk0, rp0, rd0, rl1, rd1, bk0, br0, bp0, bd0, bs3, own4, slots, strip,
    load_sem, out_sem, send0, recv0, send1, recv1, sendb, recvb, sendc, recvc, senda, recva, sendg, recvg,
):
    me_a, me_r = lax.axis_index("ang"), lax.axis_index("rad")

    def device(dr, da):
        return {"ang": lax.rem(me_a + da + NA, NA), "rad": lax.rem(me_r + dr + NB, NB)}

    a0 = s0.at[0]
    raw = s0.at[1]
    loads = []
    for t in range(8):
        for k, src in ((0, guess_hbm), (1, right_hbm)):
            loads.append(pltpu.make_async_copy(
                src.at[:, pl.ds(128 * t, 128)], s0.at[k, t, pl.ds(BASE[0], 128), :], load_sem.at[k, t]))
    for copy in loads:
        copy.start()

    barrier = pltpu.get_barrier_semaphore()
    partners = list(DIRS) + [(0, d) for d in range(2, NA - 1)] + [(d, 0) for d in range(2, NB - 1)]
    for dr, da in partners:
        pl.semaphore_signal(barrier, inc=1, device_id=device(dr, da), device_id_type=MESH)

    zero = jnp.zeros((8, 128), F32)
    for ref, l in ((a0, 0), (g0, 0), (b0, 0), (g1, 1), (a1, 1), (b1, 1), (g2, 2), (a2, 2), (b2, 2)):
        for t in range(OWN[l][1] + 1):
            ref[t, pl.ds(0, 8), :] = zero
            ref[t, pl.ds(ROWS[l] - 8, 8), :] = zero
    for ref in (s3.at[0], s3.at[1], b3):
        zero_rows(ref, 2, 0, ROWS[3] // 8)
    for l, refs in enumerate(((g4, a4, b4), (g5, a5, b5), (g6, a6, b6), (g7, a7, b7))):
        for ref in refs:
            for t in range(WHOLE[l][1]):
                ref[t, pl.ds(0, 8), :] = zero
                ref[t, pl.ds(WB + WHOLE[l][0], 8), :] = zero
    zero_rows(win, 1, 0, 5)

    def zf(i, carry):
        for t in range(9):
            f_ref[t, pl.ds(pl.multiple_of(8 * i, 8), 8), :] = zero
        return carry

    lax.fori_loop(0, 12, zf, 0)
    for l, c_ref in enumerate((c0, c1, c2, c3)):
        fill_coefficients(c_ref, ROWS[l] // 8, BASE[l], me_r * OWN[l][0], NR >> l, NT >> l)
    for l, c_ref in enumerate((c4, c5, c6, c7)):
        fill_coefficients(c_ref, WHOLE[l][0] // 8 + 2, WB, 0, WHOLE[l][0], NT >> (l + 4))

    sub, lane = ids()

    def pack(src, dst):
        for side, (tile, first) in enumerate(((0, 0), (7, 120))):
            total = None
            for b in range(16):
                x = src[tile, pl.ds(BASE[0] + 8 * b, 8), :]
                shift = (8 * b - first) % 128
                x = pltpu.roll(x, shift, 1) if shift else x
                total = x if total is None else jnp.where(lane // 8 == b, x, total)
            dst[side, :, :] = total

    def unpack(from_left, from_right, dst):
        for b in range(16):
            shift_r, shift_l = (-8 * b) % 128, (120 - 8 * b) % 128
            x = pltpu.roll(from_right, shift_r, 1) if shift_r else from_right
            y = pltpu.roll(from_left, shift_l, 1) if shift_l else from_left
            dst[8, pl.ds(BASE[0] + 8 * b, 8), :] = jnp.where(lane < 64, x, y)

    def remote(src, dst, sems, recvs, k, dr, da):
        return pltpu.make_async_remote_copy(
            src_ref=src, dst_ref=dst, send_sem=sems.at[k], recv_sem=recvs.at[k],
            device_id=device(dr, da), device_id_type=MESH)

    def edge(l, dr, width):
        if dr < 0:
            return pl.ds(BASE[l], width), pl.ds(BASE[l] + OWN[l][0], width)
        return pl.ds(BASE[l] + OWN[l][0] - width, width), pl.ds(BASE[l] - width, width)

    for copy in loads:
        copy.wait()
    for k in range(2):
        pack(s0.at[k], pk0.at[k])
    pl.semaphore_wait(barrier, len(partners))

    sends = []
    for k, (dr, da) in enumerate(DIRS):
        if da == 0:
            mine, theirs = edge(0, dr, 8)
            copy = remote(s0.at[:, pl.ds(0, 8), mine, :], s0.at[:, pl.ds(0, 8), theirs, :], send0, recv0, k, dr, da)
        elif dr == 0:
            side = 0 if da < 0 else 1
            copy = remote(pk0.at[:, side], rp0.at[:, side], send0, recv0, k, dr, da)
        else:
            mine, _ = edge(0, dr, 8)
            tile = 0 if da < 0 else 7
            copy = remote(s0.at[:, tile, mine, :], rd0.at[CORNERS.index((dr, da))], send0, recv0, k, dr, da)
        copy.start()
        sends.append(copy)

    def scale_own(p):
        w = c0[3, pl.ds(p, 8), :]
        for t in range(8):
            g0[t, pl.ds(p, 8), :] = raw[t, pl.ds(p, 8), :] * w

    blocks(BASE[0], 16, 8, scale_own)
    for copy in sends:
        copy.wait()

    def corners(dst, tile, buf, rows, l):
        for dr in (-1, 1):
            start = BASE[l] - rows if dr < 0 else BASE[l] + OWN[l][0]
            right = CORNERS.index((-dr, -1))
            left = CORNERS.index((-dr, 1))
            for j in range(rows // 8):
                x = buf(right)[pl.ds(8 * j, 8), :]
                y = buf(left)[pl.ds(8 * j, 8), :]
                dst[tile, pl.ds(start + 8 * j, 8), :] = jnp.where(lane < 64, x, y)

    for k in range(2):
        unpack(rp0[k, 1], rp0[k, 0], s0.at[k])
        corners(s0.at[k], 8, lambda c, k=k: rd0.at[c, k], 8, 0)

    def clear_outside(refs, l, n, depth):
        @pl.when(me_r == 0)
        def _():
            for ref in refs:
                zero_rows(ref, n, BASE[l] - depth, depth // 8)

        @pl.when(me_r == NB - 1)
        def _():
            for ref in refs:
                zero_rows(ref, n, BASE[l] + OWN[l][0], depth // 8)

    clear_outside((a0, raw), 0, 9, 8)
    for p in (8, BASE[0] + 128):
        w = c0[3, pl.ds(p, 8), :]
        for t in range(8):
            g0[t, pl.ds(p, 8), :] = raw[t, pl.ds(p, 8), :] * w

    def scale_tile(p):
        g0[8, pl.ds(p, 8), :] = raw[8, pl.ds(p, 8), :] * c0[3, pl.ds(p, 8), :]

    blocks(8, 18, 18, scale_tile)

    for colour, src, dst in ((0, a0, b0), (1, b0, a0), (0, a0, b0), (1, b0, a0)):
        half_sweep(src, dst, g0, c0, 8, 18, 9, colour, PER[0])
    residual_pass(a0, b0, g0, c0, 8, 18, 9, PER[0])
    restrict_pass(b0, BASE[0], 9, g1, BASE[1], c1, 0, 8, ((0, 1), (2, 3), (4, 5), (6, 7)), 4)

    sends = []
    for k, (dr, da) in enumerate(DIRS):
        tile = 0 if da < 0 else 3
        mine, theirs = edge(1, dr, 40) if dr else (pl.ds(BASE[1], 64), None)
        if da == 0:
            copy = remote(g1.at[pl.ds(0, 4), mine, :], g1.at[pl.ds(0, 4), theirs, :], send1, recv1, k, dr, da)
        elif dr == 0:
            copy = remote(g1.at[tile, mine, :], rl1.at[0 if da < 0 else 1], send1, recv1, k, dr, da)
        else:
            copy = remote(g1.at[tile, mine, :], rd1.at[CORNERS.index((dr, da))], send1, recv1, k, dr, da)
        copy.start()
        sends.append(copy)
    pack(a0, bk0)
    for copy in sends:
        copy.wait()

    back = []
    for k, (dr, da) in enumerate(DIRS):
        if da == 0:
            mine, _ = edge(0, dr, 8)
            copy = remote(a0.at[pl.ds(0, 8), mine, :], br0.at[0 if dr < 0 else 1], sendb, recvb, k, dr, da)
        elif dr == 0:
            side = 0 if da < 0 else 1
            copy = remote(bk0.at[side], bp0.at[side], sendb, recvb, k, dr, da)
        else:
            mine, _ = edge(0, dr, 8)
            copy = remote(a0.at[0 if da < 0 else 7, mine, :], bd0.at[CORNERS.index((dr, da))], sendb, recvb, k, dr, da)
        copy.start()
        back.append(copy)

    for b in range(8):
        g1[4, pl.ds(BASE[1] + 8 * b, 8), :] = jnp.where(
            lane < 64, rl1[0, pl.ds(8 * b, 8), :], rl1[1, pl.ds(8 * b, 8), :])
    corners(g1, 4, lambda c: rd1.at[c], 40, 1)
    clear_outside((g1,), 1, 5, 40)

    g3, a3 = s3.at[0], s3.at[1]

    def down(g, a, b, c, start, count, n, per):
        half_sweep(g, a, g, c, start, count, n, 1, per)
        half_sweep(a, b, g, c, start, count, n, 0, per)
        half_sweep(b, a, g, c, start, count, n, 1, per)
        residual_pass(a, b, g, c, start, count, n, per)

    down(g1, a1, b1, c1, 8, 18, 5, PER[1])
    restrict_pass(b1, BASE[1], 5, g2, BASE[2], c2, -16, 8, ((0, 1), (2, 3), (4, 4)), 8)
    down(g2, a2, b2, c2, BASE[2] - 16, 8, 3, PER[2])
    restrict_pass(b2, BASE[2], 3, g3, BASE[3], c3, -8, 4, ((0, 1), (2, 2)), 4)
    down(g3, a3, b3, c3, BASE[3] - 8, 4, 2, PER[3])

    sub, lane = ids()
    even = lane % 2 == 0
    r = [
        (b3[t, pl.ds(BASE[3] - 1, 8, stride=2), :] + b3[t, pl.ds(BASE[3] + 2, 8, stride=2), :])
        + 3.0 * (b3[t, pl.ds(BASE[3], 8, stride=2), :] + b3[t, pl.ds(BASE[3] + 1, 8, stride=2), :])
        for t in range(2)
    ]
    left, right = ring_shift(r, lane)
    m = 3.0 * r[0] + jnp.where(even, left[0], right[0])
    joined = jnp.where(even, m + pltpu.roll(m, 127, 1), m + pltpu.roll(m, 1, 1))
    perm = jnp.where(lane < 64, 2 * lane, 2 * lane - 127)
    my_rows = pl.ds(pl.multiple_of(WB + 8 * me_r, 8), 8)
    own4[...] = pick(joined, perm) * (c4[3, my_rows, :] * 0.0625)

    ring = []
    for d in range(1, NA):
        copy = remote(own4, slots.at[d - 1], senda, recva, d - 1, 0, d)
        copy.start()
        ring.append(copy)
    back3 = []
    for k, (dr, da) in enumerate(DIRS):
        copy = remote(s3.at[:, 0, pl.ds(BASE[3], 16), :], bs3.at[k], sendc, recvc, k, dr, da)
        copy.start()
        back3.append(copy)
    for copy in ring:
        copy.wait()
    for t in range(4):
        total = own4[...]
        for d in range(1, NA):
            source = lax.rem(me_a - d + NA, NA)
            hit = jnp.logical_and(source // 2 == t, lane // 64 == source % 2)
            total = jnp.where(hit, slots[d - 1], total)
        strip[t, :, :] = total
        g4[t, my_rows, :] = total
    column = []
    for d in range(1, NB):
        copy = remote(strip, g4.at[:, my_rows, :], sendg, recvg, d - 1, d, 0)
        copy.start()
        column.append(copy)
    for copy in column:
        copy.wait()

    def whole_down(g, a, b, c, l):
        down(g, a, b, c, WB, WHOLE[l][0] // 8, WHOLE[l][1], 16)

    def post(a, b, g, c, start, count, n, per):
        for colour, src, dst in ((0, a, b), (1, b, a), (0, a, b), (1, b, a)):
            half_sweep(src, dst, g, c, start, count, n, colour, per)

    whole_down(g4, a4, b4, c4, 0)
    restrict_pass(b4, WB, 4, g5, WB, c5, 0, 8, ((0, 1), (2, 3)), 8)
    whole_down(g5, a5, b5, c5, 1)
    restrict_pass(b5, WB, 2, g6, WB, c6, 0, 4, ((0, 1),), 4)
    whole_down(g6, a6, b6, c6, 2)
    restrict_pass(b6, WB, 1, g7, WB, c7, 0, 2, ((0, 0),), 2)
    half_sweep(g7, a7, g7, c7, WB, 2, 1, 1, 2)

    def coarse(i, carry):
        half_sweep(a7, b7, g7, c7, WB, 2, 1, 0, 2)
        half_sweep(b7, a7, g7, c7, WB, 2, 1, 1, 2)
        return carry

    lax.fori_loop(0, 7, coarse, 0)
    prolong_pass(a7, WB, 1, f_ref, 0, 2, a6, WB, ((0, 0),), 2, True)
    post(a6, b6, g6, c6, WB, 4, 1, 4)
    prolong_pass(a6, WB, 1, f_ref, 0, 4, a5, WB, ((0, 0), (0, 1)), 4, True)
    post(a5, b5, g5, c5, WB, 8, 2, 8)
    prolong_pass(a5, WB, 2, f_ref, 0, 8, a4, WB, ((0, 0), (0, 1), (1, 0), (1, 1)), 8, True)
    post(a4, b4, g4, c4, WB, 16, 4, 16)

    for k in range(3):
        rows = pl.ds(pl.multiple_of(WB + 8 * me_r, 8) + 8 * (k - 1), 8)

        def block(da, wanted):
            b = lax.rem(me_a + da + NA, NA)
            x = a4[b // 2, rows, :]
            return jnp.where(b % 2 == wanted, x, pltpu.roll(x, 64, 1))

        mine, rightward, leftward = block(0, 0), block(1, 1), block(-1, 1)
        win[0, pl.ds(8 + 8 * k, 8), :] = jnp.where(lane < 64, mine, jnp.where(lane < 96, rightward, leftward))

    for copy in back3:
        copy.wait()
    for q, ref in enumerate((g3, a3)):
        for half in range(2):
            at = pl.ds(8 * half, 8)
            got = lambda dr, da: bs3[DIRS.index((-dr, -da)), q, at, :]
            ref[0, pl.ds(BASE[3] - 16 + 8 * half, 8), :] = got(-1, 0)
            ref[0, pl.ds(BASE[3] + 16 + 8 * half, 8), :] = got(1, 0)
            for dr in (-1, 0, 1):
                ref[1, pl.ds(BASE[3] + 16 * dr + 8 * half, 8), :] = jnp.where(lane < 64, got(dr, 1), got(dr, -1))
    clear_outside((g3,), 3, 2, 16)
    prolong_pass(win, 16, 1, f_ref, -8, 3, a3, BASE[3], ((0, 0), (0, 1)), 3, False)
    clear_outside((a3,), 3, 2, 16)
    post(a3, b3, g3, c3, BASE[3] - 16, 6, 2, 6)

    prolong_pass(a3, BASE[3], 2, f_ref, -8, 4, a2, BASE[2], ((0, 0), (0, 1), (1, 2)), 4, False)
    clear_outside((a2,), 2, 3, 16)
    post(a2, b2, g2, c2, BASE[2] - 8, 6, 3, 6)

    prolong_pass(a2, BASE[2], 3, f_ref, -8, 6, a1, BASE[1], ((0, 0), (0, 1), (1, 0), (1, 1), (2, 2)), 6, False)
    clear_outside((a1,), 1, 5, 16)
    post(a1, b1, g1, c1, BASE[1] - 8, 10, 5, 10)

    for copy in back:
        copy.wait()
    unpack(bp0[1], bp0[0], a0)
    corners(a0, 8, lambda c: bd0.at[c], 8, 0)
    for t in range(8):
        a0[t, pl.ds(BASE[0] + 128, 8), :] = br0[0, t]
        a0[t, pl.ds(8, 8), :] = br0[1, t]
    plan = tuple((t // 2, t % 2) for t in range(8)) + ((4, 2),)
    prolong_pass(a1, BASE[1], 5, f_ref, -8, 10, a0, BASE[0], plan, 5, False)
    clear_outside((a0,), 0, 9, 16)
    post(a0, b0, g0, c0, 8, 18, 9, PER[0])

    outs = []
    for t in range(8):
        copy = pltpu.make_async_copy(
            a0.at[t, pl.ds(BASE[0], 128), :], sol_hbm.at[:, pl.ds(128 * t, 128)], out_sem.at[0, t])
        copy.start()
        outs.append(copy)
    residual_pass(a0, b0, g0, c0, BASE[0], 16, 9, 8, out_tiles=8)
    for t in range(8):
        copy = pltpu.make_async_copy(
            b0.at[t, pl.ds(BASE[0], 128), :], res_hbm.at[:, pl.ds(128 * t, 128)], out_sem.at[1, t])
        copy.start()
        outs.append(copy)
    for copy in outs:
        copy.wait()


def local(right_side, guess):
    def vm(*shape):
        return pltpu.VMEM(shape, F32)

    levels = [vm(2, 9, ROWS[0], 128), vm(9, ROWS[0], 128), vm(9, ROWS[0], 128)]
    for l in (1, 2):
        levels += [vm(OWN[l][1] + 1, ROWS[l], 128)] * 3
    levels += [vm(2, 2, ROWS[3], 128), vm(2, ROWS[3], 128)]
    for rows, tiles in WHOLE:
        levels += [vm(tiles, rows + 2 * WB, 128)] * 3
    coefficients = [vm(5, r, 128) for r in ROWS] + [vm(5, rows + 2 * WB, 128) for rows, _ in WHOLE]
    buffers = [
        vm(2, 2, 8, 128), vm(2, 2, 8, 128), vm(4, 2, 8, 128),
        vm(2, 64, 128), vm(4, 40, 128),
        vm(2, 8, 128), vm(2, 8, 8, 128), vm(2, 8, 128), vm(4, 8, 128),
        vm(8, 2, 16, 128), vm(8, 128), vm(NA - 1, 8, 128), vm(4, 8, 128),
    ]
    dma = pltpu.SemaphoreType.DMA
    sems = [dma((2, 8)), dma((2, 8))] + [dma((8,))] * 8 + [dma((NA - 1,))] * 2 + [dma((NB - 1,))] * 2
    block = jax.ShapeDtypeStruct(right_side.shape, F32)
    return pl.pallas_call(
        kernel,
        out_shape=(block, block),
        in_specs=[pl.BlockSpec(memory_space=pl.ANY)] * 2,
        out_specs=(pl.BlockSpec(memory_space=pl.ANY),) * 2,
        scratch_shapes=levels + [vm(1, 40, 128), vm(9, 96, 128)] + coefficients + buffers + sems,
        compiler_params=pltpu.CompilerParams(collective_id=0, has_side_effects=True),
    )(right_side, guess)


def solution(mesh):
    placed = (P("rad", "ang"), P("rad", "ang"))
    return jax.shard_map(local, mesh=mesh, in_specs=placed, out_specs=placed, check_vma=False)
```

```python
import math

import jax
import jax.numpy as jnp
from jax import lax
from jax.experimental import pallas as pl
from jax.experimental.pallas import tpu as pltpu
from jax.sharding import PartitionSpec as P

MESH = pl.DeviceIdType.MESH
F32 = jnp.float32
NR, NT = 2048, 8192
NA, NB = 8, 16
OWN = ((64, 8), (32, 4), (16, 2), (8, 1))
BASE = (8, 24, 16, 16)
ROWS = tuple(o[0] + 2 * b for o, b in zip(OWN, BASE))
E0, E1 = 5, 18
WHOLE = ((64, 4), (32, 2), (16, 1), (8, 1))
WB = 8
DIRS = tuple((dr, da) for dr in (-1, 0, 1) for da in (-1, 0, 1) if dr or da)
CORNERS = tuple(d for d in DIRS if d[0] and d[1])
FB = 16


def grid_ids():
    sub = lax.broadcasted_iota(jnp.int32, (8, 128), 0)
    lane = lax.broadcasted_iota(jnp.int32, (8, 128), 1)
    return sub, lane


def ring_shift(tiles, lane):
    n = len(tiles)
    one = [pltpu.roll(x, 1, 1) for x in tiles]
    back = [pltpu.roll(x, 127, 1) for x in tiles]
    if n == 1:
        return one, back
    left = [jnp.where(lane == 0, one[t - 1], one[t]) for t in range(n)]
    right = [jnp.where(lane == 127, back[(t + 1) % n], back[t]) for t in range(n)]
    return left, right


def pick(x, index):
    return jnp.take_along_axis(x, index, axis=1, mode="promise_in_bounds")


def fill_coefficients(c_ref, count, base, first_row, total_rows, cells):
    h = 2.0 * math.pi / cells
    sub, lane = grid_ids()
    even = lane % 2 == 0

    def row_values(row):
        inside = jnp.logical_and(row >= 0, row < total_rows)
        r = 1.0 + (row.astype(F32) + 0.5) * h
        rr = r * r
        q = jnp.where(inside, 0.5 / (rr + 1.0), 0.0)
        half = (0.5 * h) * r
        return (rr + half) * q, (rr - half) * q, q, rr * q, 2.0 + 2.0 / rr

    for k in range(count):
        row = first_row + 2 * (8 * k - base + sub)
        o0, i0, a0, w0, c0 = row_values(row)
        o1, i1, a1, w1, c1 = row_values(row + 1)
        at = pl.ds(8 * k, 8)
        for j, (x, y) in enumerate(((o0, i1), (i0, o1), (a0, a1), (w0, w1), (c0, c1))):
            c_ref[j, at, :] = jnp.where(even, x, y)
            c_ref[5 + j, at, :] = jnp.where(even, y, x)


def relaxed(src, g, c_ref, colour, p, n, lane):
    at = pl.ds(p, 8)
    even = lane % 2 == 0
    first, second = (p - 1, p + 1) if colour == 0 else (p + 1, p - 1)
    x = [src[t, at, :] for t in range(n)]
    left, right = ring_shift(x, lane)
    near, far, ang = (c_ref[5 * colour + k, at, :] for k in range(3))
    return [
        (g[t, at, :] + near * x[t])
        + (far * jnp.where(even, src[t, pl.ds(first, 8), :], src[t, pl.ds(second, 8), :]) + ang * (left[t] + right[t]))
        for t in range(n)
    ]


def half_sweep(dst, src, g, c_ref, colour, start, count, n):
    _, lane = grid_ids()
    for k in range(count):
        p = start + 8 * k
        new = relaxed(src, g, c_ref, colour, p, n, lane)
        for t in range(n):
            dst[t, pl.ds(p, 8), :] = new[t]


def residual_pass(dst, old, src, g, c_ref, colour, start, count, n, out_tiles=None):
    _, lane = grid_ids()
    for k in range(count):
        p = start + 8 * k
        new = relaxed(src, g, c_ref, colour, p, n, lane)
        c = c_ref[5 * colour + 4, pl.ds(p, 8), :]
        for t in range(out_tiles or n):
            dst[t, pl.ds(p, 8), :] = c * (new[t] - old[t, pl.ds(p, 8), :])


def restricted_block(s, p, n, pairs, lane):
    even = lane % 2 == 0
    perm = jnp.where(lane < 64, 2 * lane, 2 * lane - 127)
    r = [
        3.0 * s[t, pl.ds(p, 8), :] + jnp.where(even, s[t, pl.ds(p + 1, 8), :], s[t, pl.ds(p - 1, 8), :])
        for t in range(n)
    ]
    left, right = ring_shift(r, lane)
    m = [3.0 * r[t] + jnp.where(even, left[t], right[t]) for t in range(n)]
    out = []
    for a, b in pairs:
        joined = jnp.where(even, m[a] + pltpu.roll(m[a], 127, 1), m[b] + pltpu.roll(m[b], 1, 1))
        out.append(pick(joined, perm) * 0.0625)
    return out


def restrict_pass(s, fine_base, n, nat, g, coarse_base, c_ref, start, count, pairs):
    _, lane = grid_ids()
    even = lane % 2 == 0
    for k in range(2 * count):
        for t, x in enumerate(restricted_block(s, fine_base + 2 * start + 8 * k, n, pairs, lane)):
            nat[t, pl.ds(8 * k, 8), :] = x
    for k in range(count):
        p = pl.ds(coarse_base + start + 8 * k, 8)
        red, black = c_ref[3, p, :], c_ref[8, p, :]
        for t in range(len(pairs)):
            x = nat[t, pl.ds(16 * k, 8, stride=2), :]
            y = nat[t, pl.ds(16 * k + 1, 8, stride=2), :]
            g[0, t, p, :] = jnp.where(even, x, y) * red
            g[1, t, p, :] = jnp.where(even, y, x) * black


def unpair(red, black, p, dst, q, n):
    _, lane = grid_ids()
    even = lane % 2 == 0
    for t in range(n):
        x, y = red[t, pl.ds(p, 8), :], black[t, pl.ds(p, 8), :]
        dst[t, pl.ds(q, 8, stride=2), :] = jnp.where(even, x, y)
        dst[t, pl.ds(q + 1, 8, stride=2), :] = jnp.where(even, y, x)


def prolong_pass(e, f, start, count, fine, fine_base, fine_start, fine_count, plan, sealed):
    _, lane = grid_ids()
    even = lane % 2 == 0
    half = lane // 2
    kinds = (half, half + 64, jnp.where(lane < 64, half, half + 64))
    nc = max(source for source, _ in plan) + 1
    for k in range(count):
        p = FB + start + 8 * k
        x = [e[t, pl.ds(p, 8), :] for t in range(nc)]
        left, right = ring_shift(x, lane)
        a = [0.75 * x[t] + 0.25 * left[t] for t in range(nc)]
        b = [0.75 * x[t] + 0.25 * right[t] for t in range(nc)]
        for t, (source, kind) in enumerate(plan):
            f[t, pl.ds(p, 8), :] = jnp.where(even, pick(a[source], kinds[kind]), pick(b[source], kinds[kind]))
    if sealed:
        for t in range(len(plan)):
            f[t, pl.ds(FB - 8, 8), :] = jnp.zeros((8, 128), F32)
            f[t, pl.ds(FB + 8 * count, 8), :] = jnp.zeros((8, 128), F32)
    for k in range(fine_count):
        i = fine_start + 8 * k
        at = pl.ds(fine_base + i, 8)
        for t in range(len(plan)):
            other = jnp.where(even, f[t, pl.ds(FB + i + 1, 8), :], f[t, pl.ds(FB + i - 1, 8), :])
            fine[t, at, :] = fine[t, at, :] + (0.75 * f[t, pl.ds(FB + i, 8), :] + 0.25 * other)


def zero_rows(ref, n, start, count):
    for t in range(n):
        for k in range(count):
            ref[t, pl.ds(start + 8 * k, 8), :] = jnp.zeros((8, 128), F32)


def down(r, k, g, s, c, start, count, n):
    half_sweep(k, g.at[0], g.at[1], c, 1, start, count, n)
    half_sweep(r, k, g.at[0], c, 0, start, count, n)
    half_sweep(k, r, g.at[1], c, 1, start, count, n)
    residual_pass(s, r, k, g.at[0], c, 0, start, count, n)


def post(r, k, g, c, start, count, n):
    for _ in range(2):
        half_sweep(r, k, g.at[0], c, 0, start, count, n)
        half_sweep(k, r, g.at[1], c, 1, start, count, n)


def kernel(
    right_hbm, guess_hbm, sol_hbm, res_hbm,
    raw, x0, r0, s0, g1, r1, k1, s1, g2, r2, k2, s2, x3, r3, s3,
    g4, r4, k4, s4, g5, r5, k5, s5, g6, r6, k6, s6, g7, r7, k7,
    win, e_ref, f_ref, nat, c0, c1, c2, c3, c4, c5, c6, c7,
    pk0, rp0, rd0, rl1, rd1, bs3, own4, slots, strip,
    load_sem, out_sem, send0, recv0, send1, recv1, sendc, recvc, senda, recva, sendg, recvg,
):
    me_a, me_r = lax.axis_index("ang"), lax.axis_index("rad")

    def device(dr, da):
        return {"ang": lax.rem(me_a + da + NA, NA), "rad": lax.rem(me_r + dr + NB, NB)}

    loads = []
    for t in range(8):
        for k, src in ((0, guess_hbm), (1, right_hbm)):
            loads.append(pltpu.make_async_copy(
                src.at[:, pl.ds(128 * t, 128)], raw.at[k, t], load_sem.at[k, t]))
    for copy in loads:
        copy.start()

    barrier = pltpu.get_barrier_semaphore()
    partners = list(DIRS) + [(0, d) for d in range(2, NA - 1)] + [(d, 0) for d in range(2, NB - 1)]
    for dr, da in partners:
        pl.semaphore_signal(barrier, inc=1, device_id=device(dr, da), device_id_type=MESH)

    zero = jnp.zeros((8, 128), F32)
    k0, g0 = x0.at[0], x0.at[pl.ds(1, 2)]
    k3, g3 = x3.at[0], x3.at[pl.ds(1, 2)]
    edges = [(r, 0) for r in (r0, s0)] + [(r, 1) for r in (r1, k1, s1)]
    edges += [(r, 2) for r in (g2.at[0], g2.at[1], r2, k2, s2)]
    edges += [(r, 3) for r in (k3, x3.at[1], x3.at[2], r3, s3)]
    for ref, l in edges:
        depth = 1 if l < 2 else 2
        for t in range(OWN[l][1] + 1):
            for d in range(depth):
                ref[t, pl.ds(8 * d, 8), :] = zero
                ref[t, pl.ds(ROWS[l] - 8 - 8 * d, 8), :] = zero
    for l, refs in enumerate(((g4, r4, k4, s4), (g5, r5, k5, s5), (g6, r6, k6, s6), (g7, r7, k7))):
        for ref in refs:
            for x in ((ref.at[0], ref.at[1]) if len(ref.shape) == 4 else (ref,)):
                for t in range(WHOLE[l][1]):
                    x[t, pl.ds(0, 8), :] = zero
                    x[t, pl.ds(WB + WHOLE[l][0], 8), :] = zero
    zero_rows(win, 1, 0, 6)
    for t in range(9):
        for d in (0, 1, 10, 11):
            f_ref[t, pl.ds(8 * d, 8), :] = zero
    for l, c_ref in enumerate((c0, c1, c2, c3)):
        fill_coefficients(c_ref, ROWS[l] // 8, BASE[l], me_r * (2 * OWN[l][0]), NR >> l, NT >> l)
    for l, c_ref in enumerate((c4, c5, c6, c7)):
        fill_coefficients(c_ref, WHOLE[l][0] // 8 + 2, WB, 0, 2 * WHOLE[l][0], NT >> (l + 4))

    sub, lane = grid_ids()
    even = lane % 2 == 0

    def remote(src, dst, sems, recvs, k, dr, da):
        return pltpu.make_async_remote_copy(
            src_ref=src, dst_ref=dst, send_sem=sems.at[k], recv_sem=recvs.at[k],
            device_id=device(dr, da), device_id_type=MESH)

    def edge(l, dr, width):
        if dr < 0:
            return pl.ds(BASE[l], width), pl.ds(BASE[l] + OWN[l][0], width)
        return pl.ds(BASE[l] + OWN[l][0] - width, width), pl.ds(BASE[l] - width, width)

    for copy in loads:
        copy.wait()
    for k in range(8):
        at = pl.ds(BASE[0] + 8 * k, 8)
        red, black = c0[3, at, :], c0[8, at, :]
        for t in range(8):
            k0[t, at, :] = jnp.where(
                even, raw[0, t, pl.ds(16 * k + 1, 8, stride=2), :], raw[0, t, pl.ds(16 * k, 8, stride=2), :])
            x = raw[1, t, pl.ds(16 * k, 8, stride=2), :]
            y = raw[1, t, pl.ds(16 * k + 1, 8, stride=2), :]
            g0[0, t, at, :] = jnp.where(even, x, y) * red
            g0[1, t, at, :] = jnp.where(even, y, x) * black
    for q in range(3):
        for side, (tile, first) in enumerate(((0, 0), (7, 112))):
            total = None
            for b in range(8):
                x = x0[q, tile, pl.ds(BASE[0] + 8 * b, 8), :]
                shift = (16 * b - first) % 128
                x = pltpu.roll(x, shift, 1) if shift else x
                total = x if total is None else jnp.where(lane // 16 == b, x, total)
            pk0[side, q, :, :] = total
    pl.semaphore_wait(barrier, len(partners))

    sends = []
    for k, (dr, da) in enumerate(DIRS):
        if da == 0:
            mine, theirs = edge(0, dr, E0)
            copy = remote(x0.at[:, pl.ds(0, 8), mine, :], x0.at[:, pl.ds(0, 8), theirs, :], send0, recv0, k, dr, da)
        elif dr == 0:
            side = 0 if da < 0 else 1
            copy = remote(pk0.at[side], rp0.at[side], send0, recv0, k, dr, da)
        else:
            mine, _ = edge(0, dr, E0)
            tile = 0 if da < 0 else 7
            copy = remote(
                x0.at[:, tile, mine, :], rd0.at[CORNERS.index((dr, da)), :, pl.ds(0, E0), :], send0, recv0, k, dr, da)
        copy.start()
        sends.append(copy)
    for copy in sends:
        copy.wait()

    def clear_outside(refs, l, n, depth=1):
        @pl.when(me_r == 0)
        def _():
            for ref in refs:
                zero_rows(ref, n, BASE[l] - 8 * depth, depth)

        @pl.when(me_r == NB - 1)
        def _():
            for ref in refs:
                zero_rows(ref, n, BASE[l] + OWN[l][0], depth)

    for q in range(3):
        from_left, from_right = rp0[1, q], rp0[0, q]
        for b in range(8):
            shift_r, shift_l = (-16 * b) % 128, (112 - 16 * b) % 128
            x = pltpu.roll(from_right, shift_r, 1) if shift_r else from_right
            y = pltpu.roll(from_left, shift_l, 1) if shift_l else from_left
            x0[q, 8, pl.ds(BASE[0] + 8 * b, 8), :] = jnp.where(lane < 64, x, y)
        for dr in (-1, 1):
            start = BASE[0] - E0 if dr < 0 else BASE[0] + OWN[0][0]
            x = rd0[CORNERS.index((-dr, -1)), q, pl.ds(0, E0), :]
            y = rd0[CORNERS.index((-dr, 1)), q, pl.ds(0, E0), :]
            x0[q, 8, pl.ds(start, E0), :] = jnp.where(lane[:E0] < 64, x, y)
    clear_outside((k0, g0.at[0], g0.at[1]), 0, 9)

    for _ in range(2):
        half_sweep(r0, k0, g0.at[0], c0, 0, 4, 9, 9)
        half_sweep(k0, r0, g0.at[1], c0, 1, 4, 9, 9)
    residual_pass(s0, r0, k0, g0.at[0], c0, 0, 4, 9, 9)
    restrict_pass(s0, BASE[0], 9, nat, g1, BASE[1], c1, 0, 4, ((0, 1), (2, 3), (4, 5), (6, 7)))

    sends = []
    for k, (dr, da) in enumerate(DIRS):
        tile = 0 if da < 0 else 3
        mine, theirs = edge(1, dr, E1) if dr else (pl.ds(BASE[1], 32), None)
        if da == 0:
            copy = remote(g1.at[:, pl.ds(0, 4), mine, :], g1.at[:, pl.ds(0, 4), theirs, :], send1, recv1, k, dr, da)
        elif dr == 0:
            copy = remote(g1.at[:, tile, mine, :], rl1.at[0 if da < 0 else 1], send1, recv1, k, dr, da)
        else:
            copy = remote(
                g1.at[:, tile, mine, :], rd1.at[CORNERS.index((dr, da)), :, pl.ds(0, E1), :], send1, recv1, k, dr, da)
        copy.start()
        sends.append(copy)
    for copy in sends:
        copy.wait()
    for q in range(2):
        for b in range(4):
            g1[q, 4, pl.ds(BASE[1] + 8 * b, 8), :] = jnp.where(
                lane < 64, rl1[0, q, pl.ds(8 * b, 8), :], rl1[1, q, pl.ds(8 * b, 8), :])
        for dr in (-1, 1):
            start = BASE[1] - E1 if dr < 0 else BASE[1] + OWN[1][0]
            for first, size in ((0, 8), (8, 8), (16, 2)):
                x = rd1[CORNERS.index((-dr, -1)), q, pl.ds(first, size), :]
                y = rd1[CORNERS.index((-dr, 1)), q, pl.ds(first, size), :]
                g1[q, 4, pl.ds(start + first, size), :] = jnp.where(lane[:size] < 64, x, y)
            rest = BASE[1] - E1 - 3 if dr < 0 else BASE[1] + OWN[1][0] + E1
            for t in range(5):
                g1[q, t, pl.ds(rest, 3), :] = jnp.zeros((3, 128), F32)
    clear_outside((g1.at[0], g1.at[1]), 1, 5, 3)

    down(r1, k1, g1, s1, c1, BASE[1] - 20, 9, 5)
    restrict_pass(s1, BASE[1], 5, nat, g2, BASE[2], c2, -8, 4, ((0, 1), (2, 3), (4, 4)))
    down(r2, k2, g2, s2, c2, BASE[2] - 8, 4, 3)
    restrict_pass(s2, BASE[2], 3, nat, g3, BASE[3], c3, -4, 2, ((0, 1), (2, 2)))
    down(r3, k3, g3, s3, c3, BASE[3] - 4, 2, 2)

    nat[0, pl.ds(0, 8), :] = restricted_block(s3, BASE[3], 2, ((0, 0),), lane)[0]
    x, y = nat[0, pl.ds(0, 4, stride=2), :], nat[0, pl.ds(1, 4, stride=2), :]
    my_pairs = pl.ds(WB + 4 * me_r, 4)
    own4[pl.ds(0, 4), :] = jnp.where(even[:4], x, y) * c4[3, my_pairs, :]
    own4[pl.ds(4, 4), :] = jnp.where(even[:4], y, x) * c4[8, my_pairs, :]
    ring = []
    for d in range(1, NA):
        copy = remote(own4, slots.at[d - 1], senda, recva, d - 1, 0, d)
        copy.start()
        ring.append(copy)
    back3 = []
    for k, (dr, da) in enumerate(DIRS):
        copy = remote(x3.at[:, 0, pl.ds(BASE[3], 8), :], bs3.at[k], sendc, recvc, k, dr, da)
        copy.start()
        back3.append(copy)
    for copy in ring:
        copy.wait()
    for t in range(4):
        total = own4[...]
        for d in range(1, NA):
            source = lax.rem(me_a - d + NA, NA)
            hit = jnp.logical_and(source // 2 == t, lane // 64 == source % 2)
            total = jnp.where(hit, slots[d - 1], total)
        for q in range(2):
            strip[q, t, pl.ds(0, 4), :] = total[4 * q:4 * q + 4]
            g4[q, t, my_pairs, :] = total[4 * q:4 * q + 4]
    column = []
    for d in range(1, NB):
        copy = remote(strip.at[:, :, pl.ds(0, 4), :], g4.at[:, :, my_pairs, :], sendg, recvg, d - 1, d, 0)
        copy.start()
        column.append(copy)
    for copy in column:
        copy.wait()

    down(r4, k4, g4, s4, c4, WB, 8, 4)
    restrict_pass(s4, WB, 4, nat, g5, WB, c5, 0, 4, ((0, 1), (2, 3)))
    down(r5, k5, g5, s5, c5, WB, 4, 2)
    restrict_pass(s5, WB, 2, nat, g6, WB, c6, 0, 2, ((0, 1),))
    down(r6, k6, g6, s6, c6, WB, 2, 1)
    restrict_pass(s6, WB, 1, nat, g7, WB, c7, 0, 1, ((0, 0),))
    half_sweep(k7, g7.at[0], g7.at[1], c7, 1, WB, 1, 1)
    for _ in range(7):
        half_sweep(r7, k7, g7.at[0], c7, 0, WB, 1, 1)
        half_sweep(k7, r7, g7.at[1], c7, 1, WB, 1, 1)

    def whole_up(rc, kc, blocks, nc, fine, plan):
        for k in range(blocks):
            unpair(rc, kc, WB + 8 * k, e_ref, FB + 16 * k, nc)
        prolong_pass(e_ref, f_ref, 0, 2 * blocks, fine, WB, 0, 2 * blocks, plan, True)

    whole_up(r7, k7, 1, 1, k6, ((0, 0),))
    post(r6, k6, g6, c6, WB, 2, 1)
    whole_up(r6, k6, 2, 1, k5, ((0, 0), (0, 1)))
    post(r5, k5, g5, c5, WB, 4, 2)
    whole_up(r5, k5, 4, 2, k4, ((0, 0), (0, 1), (1, 0), (1, 1)))
    post(r4, k4, g4, c4, WB, 8, 4)

    def block(ref, da, wanted, at):
        b = lax.rem(me_a + da + NA, NA)
        x = ref[b // 2, at, :]
        return jnp.where(b % 2 == wanted, x, pltpu.roll(x, 64, 1))

    for k in range(2):
        at = pl.ds(WB - 4 + 4 * me_r + 8 * k, 8)
        seen = []
        for ref in (r4, k4):
            mine, rightward, leftward = block(ref, 0, 0, at), block(ref, 1, 1, at), block(ref, -1, 1, at)
            seen.append(jnp.where(lane < 64, mine, jnp.where(lane < 96, rightward, leftward)))
        q = FB - 8 + 16 * k
        win[0, pl.ds(q, 8, stride=2), :] = jnp.where(even, seen[0], seen[1])
        win[0, pl.ds(q + 1, 8, stride=2), :] = jnp.where(even, seen[1], seen[0])

    for copy in back3:
        copy.wait()
    for q in range(3):
        got = lambda dr, da: bs3[DIRS.index((-dr, -da)), q]
        x3[q, 0, pl.ds(BASE[3] - 8, 8), :] = got(-1, 0)
        x3[q, 0, pl.ds(BASE[3] + 8, 8), :] = got(1, 0)
        for dr in (-1, 0, 1):
            x3[q, 1, pl.ds(BASE[3] + 8 * dr, 8), :] = jnp.where(lane < 64, got(dr, 1), got(dr, -1))
    prolong_pass(win, f_ref, -8, 3, k3, BASE[3], -8, 3, ((0, 0), (0, 1)), False)
    clear_outside((k3, g3.at[0], g3.at[1]), 3, 2)
    post(r3, k3, g3, c3, BASE[3] - 8, 3, 2)

    for k in range(2):
        unpair(r3, k3, BASE[3] - 4 + 8 * k, e_ref, FB - 8 + 16 * k, 2)
    prolong_pass(e_ref, f_ref, -8, 4, k2, BASE[2], -4, 3, ((0, 0), (0, 1), (1, 2)), False)
    clear_outside((k2,), 2, 3)
    post(r2, k2, g2, c2, BASE[2] - 4, 3, 3)

    for k in range(3):
        unpair(r2, k2, BASE[2] - 4 + 8 * k, e_ref, FB - 8 + 16 * k, 3)
    prolong_pass(e_ref, f_ref, -8, 6, k1, BASE[1], -4, 5, ((0, 0), (0, 1), (1, 0), (1, 1), (2, 2)), False)
    clear_outside((k1,), 1, 5)
    post(r1, k1, g1, c1, BASE[1] - 4, 5, 5)

    for k in range(5):
        unpair(r1, k1, BASE[1] - 4 + 8 * k, e_ref, FB - 8 + 16 * k, 5)
    plan = tuple((t // 2, t % 2) for t in range(8)) + ((4, 2),)
    prolong_pass(e_ref, f_ref, -8, 10, k0, BASE[0], -4, 9, plan, False)
    clear_outside((k0,), 0, 9)
    post(r0, k0, g0, c0, 4, 9, 9)

    outs = []

    def write(slot, hbm):
        for t in range(8):
            copy = pltpu.make_async_copy(raw.at[slot, t], hbm.at[:, pl.ds(128 * t, 128)], out_sem.at[slot, t])
            copy.start()
            outs.append(copy)

    for k in range(8):
        unpair(r0, k0, BASE[0] + 8 * k, raw.at[0], 16 * k, 8)
    write(0, sol_hbm)
    residual_pass(s0, r0, k0, g0.at[0], c0, 0, BASE[0], 8, 9, out_tiles=8)
    residual_pass(g0.at[0], k0, r0, g0.at[1], c0, 1, BASE[0], 8, 9, out_tiles=8)
    for k in range(8):
        unpair(s0, g0.at[0], BASE[0] + 8 * k, raw.at[1], 16 * k, 8)
    write(1, res_hbm)
    for copy in outs:
        copy.wait()


def local(right_side, guess):
    def vm(*shape):
        return pltpu.VMEM(shape, F32)

    levels = [vm(2, 8, 128, 128), vm(3, 9, ROWS[0], 128), vm(9, ROWS[0], 128), vm(9, ROWS[0], 128)]
    for l in (1, 2):
        n = OWN[l][1] + 1
        levels += [vm(2, n, ROWS[l], 128)] + [vm(n, ROWS[l], 128)] * 3
    levels += [vm(3, 2, ROWS[3], 128), vm(2, ROWS[3], 128), vm(2, ROWS[3], 128)]
    for l, (pairs, tiles) in enumerate(WHOLE):
        levels += [vm(2, tiles, pairs + 2 * WB, 128)] + [vm(tiles, pairs + 2 * WB, 128)] * (2 if l == 3 else 3)
    coefficients = [vm(10, r, 128) for r in ROWS] + [vm(10, pairs + 2 * WB, 128) for pairs, _ in WHOLE]
    buffers = [
        vm(2, 3, 8, 128), vm(2, 3, 8, 128), vm(4, 3, 8, 128),
        vm(2, 2, 32, 128), vm(4, 2, 24, 128),
        vm(8, 3, 8, 128), vm(8, 128), vm(NA - 1, 8, 128), vm(2, 4, 8, 128),
    ]
    dma = pltpu.SemaphoreType.DMA
    sems = [dma((2, 8)), dma((2, 8))] + [dma((8,))] * 6 + [dma((NA - 1,))] * 2 + [dma((NB - 1,))] * 2
    natural = [vm(1, 48, 128), vm(5, 96, 128), vm(9, 96, 128), vm(4, 64, 128)]
    block = jax.ShapeDtypeStruct(right_side.shape, F32)
    return pl.pallas_call(
        kernel,
        out_shape=(block, block),
        in_specs=[pl.BlockSpec(memory_space=pl.ANY)] * 2,
        out_specs=(pl.BlockSpec(memory_space=pl.ANY),) * 2,
        scratch_shapes=levels + natural + coefficients + buffers + sems,
        compiler_params=pltpu.CompilerParams(collective_id=0, has_side_effects=True),
    )(right_side, guess)


def solution(mesh):
    placed = (P("rad", "ang"), P("rad", "ang"))
    return jax.shard_map(local, mesh=mesh, in_specs=placed, out_specs=placed, check_vma=False)
```

```python
import math

import jax
import jax.numpy as jnp
from jax import lax
from jax.experimental import pallas as pl
from jax.experimental.pallas import tpu as pltpu
from jax.sharding import PartitionSpec as P

MESH = pl.DeviceIdType.MESH
F32 = jnp.float32
NR, NT = 2048, 8192
NA, NB = 8, 16
OWN = ((64, 8), (32, 4), (16, 2), (8, 1))
BASE = (8, 24, 16, 16)
ROWS = tuple(o[0] + 2 * b for o, b in zip(OWN, BASE))
E0, E1 = 5, 18
WHOLE = ((64, 4), (32, 2), (16, 1), (8, 1))
WB = 8
DIRS = tuple((dr, da) for dr in (-1, 0, 1) for da in (-1, 0, 1) if dr or da)
CORNERS = tuple(d for d in DIRS if d[0] and d[1])
FB = 16


def grid_ids():
    sub = lax.broadcasted_iota(jnp.int32, (8, 128), 0)
    lane = lax.broadcasted_iota(jnp.int32, (8, 128), 1)
    return sub, lane


def ring_shift(tiles, lane):
    n = len(tiles)
    one = [pltpu.roll(x, 1, 1) for x in tiles]
    back = [pltpu.roll(x, 127, 1) for x in tiles]
    if n == 1:
        return one, back
    left = [jnp.where(lane == 0, one[t - 1], one[t]) for t in range(n)]
    right = [jnp.where(lane == 127, back[(t + 1) % n], back[t]) for t in range(n)]
    return left, right


def pick(x, index):
    return jnp.take_along_axis(x, index, axis=1, mode="promise_in_bounds")


def fill_coefficients(c_ref, count, base, first_row, total_rows, cells):
    h = 2.0 * math.pi / cells
    sub, lane = grid_ids()
    even = lane % 2 == 0

    def row_values(row):
        inside = jnp.logical_and(row >= 0, row < total_rows)
        r = 1.0 + (row.astype(F32) + 0.5) * h
        rr = r * r
        q = jnp.where(inside, 0.5 / (rr + 1.0), 0.0)
        half = (0.5 * h) * r
        return (rr + half) * q, (rr - half) * q, q, rr * q, 2.0 + 2.0 / rr

    for k in range(count):
        row = first_row + 2 * (8 * k - base + sub)
        o0, i0, a0, w0, c0 = row_values(row)
        o1, i1, a1, w1, c1 = row_values(row + 1)
        at = pl.ds(8 * k, 8)
        for j, (x, y) in enumerate(((o0, i1), (i0, o1), (a0, a1), (w0, w1), (c0, c1))):
            c_ref[j, at, :] = jnp.where(even, x, y)
            c_ref[5 + j, at, :] = jnp.where(even, y, x)


def relaxed(src, g, c_ref, colour, p, n, lane):
    at = pl.ds(p, 8)
    even = lane % 2 == 0
    first, second = (p - 1, p + 1) if colour == 0 else (p + 1, p - 1)
    x = [src[t, at, :] for t in range(n)]
    left, right = ring_shift(x, lane)
    near, far, ang = (c_ref[5 * colour + k, at, :] for k in range(3))
    return [
        (g[t, at, :] + near * x[t])
        + (far * jnp.where(even, src[t, pl.ds(first, 8), :], src[t, pl.ds(second, 8), :]) + ang * (left[t] + right[t]))
        for t in range(n)
    ]


def half_sweep(dst, src, g, c_ref, colour, start, count, n):
    _, lane = grid_ids()
    for k in range(count):
        p = start + 8 * k
        new = relaxed(src, g, c_ref, colour, p, n, lane)
        for t in range(n):
            dst[t, pl.ds(p, 8), :] = new[t]


def residual_pass(dst, old, src, g, c_ref, colour, start, count, n, out_tiles=None):
    _, lane = grid_ids()
    for k in range(count):
        p = start + 8 * k
        new = relaxed(src, g, c_ref, colour, p, n, lane)
        c = c_ref[5 * colour + 4, pl.ds(p, 8), :]
        for t in range(out_tiles or n):
            dst[t, pl.ds(p, 8), :] = c * (new[t] - old[t, pl.ds(p, 8), :])


def fence(step):
    pl.when(lax.axis_index("rad") < NB)(step)


def joined_block(s, p, n, pairs, lane):
    even = lane % 2 == 0
    r = [
        3.0 * s[t, pl.ds(p, 8), :] + jnp.where(even, s[t, pl.ds(p + 1, 8), :], s[t, pl.ds(p - 1, 8), :])
        for t in range(n)
    ]
    left, right = ring_shift(r, lane)
    m = [3.0 * r[t] + jnp.where(even, left[t], right[t]) for t in range(n)]
    return [
        jnp.where(even, m[a] + pltpu.roll(m[a], 127, 1), m[b] + pltpu.roll(m[b], 1, 1))
        for a, b in pairs
    ]


def gathered(x, lane):
    return pick(x, jnp.where(lane < 64, 2 * lane, 2 * lane - 127)) * 0.0625


def restrict_pass(s, fine_base, n, nat, g, coarse_base, c_ref, start, count, pairs):
    _, lane = grid_ids()
    even = lane % 2 == 0
    for k in range(2 * count):
        for t, x in enumerate(joined_block(s, fine_base + 2 * start + 8 * k, n, pairs, lane)):
            nat[t, pl.ds(8 * k, 8), :] = x

    def gathers():
        for k in range(2 * count):
            for t in range(len(pairs)):
                nat[t, pl.ds(8 * k, 8), :] = gathered(nat[t, pl.ds(8 * k, 8), :], lane)

    fence(gathers)
    for k in range(count):
        p = pl.ds(coarse_base + start + 8 * k, 8)
        red, black = c_ref[3, p, :], c_ref[8, p, :]
        for t in range(len(pairs)):
            x = nat[t, pl.ds(16 * k, 8, stride=2), :]
            y = nat[t, pl.ds(16 * k + 1, 8, stride=2), :]
            g[0, t, p, :] = jnp.where(even, x, y) * red
            g[1, t, p, :] = jnp.where(even, y, x) * black


def unpair(red, black, p, dst, q, n):
    _, lane = grid_ids()
    even = lane % 2 == 0
    for t in range(n):
        x, y = red[t, pl.ds(p, 8), :], black[t, pl.ds(p, 8), :]
        dst[t, pl.ds(q, 8, stride=2), :] = jnp.where(even, x, y)
        dst[t, pl.ds(q + 1, 8, stride=2), :] = jnp.where(even, y, x)


def prolong_pass(e, f, fb, start, count, fine, fine_base, fine_start, fine_count, plan, sealed):
    _, lane = grid_ids()
    even = lane % 2 == 0
    half = lane // 2
    nc = max(source for source, _ in plan) + 1

    def arranged(x, kind):
        if kind == 0:
            return x
        turned = pltpu.roll(x, 64, 1)
        return turned if kind == 1 else jnp.where(lane < 32, x, turned)

    for k in range(count):
        p = FB + start + 8 * k
        x = [e[t, pl.ds(p, 8), :] for t in range(nc)]
        left, right = ring_shift(x, lane)
        for t, (source, kind) in enumerate(plan):
            f[t, pl.ds(p, 8), :] = arranged(0.75 * x[source] + 0.25 * left[source], kind)
            fb[t, pl.ds(p, 8), :] = arranged(0.75 * x[source] + 0.25 * right[source], kind)

    def gathers():
        for k in range(count):
            at = pl.ds(FB + start + 8 * k, 8)
            for t in range(len(plan)):
                f[t, at, :] = jnp.where(even, pick(f[t, at, :], half), pick(fb[t, at, :], half))

    fence(gathers)
    if sealed:
        for t in range(len(plan)):
            f[t, pl.ds(FB - 8, 8), :] = jnp.zeros((8, 128), F32)
            f[t, pl.ds(FB + 8 * count, 8), :] = jnp.zeros((8, 128), F32)
    for k in range(fine_count):
        i = fine_start + 8 * k
        at = pl.ds(fine_base + i, 8)
        for t in range(len(plan)):
            other = jnp.where(even, f[t, pl.ds(FB + i + 1, 8), :], f[t, pl.ds(FB + i - 1, 8), :])
            fine[t, at, :] = fine[t, at, :] + (0.75 * f[t, pl.ds(FB + i, 8), :] + 0.25 * other)


def zero_rows(ref, n, start, count):
    for t in range(n):
        for k in range(count):
            ref[t, pl.ds(start + 8 * k, 8), :] = jnp.zeros((8, 128), F32)


def down(r, k, g, s, c, start, count, n):
    half_sweep(k, g.at[0], g.at[1], c, 1, start, count, n)
    half_sweep(r, k, g.at[0], c, 0, start, count, n)
    half_sweep(k, r, g.at[1], c, 1, start, count, n)
    residual_pass(s, r, k, g.at[0], c, 0, start, count, n)


def post(r, k, g, c, start, count, n):
    for _ in range(2):
        half_sweep(r, k, g.at[0], c, 0, start, count, n)
        half_sweep(k, r, g.at[1], c, 1, start, count, n)


def kernel(
    right_hbm, guess_hbm, x0, c0,
    raw, r0, s0, g1, r1, k1, s1, g2, r2, k2, s2, x3, r3, s3,
    g4, r4, k4, s4, g5, r5, k5, s5, g6, r6, k6, s6, g7, r7, k7,
    win, e_ref, f_ref, fb_ref, nat, c1, c2, c3, c4, c5, c6, c7,
    pk0, rp0, rd0, rl1, rd1, bs3, own4, slots, strip,
    load_sem, send0, recv0, send1, recv1, sendc, recvc, senda, recva, sendg, recvg,
):
    me_a, me_r = lax.axis_index("ang"), lax.axis_index("rad")

    def device(dr, da):
        return {"ang": lax.rem(me_a + da + NA, NA), "rad": lax.rem(me_r + dr + NB, NB)}

    barrier = pltpu.get_barrier_semaphore()
    partners = list(DIRS) + [(0, d) for d in range(2, NA - 1)] + [(d, 0) for d in range(2, NB - 1)]
    for dr, da in partners:
        pl.semaphore_signal(barrier, inc=1, device_id=device(dr, da), device_id_type=MESH)

    loads = []
    for t in range(8):
        for k, src in ((0, guess_hbm), (1, right_hbm)):
            loads.append(pltpu.make_async_copy(
                src.at[:, pl.ds(128 * t, 128)], raw.at[k, t], load_sem.at[k, t]))
    for copy in loads:
        copy.start()

    zero = jnp.zeros((8, 128), F32)
    k0, g0 = x0.at[0], x0.at[pl.ds(1, 2)]
    k3, g3 = x3.at[0], x3.at[pl.ds(1, 2)]
    edges = [(r, 0) for r in (r0, s0)] + [(r, 1) for r in (r1, k1, s1)]
    edges += [(r, 2) for r in (g2.at[0], g2.at[1], r2, k2, s2)]
    edges += [(r, 3) for r in (k3, x3.at[1], x3.at[2], r3, s3)]
    for ref, l in edges:
        depth = 1 if l < 2 else 2
        for t in range(OWN[l][1] + 1):
            for d in range(depth):
                ref[t, pl.ds(8 * d, 8), :] = zero
                ref[t, pl.ds(ROWS[l] - 8 - 8 * d, 8), :] = zero
    for l, refs in enumerate(((g4, r4, k4, s4), (g5, r5, k5, s5), (g6, r6, k6, s6), (g7, r7, k7))):
        for ref in refs:
            for x in ((ref.at[0], ref.at[1]) if len(ref.shape) == 4 else (ref,)):
                for t in range(WHOLE[l][1]):
                    x[t, pl.ds(0, 8), :] = zero
                    x[t, pl.ds(WB + WHOLE[l][0], 8), :] = zero
    zero_rows(win, 1, 0, 6)
    for t in range(9):
        for d in (0, 1, 10, 11):
            f_ref[t, pl.ds(8 * d, 8), :] = zero
    for l, c_ref in enumerate((c0, c1, c2, c3)):
        fill_coefficients(c_ref, ROWS[l] // 8, BASE[l], me_r * (2 * OWN[l][0]), NR >> l, NT >> l)
    for l, c_ref in enumerate((c4, c5, c6, c7)):
        fill_coefficients(c_ref, WHOLE[l][0] // 8 + 2, WB, 0, 2 * WHOLE[l][0], NT >> (l + 4))

    sub, lane = grid_ids()
    even = lane % 2 == 0

    def remote(src, dst, sems, recvs, k, dr, da):
        return pltpu.make_async_remote_copy(
            src_ref=src, dst_ref=dst, send_sem=sems.at[k], recv_sem=recvs.at[k],
            device_id=device(dr, da), device_id_type=MESH)

    def edge(l, dr, width):
        if dr < 0:
            return pl.ds(BASE[l], width), pl.ds(BASE[l] + OWN[l][0], width)
        return pl.ds(BASE[l] + OWN[l][0] - width, width), pl.ds(BASE[l] - width, width)

    for copy in loads:
        copy.wait()
    for k in range(8):
        at = pl.ds(BASE[0] + 8 * k, 8)
        red, black = c0[3, at, :], c0[8, at, :]
        for t in range(8):
            k0[t, at, :] = jnp.where(
                even, raw[0, t, pl.ds(16 * k + 1, 8, stride=2), :], raw[0, t, pl.ds(16 * k, 8, stride=2), :])
            x = raw[1, t, pl.ds(16 * k, 8, stride=2), :]
            y = raw[1, t, pl.ds(16 * k + 1, 8, stride=2), :]
            g0[0, t, at, :] = jnp.where(even, x, y) * red
            g0[1, t, at, :] = jnp.where(even, y, x) * black
    for q in range(3):
        for side, (tile, first) in enumerate(((0, 0), (7, 112))):
            total = None
            for b in range(8):
                x = x0[q, tile, pl.ds(BASE[0] + 8 * b, 8), :]
                shift = (16 * b - first) % 128
                x = pltpu.roll(x, shift, 1) if shift else x
                total = x if total is None else jnp.where(lane // 16 == b, x, total)
            pk0[side, q, :, :] = total
    pl.semaphore_wait(barrier, len(partners))

    sends = []
    for k, (dr, da) in enumerate(DIRS):
        if da == 0:
            mine, theirs = edge(0, dr, E0)
            copy = remote(x0.at[:, pl.ds(0, 8), mine, :], x0.at[:, pl.ds(0, 8), theirs, :], send0, recv0, k, dr, da)
        elif dr == 0:
            side = 0 if da < 0 else 1
            copy = remote(pk0.at[side], rp0.at[side], send0, recv0, k, dr, da)
        else:
            mine, _ = edge(0, dr, E0)
            tile = 0 if da < 0 else 7
            copy = remote(
                x0.at[:, tile, mine, :], rd0.at[CORNERS.index((dr, da)), :, pl.ds(0, E0), :], send0, recv0, k, dr, da)
        copy.start()
        sends.append(copy)
    for copy in sends:
        copy.wait()

    def clear_outside(refs, l, n, depth=1):
        @pl.when(me_r == 0)
        def _():
            for ref in refs:
                zero_rows(ref, n, BASE[l] - 8 * depth, depth)

        @pl.when(me_r == NB - 1)
        def _():
            for ref in refs:
                zero_rows(ref, n, BASE[l] + OWN[l][0], depth)

    for q in range(3):
        from_left, from_right = rp0[1, q], rp0[0, q]
        for b in range(8):
            shift_r, shift_l = (-16 * b) % 128, (112 - 16 * b) % 128
            x = pltpu.roll(from_right, shift_r, 1) if shift_r else from_right
            y = pltpu.roll(from_left, shift_l, 1) if shift_l else from_left
            x0[q, 8, pl.ds(BASE[0] + 8 * b, 8), :] = jnp.where(lane < 64, x, y)
        for dr in (-1, 1):
            start = BASE[0] - E0 if dr < 0 else BASE[0] + OWN[0][0]
            x = rd0[CORNERS.index((-dr, -1)), q, pl.ds(0, E0), :]
            y = rd0[CORNERS.index((-dr, 1)), q, pl.ds(0, E0), :]
            x0[q, 8, pl.ds(start, E0), :] = jnp.where(lane[:E0] < 64, x, y)
    clear_outside((k0, g0.at[0], g0.at[1]), 0, 9)

    for _ in range(2):
        half_sweep(r0, k0, g0.at[0], c0, 0, 4, 9, 9)
        half_sweep(k0, r0, g0.at[1], c0, 1, 4, 9, 9)
    residual_pass(s0, r0, k0, g0.at[0], c0, 0, 4, 9, 9)
    restrict_pass(s0, BASE[0], 9, nat, g1, BASE[1], c1, 0, 4, ((0, 1), (2, 3), (4, 5), (6, 7)))

    sends = []
    for k, (dr, da) in enumerate(DIRS):
        tile = 0 if da < 0 else 3
        mine, theirs = edge(1, dr, E1) if dr else (pl.ds(BASE[1], 32), None)
        if da == 0:
            copy = remote(g1.at[:, pl.ds(0, 4), mine, :], g1.at[:, pl.ds(0, 4), theirs, :], send1, recv1, k, dr, da)
        elif dr == 0:
            copy = remote(g1.at[:, tile, mine, :], rl1.at[0 if da < 0 else 1], send1, recv1, k, dr, da)
        else:
            copy = remote(
                g1.at[:, tile, mine, :], rd1.at[CORNERS.index((dr, da)), :, pl.ds(0, E1), :], send1, recv1, k, dr, da)
        copy.start()
        sends.append(copy)
    for copy in sends:
        copy.wait()
    for q in range(2):
        for b in range(4):
            g1[q, 4, pl.ds(BASE[1] + 8 * b, 8), :] = jnp.where(
                lane < 64, rl1[0, q, pl.ds(8 * b, 8), :], rl1[1, q, pl.ds(8 * b, 8), :])
        for dr in (-1, 1):
            start = BASE[1] - E1 if dr < 0 else BASE[1] + OWN[1][0]
            for first, size in ((0, 8), (8, 8), (16, 2)):
                x = rd1[CORNERS.index((-dr, -1)), q, pl.ds(first, size), :]
                y = rd1[CORNERS.index((-dr, 1)), q, pl.ds(first, size), :]
                g1[q, 4, pl.ds(start + first, size), :] = jnp.where(lane[:size] < 64, x, y)
            rest = BASE[1] - E1 - 3 if dr < 0 else BASE[1] + OWN[1][0] + E1
            for t in range(5):
                g1[q, t, pl.ds(rest, 3), :] = jnp.zeros((3, 128), F32)
    clear_outside((g1.at[0], g1.at[1]), 1, 5, 3)

    down(r1, k1, g1, s1, c1, BASE[1] - 20, 9, 5)
    restrict_pass(s1, BASE[1], 5, nat, g2, BASE[2], c2, -8, 4, ((0, 1), (2, 3), (4, 4)))
    down(r2, k2, g2, s2, c2, BASE[2] - 8, 4, 3)
    restrict_pass(s2, BASE[2], 3, nat, g3, BASE[3], c3, -4, 2, ((0, 1), (2, 2)))
    down(r3, k3, g3, s3, c3, BASE[3] - 4, 2, 2)

    nat[0, pl.ds(0, 8), :] = gathered(joined_block(s3, BASE[3], 2, ((0, 0),), lane)[0], lane)
    x, y = nat[0, pl.ds(0, 4, stride=2), :], nat[0, pl.ds(1, 4, stride=2), :]
    my_pairs = pl.ds(WB + 4 * me_r, 4)
    own4[pl.ds(0, 4), :] = jnp.where(even[:4], x, y) * c4[3, my_pairs, :]
    own4[pl.ds(4, 4), :] = jnp.where(even[:4], y, x) * c4[8, my_pairs, :]
    ring = []
    for d in range(1, NA):
        copy = remote(own4, slots.at[d - 1], senda, recva, d - 1, 0, d)
        copy.start()
        ring.append(copy)
    back3 = []
    for k, (dr, da) in enumerate(DIRS):
        copy = remote(x3.at[:, 0, pl.ds(BASE[3], 8), :], bs3.at[k], sendc, recvc, k, dr, da)
        copy.start()
        back3.append(copy)
    for copy in ring:
        copy.wait()
    for t in range(4):
        total = own4[...]
        for d in range(1, NA):
            source = lax.rem(me_a - d + NA, NA)
            hit = jnp.logical_and(source // 2 == t, lane // 64 == source % 2)
            total = jnp.where(hit, slots[d - 1], total)
        for q in range(2):
            strip[q, t, pl.ds(0, 4), :] = total[4 * q:4 * q + 4]
            g4[q, t, my_pairs, :] = total[4 * q:4 * q + 4]
    column = []
    for d in range(1, NB):
        copy = remote(strip.at[:, :, pl.ds(0, 4), :], g4.at[:, :, my_pairs, :], sendg, recvg, d - 1, d, 0)
        copy.start()
        column.append(copy)
    for copy in column:
        copy.wait()

    down(r4, k4, g4, s4, c4, WB, 8, 4)
    restrict_pass(s4, WB, 4, nat, g5, WB, c5, 0, 4, ((0, 1), (2, 3)))
    down(r5, k5, g5, s5, c5, WB, 4, 2)
    restrict_pass(s5, WB, 2, nat, g6, WB, c6, 0, 2, ((0, 1),))
    down(r6, k6, g6, s6, c6, WB, 2, 1)
    restrict_pass(s6, WB, 1, nat, g7, WB, c7, 0, 1, ((0, 0),))
    half_sweep(k7, g7.at[0], g7.at[1], c7, 1, WB, 1, 1)
    for _ in range(7):
        half_sweep(r7, k7, g7.at[0], c7, 0, WB, 1, 1)
        half_sweep(k7, r7, g7.at[1], c7, 1, WB, 1, 1)

    def whole_up(rc, kc, blocks, nc, fine, plan):
        for k in range(blocks):
            unpair(rc, kc, WB + 8 * k, e_ref, FB + 16 * k, nc)
        prolong_pass(e_ref, f_ref, fb_ref, 0, 2 * blocks, fine, WB, 0, 2 * blocks, plan, True)

    whole_up(r7, k7, 1, 1, k6, ((0, 0),))
    post(r6, k6, g6, c6, WB, 2, 1)
    whole_up(r6, k6, 2, 1, k5, ((0, 0), (0, 1)))
    post(r5, k5, g5, c5, WB, 4, 2)
    whole_up(r5, k5, 4, 2, k4, ((0, 0), (0, 1), (1, 0), (1, 1)))
    post(r4, k4, g4, c4, WB, 8, 4)

    def block(ref, da, wanted, at):
        b = lax.rem(me_a + da + NA, NA)
        x = ref[b // 2, at, :]
        return jnp.where(b % 2 == wanted, x, pltpu.roll(x, 64, 1))

    for k in range(2):
        at = pl.ds(WB - 4 + 4 * me_r + 8 * k, 8)
        seen = []
        for ref in (r4, k4):
            mine, rightward, leftward = block(ref, 0, 0, at), block(ref, 1, 1, at), block(ref, -1, 1, at)
            seen.append(jnp.where(lane < 64, mine, jnp.where(lane < 96, rightward, leftward)))
        q = FB - 8 + 16 * k
        win[0, pl.ds(q, 8, stride=2), :] = jnp.where(even, seen[0], seen[1])
        win[0, pl.ds(q + 1, 8, stride=2), :] = jnp.where(even, seen[1], seen[0])

    for copy in back3:
        copy.wait()
    for q in range(3):
        got = lambda dr, da: bs3[DIRS.index((-dr, -da)), q]
        x3[q, 0, pl.ds(BASE[3] - 8, 8), :] = got(-1, 0)
        x3[q, 0, pl.ds(BASE[3] + 8, 8), :] = got(1, 0)
        for dr in (-1, 0, 1):
            x3[q, 1, pl.ds(BASE[3] + 8 * dr, 8), :] = jnp.where(lane < 64, got(dr, 1), got(dr, -1))
    prolong_pass(win, f_ref, fb_ref, -8, 3, k3, BASE[3], -8, 3, ((0, 0), (0, 1)), False)
    clear_outside((k3, g3.at[0], g3.at[1]), 3, 2)
    post(r3, k3, g3, c3, BASE[3] - 8, 3, 2)

    for k in range(2):
        unpair(r3, k3, BASE[3] - 4 + 8 * k, e_ref, FB - 8 + 16 * k, 2)
    prolong_pass(e_ref, f_ref, fb_ref, -8, 4, k2, BASE[2], -4, 3, ((0, 0), (0, 1), (1, 2)), False)
    clear_outside((k2,), 2, 3)
    post(r2, k2, g2, c2, BASE[2] - 4, 3, 3)

    for k in range(3):
        unpair(r2, k2, BASE[2] - 4 + 8 * k, e_ref, FB - 8 + 16 * k, 3)
    prolong_pass(e_ref, f_ref, fb_ref, -8, 6, k1, BASE[1], -4, 5, ((0, 0), (0, 1), (1, 0), (1, 1), (2, 2)), False)
    clear_outside((k1,), 1, 5)
    post(r1, k1, g1, c1, BASE[1] - 4, 5, 5)

    for k in range(5):
        unpair(r1, k1, BASE[1] - 4 + 8 * k, e_ref, FB - 8 + 16 * k, 5)
    plan = tuple((t // 2, t % 2) for t in range(8)) + ((4, 2),)
    prolong_pass(e_ref, f_ref, fb_ref, -8, 10, k0, BASE[0], -4, 9, plan, False)
    clear_outside((k0,), 0, 9)


def finish(x0, c0, sol_hbm, res_hbm, r, k, s, b, raw, out_sem):
    zero = jnp.zeros((8, 128), F32)
    for ref in (r, k):
        for t in range(9):
            ref[t, pl.ds(0, 8), :] = zero
            ref[t, pl.ds(ROWS[0] - 8, 8), :] = zero
    start, gr, gk = x0.at[0], x0.at[1], x0.at[2]
    half_sweep(r, start, gr, c0, 0, 4, 9, 9)
    half_sweep(k, r, gk, c0, 1, 4, 9, 9)
    half_sweep(r, k, gr, c0, 0, 4, 9, 9)
    half_sweep(k, r, gk, c0, 1, 4, 9, 9)
    outs = []

    def write(slot, red, black, hbm):
        for t in range(8):
            for q in range(8):
                unpair(red.at[pl.ds(t, 1)], black.at[pl.ds(t, 1)], BASE[0] + 8 * q, raw.at[slot, pl.ds(t, 1)], 16 * q, 1)
            copy = pltpu.make_async_copy(raw.at[slot, t], hbm.at[:, pl.ds(128 * t, 128)], out_sem.at[slot, t])
            copy.start()
            outs.append(copy)

    write(0, r, k, sol_hbm)
    residual_pass(s, r, k, gr, c0, 0, BASE[0], 8, 9, out_tiles=8)
    residual_pass(b, k, r, gk, c0, 1, BASE[0], 8, 9, out_tiles=8)
    write(1, s, b, res_hbm)
    for copy in outs:
        copy.wait()


def local(right_side, guess):
    def vm(*shape):
        return pltpu.VMEM(shape, F32)

    levels = [vm(2, 8, 128, 128), vm(9, ROWS[0], 128), vm(9, ROWS[0], 128)]
    for l in (1, 2):
        n = OWN[l][1] + 1
        levels += [vm(2, n, ROWS[l], 128)] + [vm(n, ROWS[l], 128)] * 3
    levels += [vm(3, 2, ROWS[3], 128), vm(2, ROWS[3], 128), vm(2, ROWS[3], 128)]
    for l, (pairs, tiles) in enumerate(WHOLE):
        levels += [vm(2, tiles, pairs + 2 * WB, 128)] + [vm(tiles, pairs + 2 * WB, 128)] * (2 if l == 3 else 3)
    coefficients = [vm(10, r, 128) for r in ROWS[1:]] + [vm(10, pairs + 2 * WB, 128) for pairs, _ in WHOLE]
    buffers = [
        vm(2, 3, 8, 128), vm(2, 3, 8, 128), vm(4, 3, 8, 128),
        vm(2, 2, 32, 128), vm(4, 2, 24, 128),
        vm(8, 3, 8, 128), vm(8, 128), vm(NA - 1, 8, 128), vm(2, 4, 8, 128),
    ]
    dma = pltpu.SemaphoreType.DMA
    sems = [dma((2, 8))] + [dma((8,))] * 6 + [dma((NA - 1,))] * 2 + [dma((NB - 1,))] * 2
    natural = [vm(1, 48, 128), vm(5, 96, 128), vm(9, 96, 128), vm(9, 96, 128), vm(4, 64, 128)]
    held = (vm(3, 9, ROWS[0], 128), vm(10, ROWS[0], 128))
    inside = pl.BlockSpec(memory_space=pltpu.VMEM)
    outside = pl.BlockSpec(memory_space=pl.ANY)
    x0, c0 = pl.pallas_call(
        kernel,
        out_shape=held,
        in_specs=[outside] * 2,
        out_specs=(inside,) * 2,
        scratch_shapes=levels + natural + coefficients + buffers + sems,
        compiler_params=pltpu.CompilerParams(collective_id=0, has_side_effects=True),
    )(right_side, guess)
    x0, c0 = (pltpu.with_memory_space_constraint(x, pltpu.VMEM) for x in (x0, c0))
    block = jax.ShapeDtypeStruct(right_side.shape, F32)
    return pl.pallas_call(
        finish,
        out_shape=(block, block),
        in_specs=[inside] * 2,
        out_specs=(outside,) * 2,
        scratch_shapes=[vm(9, ROWS[0], 128)] * 4 + [vm(2, 8, 128, 128), dma((2, 8))],
    )(x0, c0)


def solution(mesh):
    placed = (P("rad", "ang"), P("rad", "ang"))
    return jax.shard_map(local, mesh=mesh, in_specs=placed, out_specs=placed, check_vma=False)
```

```python
import math

import jax
import jax.numpy as jnp
from jax import lax
from jax.experimental import pallas as pl
from jax.experimental.pallas import tpu as pltpu
from jax.sharding import PartitionSpec as P

MESH = pl.DeviceIdType.MESH
F32 = jnp.float32
NR, NT = 2048, 8192
NA, NB = 8, 16
OWN = ((64, 8), (32, 4), (16, 2), (8, 1))
BASE = (8, 24, 16, 16)
ROWS = tuple(o[0] + 2 * b for o, b in zip(OWN, BASE))
E0, E1 = 5, 18
WHOLE = ((64, 4), (32, 2), (16, 1), (8, 1))
WB = 8
DIRS = tuple((dr, da) for dr in (-1, 0, 1) for da in (-1, 0, 1) if dr or da)
CORNERS = tuple(d for d in DIRS if d[0] and d[1])
ORDER = tuple(sorted(DIRS, key=lambda d: (d[1] != 0, d[0] == 0)))
FB = 16


def grid_ids():
    sub = lax.broadcasted_iota(jnp.int32, (8, 128), 0)
    lane = lax.broadcasted_iota(jnp.int32, (8, 128), 1)
    return sub, lane


def ring_shift(tiles, lane):
    n = len(tiles)
    one = [pltpu.roll(x, 1, 1) for x in tiles]
    back = [pltpu.roll(x, 127, 1) for x in tiles]
    if n == 1:
        return one, back
    left = [jnp.where(lane == 0, one[t - 1], one[t]) for t in range(n)]
    right = [jnp.where(lane == 127, back[(t + 1) % n], back[t]) for t in range(n)]
    return left, right


def pick(x, index):
    return jnp.take_along_axis(x, index, axis=1, mode="promise_in_bounds")


def fill_coefficients(c_ref, count, base, first_row, total_rows, cells):
    h = 2.0 * math.pi / cells
    sub, lane = grid_ids()
    even = lane % 2 == 0

    def row_values(row):
        inside = jnp.logical_and(row >= 0, row < total_rows)
        r = 1.0 + (row.astype(F32) + 0.5) * h
        rr = r * r
        q = jnp.where(inside, 0.5 / (rr + 1.0), 0.0)
        half = (0.5 * h) * r
        return (rr + half) * q, (rr - half) * q, q, rr * q, 2.0 + 2.0 / rr

    for k in range(count):
        row = first_row + 2 * (8 * k - base + sub)
        o0, i0, a0, w0, c0 = row_values(row)
        o1, i1, a1, w1, c1 = row_values(row + 1)
        at = pl.ds(8 * k, 8)
        for j, (x, y) in enumerate(((o0, i1), (i0, o1), (a0, a1), (w0, w1), (c0, c1))):
            c_ref[j, at, :] = jnp.where(even, x, y)
            c_ref[5 + j, at, :] = jnp.where(even, y, x)


def relaxed(src, g, c_ref, colour, p, n, lane):
    at = pl.ds(p, 8)
    even = lane % 2 == 0
    first, second = (p - 1, p + 1) if colour == 0 else (p + 1, p - 1)
    x = [src[t, at, :] for t in range(n)]
    left, right = ring_shift(x, lane)
    near, far, ang = (c_ref[5 * colour + k, at, :] for k in range(3))
    return [
        (g[t, at, :] + near * x[t])
        + (far * jnp.where(even, src[t, pl.ds(first, 8), :], src[t, pl.ds(second, 8), :]) + ang * (left[t] + right[t]))
        for t in range(n)
    ]


def half_sweep(dst, src, g, c_ref, colour, start, count, n):
    _, lane = grid_ids()
    for k in range(count):
        p = start + 8 * k
        new = relaxed(src, g, c_ref, colour, p, n, lane)
        for t in range(n):
            dst[t, pl.ds(p, 8), :] = new[t]


def residual_pass(dst, old, src, g, c_ref, colour, start, count, n, out_tiles=None):
    _, lane = grid_ids()
    for k in range(count):
        p = start + 8 * k
        new = relaxed(src, g, c_ref, colour, p, n, lane)
        c = c_ref[5 * colour + 4, pl.ds(p, 8), :]
        for t in range(out_tiles or n):
            dst[t, pl.ds(p, 8), :] = c * (new[t] - old[t, pl.ds(p, 8), :])


def fence(step):
    pl.when(lax.axis_index("rad") < NB)(step)


def joined_block(s, p, n, pairs, lane):
    even = lane % 2 == 0
    r = [
        3.0 * s[t, pl.ds(p, 8), :] + jnp.where(even, s[t, pl.ds(p + 1, 8), :], s[t, pl.ds(p - 1, 8), :])
        for t in range(n)
    ]
    left, right = ring_shift(r, lane)
    m = [3.0 * r[t] + jnp.where(even, left[t], right[t]) for t in range(n)]
    return [
        jnp.where(even, m[a] + pltpu.roll(m[a], 127, 1), m[b] + pltpu.roll(m[b], 1, 1))
        for a, b in pairs
    ]


def gathered(x, lane):
    return pick(x, jnp.where(lane < 64, 2 * lane, 2 * lane - 127)) * 0.0625


def restrict_pass(s, fine_base, n, nat, g, coarse_base, c_ref, start, count, pairs):
    _, lane = grid_ids()
    even = lane % 2 == 0
    for k in range(2 * count):
        for t, x in enumerate(joined_block(s, fine_base + 2 * start + 8 * k, n, pairs, lane)):
            nat[t, pl.ds(8 * k, 8), :] = x

    def gathers():
        for k in range(2 * count):
            for t in range(len(pairs)):
                nat[t, pl.ds(8 * k, 8), :] = gathered(nat[t, pl.ds(8 * k, 8), :], lane)

    fence(gathers)
    for k in range(count):
        p = pl.ds(coarse_base + start + 8 * k, 8)
        red, black = c_ref[3, p, :], c_ref[8, p, :]
        for t in range(len(pairs)):
            x = nat[t, pl.ds(16 * k, 8, stride=2), :]
            y = nat[t, pl.ds(16 * k + 1, 8, stride=2), :]
            g[0, t, p, :] = jnp.where(even, x, y) * red
            g[1, t, p, :] = jnp.where(even, y, x) * black


def unpair(red, black, p, dst, q, n):
    _, lane = grid_ids()
    even = lane % 2 == 0
    for t in range(n):
        x, y = red[t, pl.ds(p, 8), :], black[t, pl.ds(p, 8), :]
        dst[t, pl.ds(q, 8, stride=2), :] = jnp.where(even, x, y)
        dst[t, pl.ds(q + 1, 8, stride=2), :] = jnp.where(even, y, x)


def prolong_pass(e, f, fb, start, count, fine, fine_base, fine_start, fine_count, plan, sealed):
    _, lane = grid_ids()
    even = lane % 2 == 0
    half = lane // 2
    nc = max(source for source, _ in plan) + 1

    def arranged(x, kind):
        if kind == 0:
            return x
        turned = pltpu.roll(x, 64, 1)
        return turned if kind == 1 else jnp.where(lane < 32, x, turned)

    for k in range(count):
        p = FB + start + 8 * k
        x = [e[t, pl.ds(p, 8), :] for t in range(nc)]
        left, right = ring_shift(x, lane)
        for t, (source, kind) in enumerate(plan):
            f[t, pl.ds(p, 8), :] = arranged(0.75 * x[source] + 0.25 * left[source], kind)
            fb[t, pl.ds(p, 8), :] = arranged(0.75 * x[source] + 0.25 * right[source], kind)

    def gathers():
        for k in range(count):
            at = pl.ds(FB + start + 8 * k, 8)
            for t in range(len(plan)):
                f[t, at, :] = jnp.where(even, pick(f[t, at, :], half), pick(fb[t, at, :], half))

    fence(gathers)
    if sealed:
        for t in range(len(plan)):
            f[t, pl.ds(FB - 8, 8), :] = jnp.zeros((8, 128), F32)
            f[t, pl.ds(FB + 8 * count, 8), :] = jnp.zeros((8, 128), F32)
    for k in range(fine_count):
        i = fine_start + 8 * k
        at = pl.ds(fine_base + i, 8)
        for t in range(len(plan)):
            other = jnp.where(even, f[t, pl.ds(FB + i + 1, 8), :], f[t, pl.ds(FB + i - 1, 8), :])
            fine[t, at, :] = fine[t, at, :] + (0.75 * f[t, pl.ds(FB + i, 8), :] + 0.25 * other)


def wait_bytes(ref, *sems):
    for sem in sems:
        pltpu.make_async_copy(ref, ref, sem).wait()


def zero_rows(ref, n, start, count):
    for t in range(n):
        for k in range(count):
            ref[t, pl.ds(start + 8 * k, 8), :] = jnp.zeros((8, 128), F32)


def down(r, k, g, s, c, start, count, n):
    half_sweep(k, g.at[0], g.at[1], c, 1, start, count, n)
    half_sweep(r, k, g.at[0], c, 0, start, count, n)
    half_sweep(k, r, g.at[1], c, 1, start, count, n)
    residual_pass(s, r, k, g.at[0], c, 0, start, count, n)


def post(r, k, g, c, start, count, n):
    for _ in range(2):
        half_sweep(r, k, g.at[0], c, 0, start, count, n)
        half_sweep(k, r, g.at[1], c, 1, start, count, n)


def spread(blocks, reach):
    return {d: [pltpu.roll(x, -d % 128, 1) if d else x for x in blocks] for d in range(-reach, reach + 1)}


def weights(c_ref, count):
    return [
        [tuple(c_ref[5 * colour + k, pl.ds(WB + 8 * b, 8), :] for k in range(3)) for b in range(count)]
        for colour in range(2)
    ]


def relaxed_spread(src, g, w, colour, reach):
    sub, lane = grid_ids()
    even = lane % 2 == 0
    out = {}
    for d in range(-reach, reach + 1):
        kind = (colour + d) % 2
        x = src[d]
        one = [pltpu.roll(y, 1, 0) for y in x]
        back = [pltpu.roll(y, 7, 0) for y in x]
        n = len(x)
        out[d] = []
        for b in range(n):
            before = jnp.where(sub == 0, one[b - 1] if b else 0.0, one[b])
            after = jnp.where(sub == 7, back[b + 1] if b < n - 1 else 0.0, back[b])
            near, far, ang = w[kind][b]
            other = jnp.where(even, before, after) if kind == 0 else jnp.where(even, after, before)
            out[d].append((g[d][b] + near * x[b]) + (far * other + ang * (src[d - 1][b] + src[d + 1][b])))
    return out


def read(ref, count):
    return [ref[0, pl.ds(WB + 8 * b, 8), :] for b in range(count)]


def put(ref, blocks):
    for b, x in enumerate(blocks):
        ref[0, pl.ds(WB + 8 * b, 8), :] = x


def kernel(
    right_hbm, guess_hbm, x0, c0,
    raw, r0, s0, g1, r1, k1, s1, g2, r2, k2, s2, x3, r3, s3,
    g4, r4, k4, s4, g5, r5, k5, s5, g6, r6, k6, s6, g7, r7, k7,
    win, e_ref, f_ref, fb_ref, nat, c1, c2, c3, c4, c5, c6, c7,
    pk0, rp0, rd0, pk1, rl1, rd1, bs3, own4, slots, strip,
    load_sem, send0, recv0, send1, recv1, sendc, recvc, senda, recva, sendg, recvg,
):
    me_a, me_r = lax.axis_index("ang"), lax.axis_index("rad")

    def device(dr, da):
        return {"ang": lax.rem(me_a + da + NA, NA), "rad": lax.rem(me_r + dr + NB, NB)}

    barrier = pltpu.get_barrier_semaphore()
    partners = list(DIRS) + [(0, d) for d in range(2, NA - 1)] + [(d, 0) for d in range(2, NB - 1)]
    for dr, da in partners:
        pl.semaphore_signal(barrier, inc=1, device_id=device(dr, da), device_id_type=MESH)

    loads = []
    for t in range(8):
        for k, src in ((0, guess_hbm), (1, right_hbm)):
            loads.append(pltpu.make_async_copy(
                src.at[:, pl.ds(128 * t, 128)], raw.at[k, t], load_sem))
    for copy in loads:
        copy.start()

    zero = jnp.zeros((8, 128), F32)
    k0, g0 = x0.at[0], x0.at[pl.ds(1, 2)]
    k3, g3 = x3.at[0], x3.at[pl.ds(1, 2)]
    edges = [(r, 0) for r in (r0, s0)] + [(r, 1) for r in (r1, k1, s1)]
    edges += [(r, 2) for r in (g2.at[0], g2.at[1], r2, k2, s2)]
    edges += [(r, 3) for r in (k3, x3.at[1], x3.at[2], r3, s3)]
    for ref, l in edges:
        depth = 1 if l < 2 else 2
        for t in range(OWN[l][1] + 1):
            for d in range(depth):
                ref[t, pl.ds(8 * d, 8), :] = zero
                ref[t, pl.ds(ROWS[l] - 8 - 8 * d, 8), :] = zero
    for l, refs in enumerate(((g4, r4, k4, s4), (g5, r5, k5, s5), (g6, r6, k6, s6), (g7, r7, k7))):
        for ref in refs:
            for x in ((ref.at[0], ref.at[1]) if len(ref.shape) == 4 else (ref,)):
                for t in range(WHOLE[l][1]):
                    x[t, pl.ds(0, 8), :] = zero
                    x[t, pl.ds(WB + WHOLE[l][0], 8), :] = zero
    zero_rows(win, 1, 0, 6)
    for t in range(9):
        for d in (0, 1, 10, 11):
            f_ref[t, pl.ds(8 * d, 8), :] = zero
    for l, c_ref in enumerate((c0, c1, c2, c3)):
        fill_coefficients(c_ref, ROWS[l] // 8, BASE[l], me_r * (2 * OWN[l][0]), NR >> l, NT >> l)
    for l, c_ref in enumerate((c4, c5, c6, c7)):
        fill_coefficients(c_ref, WHOLE[l][0] // 8 + 2, WB, 0, 2 * WHOLE[l][0], NT >> (l + 4))

    sub, lane = grid_ids()
    even = lane % 2 == 0

    def send(src, dst, send_sem, recv_sem, dr, da):
        pltpu.make_async_remote_copy(
            src_ref=src, dst_ref=dst, send_sem=send_sem, recv_sem=recv_sem,
            device_id=device(dr, da), device_id_type=MESH).start()

    def edge(l, dr, width):
        if dr < 0:
            return pl.ds(BASE[l], width), pl.ds(BASE[l] + OWN[l][0], width)
        return pl.ds(BASE[l] + OWN[l][0] - width, width), pl.ds(BASE[l] - width, width)

    wait_bytes(raw, load_sem)
    for k in range(8):
        at = pl.ds(BASE[0] + 8 * k, 8)
        red, black = c0[3, at, :], c0[8, at, :]
        for t in range(8):
            k0[t, at, :] = jnp.where(
                even, raw[0, t, pl.ds(16 * k + 1, 8, stride=2), :], raw[0, t, pl.ds(16 * k, 8, stride=2), :])
            x = raw[1, t, pl.ds(16 * k, 8, stride=2), :]
            y = raw[1, t, pl.ds(16 * k + 1, 8, stride=2), :]
            g0[0, t, at, :] = jnp.where(even, x, y) * red
            g0[1, t, at, :] = jnp.where(even, y, x) * black
    for q in range(3):
        for side, (tile, first) in enumerate(((0, 0), (7, 112))):
            total = None
            for b in range(8):
                x = x0[q, tile, pl.ds(BASE[0] + 8 * b, 8), :]
                shift = (16 * b - first) % 128
                x = pltpu.roll(x, shift, 1) if shift else x
                total = x if total is None else jnp.where(lane // 16 == b, x, total)
            pk0[side, q, :, :] = total
    pl.semaphore_wait(barrier, len(partners))

    for dr, da in ORDER:
        mine, theirs = edge(0, dr, E0) if dr else (None, None)
        if da == 0:
            send(x0.at[0, pl.ds(0, 8), mine, :], x0.at[0, pl.ds(0, 8), theirs, :], send0, recv0, dr, da)
            mine, theirs = edge(0, dr, 4)
            send(x0.at[pl.ds(1, 2), pl.ds(0, 8), mine, :], x0.at[pl.ds(1, 2), pl.ds(0, 8), theirs, :],
                 send0, recv0, dr, da)
        elif dr == 0:
            side = 0 if da < 0 else 1
            send(pk0.at[side], rp0.at[side], send0, recv0, dr, da)
        else:
            tile = 0 if da < 0 else 7
            send(x0.at[:, tile, mine, :], rd0.at[CORNERS.index((dr, da)), :, pl.ds(0, E0), :], send0, recv0, dr, da)
    wait_bytes(f_ref.at[pl.ds(0, 4), pl.ds(0, 79), :], send0, recv0)

    def clear_outside(refs, l, n, depth=1):
        @pl.when(me_r == 0)
        def _():
            for ref in refs:
                zero_rows(ref, n, BASE[l] - 8 * depth, depth)

        @pl.when(me_r == NB - 1)
        def _():
            for ref in refs:
                zero_rows(ref, n, BASE[l] + OWN[l][0], depth)

    for q in range(3):
        from_left, from_right = rp0[1, q], rp0[0, q]
        for b in range(8):
            shift_r, shift_l = (-16 * b) % 128, (112 - 16 * b) % 128
            x = pltpu.roll(from_right, shift_r, 1) if shift_r else from_right
            y = pltpu.roll(from_left, shift_l, 1) if shift_l else from_left
            x0[q, 8, pl.ds(BASE[0] + 8 * b, 8), :] = jnp.where(lane < 64, x, y)
        for dr in (-1, 1):
            start = BASE[0] - E0 if dr < 0 else BASE[0] + OWN[0][0]
            x = rd0[CORNERS.index((-dr, -1)), q, pl.ds(0, E0), :]
            y = rd0[CORNERS.index((-dr, 1)), q, pl.ds(0, E0), :]
            x0[q, 8, pl.ds(start, E0), :] = jnp.where(lane[:E0] < 64, x, y)
    clear_outside((k0, g0.at[0], g0.at[1]), 0, 9)

    for _ in range(2):
        half_sweep(r0, k0, g0.at[0], c0, 0, 4, 9, 9)
        half_sweep(k0, r0, g0.at[1], c0, 1, 4, 9, 9)
    residual_pass(s0, r0, k0, g0.at[0], c0, 0, 4, 9, 9)
    restrict_pass(s0, BASE[0], 9, nat, g1, BASE[1], c1, 0, 4, ((0, 1), (2, 3), (4, 5), (6, 7)))

    for b in range(4):
        at, own = pl.ds(8 * b, 8), pl.ds(BASE[1] + 8 * b, 8)
        pk1[0, at, :] = jnp.where(lane < 64, g1[0, 0, own, :], pltpu.roll(g1[1, 0, own, :], 64, 1))
        pk1[1, at, :] = jnp.where(lane < 64, pltpu.roll(g1[0, 3, own, :], 64, 1), g1[1, 3, own, :])
    for dr, da in ORDER:
        side = 0 if da < 0 else 1
        if da == 0:
            mine, theirs = edge(1, dr, E1)
            send(g1.at[:, pl.ds(0, 4), mine, :], g1.at[:, pl.ds(0, 4), theirs, :], send1, recv1, dr, da)
        elif dr == 0:
            send(pk1.at[side], rl1.at[side], send1, recv1, dr, da)
        else:
            send(pk1.at[side, pl.ds(0 if dr < 0 else 32 - E1, E1), :],
                 rd1.at[CORNERS.index((dr, da)), pl.ds(0, E1), :], send1, recv1, dr, da)
    wait_bytes(f_ref.at[pl.ds(0, 8), pl.ds(0, 53), :], send1, recv1)

    def merge_edges(row, size, from_right, from_left):
        low = lane[:size] < 64
        g1[0, 4, pl.ds(row, size), :] = jnp.where(low, from_right, pltpu.roll(from_left, 64, 1))
        g1[1, 4, pl.ds(row, size), :] = jnp.where(low, pltpu.roll(from_right, 64, 1), from_left)

    for b in range(4):
        merge_edges(BASE[1] + 8 * b, 8, rl1[0, pl.ds(8 * b, 8), :], rl1[1, pl.ds(8 * b, 8), :])
    for dr in (-1, 1):
        start = BASE[1] - E1 if dr < 0 else BASE[1] + OWN[1][0]
        right, left = CORNERS.index((-dr, -1)), CORNERS.index((-dr, 1))
        for first in (0, 8, 16):
            size = 8 if first < 16 else 2
            merge_edges(start + first, size, rd1[right, pl.ds(first, size), :], rd1[left, pl.ds(first, size), :])
    for q in range(2):
        for dr in (-1, 1):
            rest = BASE[1] - E1 - 3 if dr < 0 else BASE[1] + OWN[1][0] + E1
            for t in range(5):
                g1[q, t, pl.ds(rest, 3), :] = jnp.zeros((3, 128), F32)
    clear_outside((g1.at[0], g1.at[1]), 1, 5, 3)

    down(r1, k1, g1, s1, c1, BASE[1] - 20, 9, 5)
    restrict_pass(s1, BASE[1], 5, nat, g2, BASE[2], c2, -8, 4, ((0, 1), (2, 3), (4, 4)))
    down(r2, k2, g2, s2, c2, BASE[2] - 8, 4, 3)
    restrict_pass(s2, BASE[2], 3, nat, g3, BASE[3], c3, -4, 2, ((0, 1), (2, 2)))
    down(r3, k3, g3, s3, c3, BASE[3] - 4, 2, 2)

    nat[0, pl.ds(0, 8), :] = gathered(joined_block(s3, BASE[3], 2, ((0, 0),), lane)[0], lane)
    x, y = nat[0, pl.ds(0, 4, stride=2), :], nat[0, pl.ds(1, 4, stride=2), :]
    my_pairs = pl.ds(WB + 4 * me_r, 4)
    own4[pl.ds(0, 4), :] = jnp.where(even[:4], x, y) * c4[3, my_pairs, :]
    own4[pl.ds(4, 4), :] = jnp.where(even[:4], y, x) * c4[8, my_pairs, :]
    for d in range(1, NA):
        send(own4, slots.at[d - 1], senda, recva, 0, d)
    wait_bytes(slots, senda, recva)
    for t in range(4):
        total = own4[...]
        for d in range(1, NA):
            source = lax.rem(me_a - d + NA, NA)
            hit = jnp.logical_and(source // 2 == t, lane // 64 == source % 2)
            total = jnp.where(hit, slots[d - 1], total)
        for q in range(2):
            strip[q, t, pl.ds(0, 4), :] = total[4 * q:4 * q + 4]
            g4[q, t, my_pairs, :] = total[4 * q:4 * q + 4]
    for d in range(1, NB):
        send(strip.at[:, :, pl.ds(0, 4), :], g4.at[:, :, my_pairs, :], sendg, recvg, d, 0)
    for k, (dr, da) in enumerate(DIRS):
        send(x3.at[:, 0, pl.ds(BASE[3], 8), :], bs3.at[k], sendc, recvc, dr, da)
    wait_bytes(g4.at[:, :, pl.ds(WB, 60), :], sendg, recvg)

    down(r4, k4, g4, s4, c4, WB, 8, 4)
    restrict_pass(s4, WB, 4, nat, g5, WB, c5, 0, 4, ((0, 1), (2, 3)))
    down(r5, k5, g5, s5, c5, WB, 4, 2)
    restrict_pass(s5, WB, 2, nat, g6, WB, c6, 0, 2, ((0, 1),))
    gr6, gk6, w6 = spread(read(g6.at[0], 2), 4), spread(read(g6.at[1], 2), 3), weights(c6, 2)
    black = relaxed_spread(gr6, gk6, w6, 1, 3)
    red = relaxed_spread(black, gr6, w6, 0, 2)
    black = relaxed_spread(red, gk6, w6, 1, 1)
    put(k6, black[0])
    new = relaxed_spread(black, gr6, w6, 0, 0)[0]
    put(s6, [c6[4, pl.ds(WB + 8 * b, 8), :] * (new[b] - red[0][b]) for b in range(2)])
    restrict_pass(s6, WB, 1, nat, g7, WB, c7, 0, 1, ((0, 0),))
    gr7, gk7, w7 = spread(read(g7.at[0], 1), 4), spread(read(g7.at[1], 1), 3), weights(c7, 1)
    source = gr7
    for step in range(4):
        black = relaxed_spread(source, gk7, w7, 1, 3 if step < 3 else 2)
        red = relaxed_spread(black, gr7, w7, 0, 2 if step < 3 else 1)
        black = relaxed_spread(red, gk7, w7, 1, 1 if step < 3 else 0)
        if step < 3:
            source = spread(relaxed_spread(black, gr7, w7, 0, 0)[0], 4)
    put(r7, red[0])
    put(k7, black[0])

    def whole_up(rc, kc, blocks, nc, fine, plan):
        for k in range(blocks):
            unpair(rc, kc, WB + 8 * k, e_ref, FB + 16 * k, nc)
        prolong_pass(e_ref, f_ref, fb_ref, 0, 2 * blocks, fine, WB, 0, 2 * blocks, plan, True)

    whole_up(r7, k7, 1, 1, k6, ((0, 0),))
    red = relaxed_spread(spread(read(k6, 2), 4), gr6, w6, 0, 3)
    black = relaxed_spread(red, gk6, w6, 1, 2)
    red = relaxed_spread(black, gr6, w6, 0, 1)
    put(r6, red[0])
    put(k6, relaxed_spread(red, gk6, w6, 1, 0)[0])
    whole_up(r6, k6, 2, 1, k5, ((0, 0), (0, 1)))
    post(r5, k5, g5, c5, WB, 4, 2)
    whole_up(r5, k5, 4, 2, k4, ((0, 0), (0, 1), (1, 0), (1, 1)))
    post(r4, k4, g4, c4, WB, 8, 4)

    def block(ref, da, wanted, at):
        b = lax.rem(me_a + da + NA, NA)
        x = ref[b // 2, at, :]
        return jnp.where(b % 2 == wanted, x, pltpu.roll(x, 64, 1))

    for k in range(2):
        at = pl.ds(WB - 4 + 4 * me_r + 8 * k, 8)
        seen = []
        for ref in (r4, k4):
            mine, rightward, leftward = block(ref, 0, 0, at), block(ref, 1, 1, at), block(ref, -1, 1, at)
            seen.append(jnp.where(lane < 64, mine, jnp.where(lane < 96, rightward, leftward)))
        q = FB - 8 + 16 * k
        win[0, pl.ds(q, 8, stride=2), :] = jnp.where(even, seen[0], seen[1])
        win[0, pl.ds(q + 1, 8, stride=2), :] = jnp.where(even, seen[1], seen[0])

    wait_bytes(bs3, sendc, recvc)
    for q in range(3):
        got = lambda dr, da: bs3[DIRS.index((-dr, -da)), q]
        x3[q, 0, pl.ds(BASE[3] - 8, 8), :] = got(-1, 0)
        x3[q, 0, pl.ds(BASE[3] + 8, 8), :] = got(1, 0)
        for dr in (-1, 0, 1):
            x3[q, 1, pl.ds(BASE[3] + 8 * dr, 8), :] = jnp.where(lane < 64, got(dr, 1), got(dr, -1))
    prolong_pass(win, f_ref, fb_ref, -8, 3, k3, BASE[3], -8, 3, ((0, 0), (0, 1)), False)
    clear_outside((k3, g3.at[0], g3.at[1]), 3, 2)
    post(r3, k3, g3, c3, BASE[3] - 8, 3, 2)

    for k in range(2):
        unpair(r3, k3, BASE[3] - 4 + 8 * k, e_ref, FB - 8 + 16 * k, 2)
    prolong_pass(e_ref, f_ref, fb_ref, -8, 4, k2, BASE[2], -4, 3, ((0, 0), (0, 1), (1, 2)), False)
    clear_outside((k2,), 2, 3)
    post(r2, k2, g2, c2, BASE[2] - 4, 3, 3)

    for k in range(3):
        unpair(r2, k2, BASE[2] - 4 + 8 * k, e_ref, FB - 8 + 16 * k, 3)
    prolong_pass(e_ref, f_ref, fb_ref, -8, 6, k1, BASE[1], -4, 5, ((0, 0), (0, 1), (1, 0), (1, 1), (2, 2)), False)
    clear_outside((k1,), 1, 5)
    post(r1, k1, g1, c1, BASE[1] - 4, 5, 5)

    for k in range(5):
        unpair(r1, k1, BASE[1] - 4 + 8 * k, e_ref, FB - 8 + 16 * k, 5)
    plan = tuple((t // 2, t % 2) for t in range(8)) + ((4, 2),)
    prolong_pass(e_ref, f_ref, fb_ref, -8, 10, k0, BASE[0], -4, 9, plan, False)
    clear_outside((k0,), 0, 9)


def finish(x0, c0, sol_hbm, res_hbm, r, k, s, b, raw, out_sem):
    zero = jnp.zeros((8, 128), F32)
    for ref in (r, k):
        for t in range(9):
            ref[t, pl.ds(0, 8), :] = zero
            ref[t, pl.ds(ROWS[0] - 8, 8), :] = zero
    start, gr, gk = x0.at[0], x0.at[1], x0.at[2]
    half_sweep(r, start, gr, c0, 0, 4, 9, 9)
    half_sweep(k, r, gk, c0, 1, 4, 9, 9)
    half_sweep(r, k, gr, c0, 0, 4, 9, 9)
    half_sweep(k, r, gk, c0, 1, 4, 9, 9)

    def write(slot, red, black, hbm):
        for t in range(8):
            for q in range(8):
                unpair(red.at[pl.ds(t, 1)], black.at[pl.ds(t, 1)], BASE[0] + 8 * q, raw.at[slot, pl.ds(t, 1)], 16 * q, 1)
            copy = pltpu.make_async_copy(raw.at[slot, t], hbm.at[:, pl.ds(128 * t, 128)], out_sem)
            copy.start()

    write(0, r, k, sol_hbm)
    residual_pass(s, r, k, gr, c0, 0, BASE[0], 8, 9, out_tiles=8)
    residual_pass(b, k, r, gk, c0, 1, BASE[0], 8, 9, out_tiles=8)
    write(1, s, b, res_hbm)
    wait_bytes(raw, out_sem)


def local(right_side, guess):
    def vm(*shape):
        return pltpu.VMEM(shape, F32)

    levels = [vm(2, 8, 128, 128), vm(9, ROWS[0], 128), vm(9, ROWS[0], 128)]
    for l in (1, 2):
        n = OWN[l][1] + 1
        levels += [vm(2, n, ROWS[l], 128)] + [vm(n, ROWS[l], 128)] * 3
    levels += [vm(3, 2, ROWS[3], 128), vm(2, ROWS[3], 128), vm(2, ROWS[3], 128)]
    for l, (pairs, tiles) in enumerate(WHOLE):
        levels += [vm(2, tiles, pairs + 2 * WB, 128)] + [vm(tiles, pairs + 2 * WB, 128)] * (2 if l == 3 else 3)
    coefficients = [vm(10, r, 128) for r in ROWS[1:]] + [vm(10, pairs + 2 * WB, 128) for pairs, _ in WHOLE]
    buffers = [
        vm(2, 3, 8, 128), vm(2, 3, 8, 128), vm(4, 3, 8, 128),
        vm(2, 32, 128), vm(2, 32, 128), vm(4, 24, 128),
        vm(8, 3, 8, 128), vm(8, 128), vm(NA - 1, 8, 128), vm(2, 4, 8, 128),
    ]
    dma = pltpu.SemaphoreType.DMA
    sems = [dma] * 11
    natural = [vm(1, 48, 128), vm(5, 96, 128), vm(9, 96, 128), vm(9, 96, 128), vm(4, 64, 128)]
    held = (vm(3, 9, ROWS[0], 128), vm(10, ROWS[0], 128))
    inside = pl.BlockSpec(memory_space=pltpu.VMEM)
    outside = pl.BlockSpec(memory_space=pl.ANY)
    x0, c0 = pl.pallas_call(
        kernel,
        out_shape=held,
        in_specs=[outside] * 2,
        out_specs=(inside,) * 2,
        scratch_shapes=levels + natural + coefficients + buffers + sems,
        compiler_params=pltpu.CompilerParams(collective_id=0, has_side_effects=True),
    )(right_side, guess)
    x0, c0 = (pltpu.with_memory_space_constraint(x, pltpu.VMEM) for x in (x0, c0))
    block = jax.ShapeDtypeStruct(right_side.shape, F32)
    return pl.pallas_call(
        finish,
        out_shape=(block, block),
        in_specs=[inside] * 2,
        out_specs=(outside,) * 2,
        scratch_shapes=[vm(9, ROWS[0], 128)] * 4 + [vm(2, 8, 128, 128), dma],
    )(x0, c0)


def solution(mesh):
    placed = (P("rad", "ang"), P("rad", "ang"))
    return jax.shard_map(local, mesh=mesh, in_specs=placed, out_specs=placed, check_vma=False)
```

```python
import math

import jax
import jax.numpy as jnp
from jax import lax
from jax.experimental import pallas as pl
from jax.experimental.pallas import tpu as pltpu
from jax.sharding import PartitionSpec as P

MESH = pl.DeviceIdType.MESH
F32 = jnp.float32
NR, NT = 2048, 8192
NA, NB = 8, 16
OWN = ((64, 8), (32, 4), (16, 2), (8, 1))
BASE = (8, 24, 16, 16)
ROWS = tuple(o[0] + 2 * b for o, b in zip(OWN, BASE))
E0, E1 = 5, 18
WHOLE = ((64, 4), (32, 2), (16, 1), (8, 1))
WB = 8
DIRS = tuple((dr, da) for dr in (-1, 0, 1) for da in (-1, 0, 1) if dr or da)
CORNERS = tuple(d for d in DIRS if d[0] and d[1])
ORDER = tuple(sorted(DIRS, key=lambda d: (d[1] != 0, d[0] == 0)))
FB = 16


def grid_ids():
    sub = lax.broadcasted_iota(jnp.int32, (8, 128), 0)
    lane = lax.broadcasted_iota(jnp.int32, (8, 128), 1)
    return sub, lane


def ring_shift(tiles, lane):
    n = len(tiles)
    one = [pltpu.roll(x, 1, 1) for x in tiles]
    back = [pltpu.roll(x, 127, 1) for x in tiles]
    if n == 1:
        return one, back
    left = [jnp.where(lane == 0, one[t - 1], one[t]) for t in range(n)]
    right = [jnp.where(lane == 127, back[(t + 1) % n], back[t]) for t in range(n)]
    return left, right


def pick(x, index):
    return jnp.take_along_axis(x, index, axis=1, mode="promise_in_bounds")


def fill_coefficients(c_ref, count, base, first_row, total_rows, cells):
    h = 2.0 * math.pi / cells
    sub, lane = grid_ids()
    even = lane % 2 == 0

    def row_values(row):
        inside = jnp.logical_and(row >= 0, row < total_rows)
        r = 1.0 + (row.astype(F32) + 0.5) * h
        rr = r * r
        q = jnp.where(inside, 0.5 / (rr + 1.0), 0.0)
        half = (0.5 * h) * r
        return (rr + half) * q, (rr - half) * q, q, rr * q, 2.0 + 2.0 / rr

    for k in range(count):
        row = first_row + 2 * (8 * k - base + sub)
        o0, i0, a0, w0, c0 = row_values(row)
        o1, i1, a1, w1, c1 = row_values(row + 1)
        at = pl.ds(8 * k, 8)
        for j, (x, y) in enumerate(((o0, i1), (i0, o1), (a0, a1), (w0, w1), (c0, c1))):
            c_ref[j, at, :] = jnp.where(even, x, y)
            c_ref[5 + j, at, :] = jnp.where(even, y, x)


def relaxed(src, g, c_ref, colour, p, n, lane, tiles):
    at = pl.ds(p, 8)
    even = lane % 2 == 0
    first, second = (p - 1, p + 1) if colour == 0 else (p + 1, p - 1)
    x = {t: src[t, at, :] for t in sorted({(u + d) % n for u in tiles for d in (-1, 0, 1)})}
    one = {t: pltpu.roll(x[t], 1, 1) for t in sorted({(u + d) % n for u in tiles for d in (-1, 0)})}
    back = {t: pltpu.roll(x[t], 127, 1) for t in sorted({(u + d) % n for u in tiles for d in (0, 1)})}
    near, far, ang = (c_ref[5 * colour + k, at, :] for k in range(3))
    new = {}
    for t in tiles:
        left, right = one[t], back[t]
        if n > 1:
            left = jnp.where(lane == 0, one[(t - 1) % n], left)
            right = jnp.where(lane == 127, back[(t + 1) % n], right)
        other = jnp.where(even, src[t, pl.ds(first, 8), :], src[t, pl.ds(second, 8), :])
        new[t] = (g[t, at, :] + near * x[t]) + (far * other + ang * (left + right))
    return new


def half_sweep(dst, src, g, c_ref, colour, start, count, n, tiles=None):
    _, lane = grid_ids()
    for k in range(count):
        p = start + 8 * k
        for t, value in relaxed(src, g, c_ref, colour, p, n, lane, tiles or range(n)).items():
            dst[t, pl.ds(p, 8), :] = value


def residual_pass(dst, old, src, g, c_ref, colour, start, count, n, tiles=None):
    _, lane = grid_ids()
    for k in range(count):
        p = start + 8 * k
        c = c_ref[5 * colour + 4, pl.ds(p, 8), :]
        for t, value in relaxed(src, g, c_ref, colour, p, n, lane, tiles or range(n)).items():
            dst[t, pl.ds(p, 8), :] = c * (value - old[t, pl.ds(p, 8), :])


def fence(step):
    pl.when(lax.axis_index("rad") < NB)(step)


def mixed_block(s, p, n, lane):
    even = lane % 2 == 0
    r = [
        3.0 * s[t, pl.ds(p, 8), :] + jnp.where(even, s[t, pl.ds(p + 1, 8), :], s[t, pl.ds(p - 1, 8), :])
        for t in range(n)
    ]
    left, right = ring_shift(r, lane)
    return [3.0 * r[t] + jnp.where(even, left[t], right[t]) for t in range(n)]


def joined(a, b, lane):
    return jnp.where(lane % 2 == 0, a + pltpu.roll(a, 127, 1), b + pltpu.roll(b, 1, 1))


def gathered(x, lane):
    return pick(x, jnp.where(lane < 64, 2 * lane, 2 * lane - 127)) * 0.0625


def restrict_pass(s, fine_base, n, mix, nat, g, coarse_base, c_ref, start, count, pairs):
    _, lane = grid_ids()
    even = lane % 2 == 0
    for k in range(2 * count):
        for t, x in enumerate(mixed_block(s, fine_base + 2 * start + 8 * k, n, lane)):
            mix[t, pl.ds(8 * k, 8), :] = x

    def joins():
        for k in range(2 * count):
            at = pl.ds(8 * k, 8)
            for t, (a, b) in enumerate(pairs):
                nat[t, at, :] = joined(mix[a, at, :], mix[b, at, :], lane)

    fence(joins)

    def gathers():
        for k in range(2 * count):
            for t in range(len(pairs)):
                nat[t, pl.ds(8 * k, 8), :] = gathered(nat[t, pl.ds(8 * k, 8), :], lane)

    fence(gathers)
    for k in range(count):
        p = pl.ds(coarse_base + start + 8 * k, 8)
        red, black = c_ref[3, p, :], c_ref[8, p, :]
        for t in range(len(pairs)):
            x = nat[t, pl.ds(16 * k, 8, stride=2), :]
            y = nat[t, pl.ds(16 * k + 1, 8, stride=2), :]
            g[0, t, p, :] = jnp.where(even, x, y) * red
            g[1, t, p, :] = jnp.where(even, y, x) * black


def unpair(red, black, p, dst, q, n):
    _, lane = grid_ids()
    even = lane % 2 == 0
    for t in range(n):
        x, y = red[t, pl.ds(p, 8), :], black[t, pl.ds(p, 8), :]
        dst[t, pl.ds(q, 8, stride=2), :] = jnp.where(even, x, y)
        dst[t, pl.ds(q + 1, 8, stride=2), :] = jnp.where(even, y, x)


def prolong_pass(e, f, fb, start, count, fine, fine_base, fine_start, fine_count, plan, sealed):
    _, lane = grid_ids()
    even = lane % 2 == 0
    half = lane // 2
    nc = max(source for source, _ in plan) + 1

    def arranged(x, kind):
        if kind == 0:
            return x
        turned = pltpu.roll(x, 64, 1)
        return turned if kind == 1 else jnp.where(lane < 32, x, turned)

    for k in range(count):
        p = FB + start + 8 * k
        x = [e[t, pl.ds(p, 8), :] for t in range(nc)]
        left, right = ring_shift(x, lane)
        for t, (source, kind) in enumerate(plan):
            f[t, pl.ds(p, 8), :] = arranged(0.75 * x[source] + 0.25 * left[source], kind)
            fb[t, pl.ds(p, 8), :] = arranged(0.75 * x[source] + 0.25 * right[source], kind)

    def gathers():
        for k in range(count):
            at = pl.ds(FB + start + 8 * k, 8)
            for t in range(len(plan)):
                f[t, at, :] = jnp.where(even, pick(f[t, at, :], half), pick(fb[t, at, :], half))

    fence(gathers)
    if sealed:
        for t in range(len(plan)):
            f[t, pl.ds(FB - 8, 8), :] = jnp.zeros((8, 128), F32)
            f[t, pl.ds(FB + 8 * count, 8), :] = jnp.zeros((8, 128), F32)
    for k in range(fine_count):
        i = fine_start + 8 * k
        at = pl.ds(fine_base + i, 8)
        for t in range(len(plan)):
            other = jnp.where(even, f[t, pl.ds(FB + i + 1, 8), :], f[t, pl.ds(FB + i - 1, 8), :])
            fine[t, at, :] = fine[t, at, :] + (0.75 * f[t, pl.ds(FB + i, 8), :] + 0.25 * other)


def wait_bytes(ref, *sems):
    for sem in sems:
        pltpu.make_async_copy(ref, ref, sem).wait()


def zero_rows(ref, n, start, count):
    for t in range(n):
        for k in range(count):
            ref[t, pl.ds(start + 8 * k, 8), :] = jnp.zeros((8, 128), F32)


def down(r, k, g, s, c, start, count, n):
    half_sweep(k, g.at[0], g.at[1], c, 1, start, count, n)
    half_sweep(r, k, g.at[0], c, 0, start, count, n)
    half_sweep(k, r, g.at[1], c, 1, start, count, n)
    residual_pass(s, r, k, g.at[0], c, 0, start, count, n)


def post(r, k, g, c, start, count, n):
    for _ in range(2):
        half_sweep(r, k, g.at[0], c, 0, start, count, n)
        half_sweep(k, r, g.at[1], c, 1, start, count, n)


def spread(tiles, reach):
    _, lane = grid_ids()
    n = len(tiles)
    out = {0: tiles}
    for d in [k for k in range(-reach, reach + 1) if k]:
        turned = [[pltpu.roll(x, -d % 128, 1) for x in blocks] for blocks in tiles]
        if n > 1:
            own = lane < 128 - d if d > 0 else lane >= -d
            step = 1 if d > 0 else -1
            turned = [
                [jnp.where(own, x, y) for x, y in zip(turned[t], turned[(t + step) % n])] for t in range(n)
            ]
        out[d] = turned
    return out


def weights(c_ref, start, count):
    return [
        [tuple(c_ref[5 * colour + k, pl.ds(start + 8 * b, 8), :] for k in range(3)) for b in range(count)]
        for colour in range(2)
    ]


def relaxed_spread(src, g, w, colour, reach):
    sub, lane = grid_ids()
    even = lane % 2 == 0
    out = {}
    for d in range(-reach, reach + 1):
        kind = (colour + d) % 2
        out[d] = []
        for t, x in enumerate(src[d]):
            one = [pltpu.roll(y, 1, 0) for y in x]
            back = [pltpu.roll(y, 7, 0) for y in x]
            n = len(x)
            new = []
            for b in range(n):
                before = jnp.where(sub == 0, one[b - 1] if b else 0.0, one[b])
                after = jnp.where(sub == 7, back[b + 1] if b < n - 1 else 0.0, back[b])
                near, far, ang = w[kind][b]
                other = jnp.where(even, before, after) if kind == 0 else jnp.where(even, after, before)
                new.append((g[d][t][b] + near * x[b]) + (far * other + ang * (src[d - 1][t][b] + src[d + 1][t][b])))
            out[d].append(new)
    return out


def read(ref, start, count, n=1):
    return [[ref[t, pl.ds(start + 8 * b, 8), :] for b in range(count)] for t in range(n)]


def put(ref, start, tiles):
    for t, blocks in enumerate(tiles):
        for b, x in enumerate(blocks):
            ref[t, pl.ds(start + 8 * b, 8), :] = x


def spread_down(k, g, s, c_ref, start, count, n):
    w = weights(c_ref, start, count)
    gr, gk = spread(read(g.at[0], start, count, n), 4), spread(read(g.at[1], start, count, n), 3)
    black = relaxed_spread(gr, gk, w, 1, 3)
    red = relaxed_spread(black, gr, w, 0, 2)
    black = relaxed_spread(red, gk, w, 1, 1)
    put(k, start, black[0])
    new = relaxed_spread(black, gr, w, 0, 0)[0]
    for t in range(n):
        for b in range(count):
            at = pl.ds(start + 8 * b, 8)
            s[t, at, :] = c_ref[4, at, :] * (new[t][b] - red[0][t][b])


def spread_post(r, k, g, c_ref, start, count, n):
    w = weights(c_ref, start, count)
    gr, gk = spread(read(g.at[0], start, count, n), 3), spread(read(g.at[1], start, count, n), 2)
    red = relaxed_spread(spread(read(k, start, count, n), 4), gr, w, 0, 3)
    black = relaxed_spread(red, gk, w, 1, 2)
    red = relaxed_spread(black, gr, w, 0, 1)
    put(r, start, red[0])
    put(k, start, relaxed_spread(red, gk, w, 1, 0)[0])


def kernel(
    right_hbm, guess_hbm, x0, c0,
    raw, r0, s0, g1, r1, k1, s1, g2, r2, k2, s2, x3, r3, s3,
    g4, r4, k4, s4, g5, r5, k5, s5, g6, r6, k6, s6, g7, r7, k7,
    win, e_ref, f_ref, fb_ref, mix, nat, c1, c2, c3, c4, c5, c6, c7,
    pk0, pc0, rp0, rd0, pk1, rl1, rd1, bs3, own4, slots, strip,
    load_sem, send0, recv0, send1, recv1, sendc, recvc, senda, recva, sendg, recvg,
):
    me_a, me_r = lax.axis_index("ang"), lax.axis_index("rad")

    def device(dr, da):
        return {"ang": lax.rem(me_a + da + NA, NA), "rad": lax.rem(me_r + dr + NB, NB)}

    barrier = pltpu.get_barrier_semaphore()
    partners = list(DIRS) + [(0, d) for d in range(2, NA - 1)] + [(d, 0) for d in range(2, NB - 1)]
    for dr, da in partners:
        pl.semaphore_signal(barrier, inc=1, device_id=device(dr, da), device_id_type=MESH)

    loads = []
    for t in range(8):
        for k, src in ((0, guess_hbm), (1, right_hbm)):
            loads.append(pltpu.make_async_copy(
                src.at[:, pl.ds(128 * t, 128)], raw.at[k, t], load_sem))
    for copy in loads:
        copy.start()

    zero = jnp.zeros((8, 128), F32)
    k0, g0 = x0.at[0], x0.at[pl.ds(1, 2)]
    k3, g3 = x3.at[0], x3.at[pl.ds(1, 2)]
    edges = [(r, 0) for r in (r0, s0)] + [(r, 1) for r in (r1, k1, s1)]
    edges += [(r, 2) for r in (g2.at[0], g2.at[1], r2, k2, s2)]
    edges += [(r, 3) for r in (k3, x3.at[1], x3.at[2], r3, s3)]
    for ref, l in edges:
        depth = 1 if l < 2 else 2
        for t in range(OWN[l][1] + 1):
            for d in range(depth):
                ref[t, pl.ds(8 * d, 8), :] = zero
                ref[t, pl.ds(ROWS[l] - 8 - 8 * d, 8), :] = zero
    for l, refs in enumerate(((g4, r4, k4, s4), (g5, r5, k5, s5), (g6, r6, k6, s6), (g7, r7, k7))):
        for ref in refs:
            for x in ((ref.at[0], ref.at[1]) if len(ref.shape) == 4 else (ref,)):
                for t in range(WHOLE[l][1]):
                    x[t, pl.ds(0, 8), :] = zero
                    x[t, pl.ds(WB + WHOLE[l][0], 8), :] = zero
    zero_rows(win, 1, 0, 6)
    for t in range(9):
        for d in (0, 1, 10, 11):
            f_ref[t, pl.ds(8 * d, 8), :] = zero
    for l, c_ref in enumerate((c0, c1, c2, c3)):
        fill_coefficients(c_ref, ROWS[l] // 8, BASE[l], me_r * (2 * OWN[l][0]), NR >> l, NT >> l)
    for l, c_ref in enumerate((c4, c5, c6, c7)):
        fill_coefficients(c_ref, WHOLE[l][0] // 8 + 2, WB, 0, 2 * WHOLE[l][0], NT >> (l + 4))

    sub, lane = grid_ids()
    even = lane % 2 == 0

    def send(src, dst, send_sem, recv_sem, dr, da):
        pltpu.make_async_remote_copy(
            src_ref=src, dst_ref=dst, send_sem=send_sem, recv_sem=recv_sem,
            device_id=device(dr, da), device_id_type=MESH).start()

    def edge(l, dr, width):
        if dr < 0:
            return pl.ds(BASE[l], width), pl.ds(BASE[l] + OWN[l][0], width)
        return pl.ds(BASE[l] + OWN[l][0] - width, width), pl.ds(BASE[l] - width, width)

    wait_bytes(raw, load_sem)
    for k in range(8):
        at = pl.ds(BASE[0] + 8 * k, 8)
        red, black = c0[3, at, :], c0[8, at, :]
        for t in range(8):
            k0[t, at, :] = jnp.where(
                even, raw[0, t, pl.ds(16 * k + 1, 8, stride=2), :], raw[0, t, pl.ds(16 * k, 8, stride=2), :])
            x = raw[1, t, pl.ds(16 * k, 8, stride=2), :]
            y = raw[1, t, pl.ds(16 * k + 1, 8, stride=2), :]
            g0[0, t, at, :] = jnp.where(even, x, y) * red
            g0[1, t, at, :] = jnp.where(even, y, x) * black
    for q in range(3):
        for side, (tile, first) in enumerate(((0, 0), (7, 112))):
            total = None
            for b in range(8):
                x = x0[q, tile, pl.ds(BASE[0] + 8 * b, 8), :]
                shift = (16 * b - first) % 128
                x = pltpu.roll(x, shift, 1) if shift else x
                total = x if total is None else jnp.where(lane // 16 == b, x, total)
            pk0[side, q, :, :] = total
    for c, (dr, da) in enumerate(CORNERS):
        rows = pl.ds(BASE[0] if dr < 0 else BASE[0] + OWN[0][0] - 8, 8)
        tile, first = (0, 0) if da < 0 else (7, 112)
        total = None
        for q in range(3):
            x = x0[q, tile, rows, :]
            shift = (16 * q - first) % 128
            x = pltpu.roll(x, shift, 1) if shift else x
            total = x if total is None else jnp.where(lane // 16 == q, x, total)
        pc0[c, :, :] = total
    pl.semaphore_wait(barrier, len(partners))

    for dr, da in ORDER:
        mine, theirs = edge(0, dr, E0) if dr else (None, None)
        if da == 0:
            send(x0.at[0, pl.ds(0, 8), mine, :], x0.at[0, pl.ds(0, 8), theirs, :], send0, recv0, dr, da)
            mine, theirs = edge(0, dr, 4)
            send(x0.at[pl.ds(1, 2), pl.ds(0, 8), mine, :], x0.at[pl.ds(1, 2), pl.ds(0, 8), theirs, :],
                 send0, recv0, dr, da)
        elif dr == 0:
            side = 0 if da < 0 else 1
            send(pk0.at[side], rp0.at[side], send0, recv0, dr, da)
        else:
            c = CORNERS.index((dr, da))
            send(pc0.at[c, pl.ds(0 if dr < 0 else 8 - E0, E0), :], rd0.at[c, pl.ds(0, E0), :], send0, recv0, dr, da)
    wait_bytes(f_ref.at[pl.ds(0, 4), pl.ds(0, 69), :], send0, recv0)

    def clear_outside(refs, l, n, depth=1):
        @pl.when(me_r == 0)
        def _():
            for ref in refs:
                zero_rows(ref, n, BASE[l] - 8 * depth, depth)

        @pl.when(me_r == NB - 1)
        def _():
            for ref in refs:
                zero_rows(ref, n, BASE[l] + OWN[l][0], depth)

    for q in range(3):
        from_left, from_right = rp0[1, q], rp0[0, q]
        for b in range(8):
            shift_r, shift_l = (-16 * b) % 128, (112 - 16 * b) % 128
            x = pltpu.roll(from_right, shift_r, 1) if shift_r else from_right
            y = pltpu.roll(from_left, shift_l, 1) if shift_l else from_left
            x0[q, 8, pl.ds(BASE[0] + 8 * b, 8), :] = jnp.where(lane < 64, x, y)
        for dr in (-1, 1):
            start = BASE[0] - E0 if dr < 0 else BASE[0] + OWN[0][0]
            x = rd0[CORNERS.index((-dr, -1)), :, :]
            y = pltpu.roll(rd0[CORNERS.index((-dr, 1)), :, :], 112 - 16 * q, 1)
            x = pltpu.roll(x, 128 - 16 * q, 1) if q else x
            x0[q, 8, pl.ds(start, E0), :] = jnp.where(lane < 64, x, y)[:E0]
    clear_outside((k0, g0.at[0], g0.at[1]), 0, 9)

    for _ in range(2):
        half_sweep(r0, k0, g0.at[0], c0, 0, 4, 9, 9)
        half_sweep(k0, r0, g0.at[1], c0, 1, 4, 9, 9)
    residual_pass(s0, r0, k0, g0.at[0], c0, 0, 4, 9, 9)
    restrict_pass(s0, BASE[0], 9, mix, nat, g1, BASE[1], c1, 0, 4, ((0, 1), (2, 3), (4, 5), (6, 7)))

    for b in range(4):
        at, own = pl.ds(8 * b, 8), pl.ds(BASE[1] + 8 * b, 8)
        pk1[0, at, :] = jnp.where(lane < 64, g1[0, 0, own, :], pltpu.roll(g1[1, 0, own, :], 64, 1))
        pk1[1, at, :] = jnp.where(lane < 64, pltpu.roll(g1[0, 3, own, :], 64, 1), g1[1, 3, own, :])
    for dr, da in ORDER:
        side = 0 if da < 0 else 1
        if da == 0:
            mine, theirs = edge(1, dr, E1)
            send(g1.at[:, pl.ds(0, 4), mine, :], g1.at[:, pl.ds(0, 4), theirs, :], send1, recv1, dr, da)
        elif dr == 0:
            send(pk1.at[side], rl1.at[side], send1, recv1, dr, da)
        else:
            send(pk1.at[side, pl.ds(0 if dr < 0 else 32 - E1, E1), :],
                 rd1.at[CORNERS.index((dr, da)), pl.ds(0, E1), :], send1, recv1, dr, da)
    wait_bytes(f_ref.at[pl.ds(0, 8), pl.ds(0, 53), :], send1, recv1)

    def merge_edges(row, size, from_right, from_left):
        low = lane[:size] < 64
        g1[0, 4, pl.ds(row, size), :] = jnp.where(low, from_right, pltpu.roll(from_left, 64, 1))
        g1[1, 4, pl.ds(row, size), :] = jnp.where(low, pltpu.roll(from_right, 64, 1), from_left)

    for b in range(4):
        merge_edges(BASE[1] + 8 * b, 8, rl1[0, pl.ds(8 * b, 8), :], rl1[1, pl.ds(8 * b, 8), :])
    for dr in (-1, 1):
        start = BASE[1] - E1 if dr < 0 else BASE[1] + OWN[1][0]
        right, left = CORNERS.index((-dr, -1)), CORNERS.index((-dr, 1))
        for first in (0, 8, 16):
            size = 8 if first < 16 else 2
            merge_edges(start + first, size, rd1[right, pl.ds(first, size), :], rd1[left, pl.ds(first, size), :])
    for q in range(2):
        for dr in (-1, 1):
            rest = BASE[1] - E1 - 3 if dr < 0 else BASE[1] + OWN[1][0] + E1
            for t in range(5):
                g1[q, t, pl.ds(rest, 3), :] = jnp.zeros((3, 128), F32)
    clear_outside((g1.at[0], g1.at[1]), 1, 5, 3)

    down(r1, k1, g1, s1, c1, BASE[1] - 20, 9, 5)
    restrict_pass(s1, BASE[1], 5, mix, nat, g2, BASE[2], c2, -8, 4, ((0, 1), (2, 3), (4, 4)))
    down(r2, k2, g2, s2, c2, BASE[2] - 8, 4, 3)
    restrict_pass(s2, BASE[2], 3, mix, nat, g3, BASE[3], c3, -4, 2, ((0, 1), (2, 2)))
    spread_down(k3, g3, s3, c3, BASE[3] - 4, 2, 2)

    nat[0, pl.ds(0, 8), :] = gathered(joined(*mixed_block(s3, BASE[3], 2, lane)[:1] * 2, lane), lane)
    x, y = nat[0, pl.ds(0, 4, stride=2), :], nat[0, pl.ds(1, 4, stride=2), :]
    my_pairs = pl.ds(WB + 4 * me_r, 4)
    own4[pl.ds(0, 4), :] = jnp.where(even[:4], x, y) * c4[3, my_pairs, :]
    own4[pl.ds(4, 4), :] = jnp.where(even[:4], y, x) * c4[8, my_pairs, :]
    for d in range(1, NA):
        send(own4, slots.at[d - 1], senda, recva, 0, d)
    wait_bytes(slots, senda, recva)
    for t in range(4):
        total = own4[...]
        for d in range(1, NA):
            source = lax.rem(me_a - d + NA, NA)
            hit = jnp.logical_and(source // 2 == t, lane // 64 == source % 2)
            total = jnp.where(hit, slots[d - 1], total)
        for q in range(2):
            strip[q, t, pl.ds(0, 4), :] = total[4 * q:4 * q + 4]
            g4[q, t, my_pairs, :] = total[4 * q:4 * q + 4]
    for d in range(1, NB):
        send(strip.at[:, :, pl.ds(0, 4), :], g4.at[:, :, my_pairs, :], sendg, recvg, d, 0)
    for k, (dr, da) in enumerate(DIRS):
        send(x3.at[:, 0, pl.ds(BASE[3], 8), :], bs3.at[k], sendc, recvc, dr, da)
    wait_bytes(g4.at[:, :, pl.ds(WB, 60), :], sendg, recvg)

    down(r4, k4, g4, s4, c4, WB, 8, 4)
    restrict_pass(s4, WB, 4, mix, nat, g5, WB, c5, 0, 4, ((0, 1), (2, 3)))
    down(r5, k5, g5, s5, c5, WB, 4, 2)
    restrict_pass(s5, WB, 2, mix, nat, g6, WB, c6, 0, 2, ((0, 1),))
    spread_down(k6, g6, s6, c6, WB, 2, 1)
    restrict_pass(s6, WB, 1, mix, nat, g7, WB, c7, 0, 1, ((0, 0),))
    gr7, gk7, w7 = spread(read(g7.at[0], WB, 1), 4), spread(read(g7.at[1], WB, 1), 3), weights(c7, WB, 1)
    source = gr7
    for step in range(4):
        black = relaxed_spread(source, gk7, w7, 1, 3 if step < 3 else 2)
        red = relaxed_spread(black, gr7, w7, 0, 2 if step < 3 else 1)
        black = relaxed_spread(red, gk7, w7, 1, 1 if step < 3 else 0)
        if step < 3:
            source = spread(relaxed_spread(black, gr7, w7, 0, 0)[0], 4)
    put(r7, WB, red[0])
    put(k7, WB, black[0])

    def whole_up(rc, kc, blocks, nc, fine, plan):
        for k in range(blocks):
            unpair(rc, kc, WB + 8 * k, e_ref, FB + 16 * k, nc)
        prolong_pass(e_ref, f_ref, fb_ref, 0, 2 * blocks, fine, WB, 0, 2 * blocks, plan, True)

    whole_up(r7, k7, 1, 1, k6, ((0, 0),))
    spread_post(r6, k6, g6, c6, WB, 2, 1)
    whole_up(r6, k6, 2, 1, k5, ((0, 0), (0, 1)))
    post(r5, k5, g5, c5, WB, 4, 2)
    whole_up(r5, k5, 4, 2, k4, ((0, 0), (0, 1), (1, 0), (1, 1)))
    post(r4, k4, g4, c4, WB, 8, 4)

    def block(ref, da, wanted, at):
        b = lax.rem(me_a + da + NA, NA)
        x = ref[b // 2, at, :]
        return jnp.where(b % 2 == wanted, x, pltpu.roll(x, 64, 1))

    for k in range(2):
        at = pl.ds(WB - 4 + 4 * me_r + 8 * k, 8)
        seen = []
        for ref in (r4, k4):
            mine, rightward, leftward = block(ref, 0, 0, at), block(ref, 1, 1, at), block(ref, -1, 1, at)
            seen.append(jnp.where(lane < 64, mine, jnp.where(lane < 96, rightward, leftward)))
        q = FB - 8 + 16 * k
        win[0, pl.ds(q, 8, stride=2), :] = jnp.where(even, seen[0], seen[1])
        win[0, pl.ds(q + 1, 8, stride=2), :] = jnp.where(even, seen[1], seen[0])

    wait_bytes(bs3, sendc, recvc)
    for q in range(3):
        got = lambda dr, da: bs3[DIRS.index((-dr, -da)), q]
        x3[q, 0, pl.ds(BASE[3] - 8, 8), :] = got(-1, 0)
        x3[q, 0, pl.ds(BASE[3] + 8, 8), :] = got(1, 0)
        for dr in (-1, 0, 1):
            x3[q, 1, pl.ds(BASE[3] + 8 * dr, 8), :] = jnp.where(lane < 64, got(dr, 1), got(dr, -1))
    prolong_pass(win, f_ref, fb_ref, -8, 3, k3, BASE[3], -8, 3, ((0, 0), (0, 1)), False)
    clear_outside((k3, g3.at[0], g3.at[1]), 3, 2)
    spread_post(r3, k3, g3, c3, BASE[3] - 8, 3, 2)

    for k in range(2):
        unpair(r3, k3, BASE[3] - 4 + 8 * k, e_ref, FB - 8 + 16 * k, 2)
    prolong_pass(e_ref, f_ref, fb_ref, -8, 4, k2, BASE[2], -4, 3, ((0, 0), (0, 1), (1, 2)), False)
    clear_outside((k2,), 2, 3)
    post(r2, k2, g2, c2, BASE[2] - 4, 3, 3)

    for k in range(3):
        unpair(r2, k2, BASE[2] - 4 + 8 * k, e_ref, FB - 8 + 16 * k, 3)
    prolong_pass(e_ref, f_ref, fb_ref, -8, 6, k1, BASE[1], -4, 5, ((0, 0), (0, 1), (1, 0), (1, 1), (2, 2)), False)
    clear_outside((k1,), 1, 5)
    post(r1, k1, g1, c1, BASE[1] - 4, 5, 5)

    for k in range(5):
        unpair(r1, k1, BASE[1] - 4 + 8 * k, e_ref, FB - 8 + 16 * k, 5)
    plan = tuple((t // 2, t % 2) for t in range(8)) + ((4, 2),)
    prolong_pass(e_ref, f_ref, fb_ref, -8, 10, k0, BASE[0], -4, 9, plan, False)
    clear_outside((k0,), 0, 9)


def finish(x0, c0, sol_hbm, res_hbm, r, k, s, b, raw, out_sem):
    zero = jnp.zeros((8, 128), F32)
    for ref in (r, k):
        for t in range(9):
            ref[t, pl.ds(0, 8), :] = zero
            ref[t, pl.ds(ROWS[0] - 8, 8), :] = zero
    start, gr, gk = x0.at[0], x0.at[1], x0.at[2]
    half_sweep(r, start, gr, c0, 0, 4, 9, 9)
    half_sweep(k, r, gk, c0, 1, 4, 9, 9)
    half_sweep(r, k, gr, c0, 0, 4, 9, 9)
    half_sweep(k, r, gk, c0, 1, 4, 9, 9)

    def write(slot, red, black, hbm):
        for t in range(8):
            for q in range(8):
                unpair(red.at[pl.ds(t, 1)], black.at[pl.ds(t, 1)], BASE[0] + 8 * q, raw.at[slot, pl.ds(t, 1)], 16 * q, 1)
            copy = pltpu.make_async_copy(raw.at[slot, t], hbm.at[:, pl.ds(128 * t, 128)], out_sem)
            copy.start()

    write(0, r, k, sol_hbm)
    residual_pass(s, r, k, gr, c0, 0, BASE[0], 8, 9, tiles=range(8))
    residual_pass(b, k, r, gk, c0, 1, BASE[0], 8, 9, tiles=range(8))
    write(1, s, b, res_hbm)
    wait_bytes(raw, out_sem)


def local(right_side, guess):
    def vm(*shape):
        return pltpu.VMEM(shape, F32)

    levels = [vm(2, 8, 128, 128), vm(9, ROWS[0], 128), vm(9, ROWS[0], 128)]
    for l in (1, 2):
        n = OWN[l][1] + 1
        levels += [vm(2, n, ROWS[l], 128)] + [vm(n, ROWS[l], 128)] * 3
    levels += [vm(3, 2, ROWS[3], 128), vm(2, ROWS[3], 128), vm(2, ROWS[3], 128)]
    for l, (pairs, tiles) in enumerate(WHOLE):
        levels += [vm(2, tiles, pairs + 2 * WB, 128)] + [vm(tiles, pairs + 2 * WB, 128)] * (2 if l == 3 else 3)
    coefficients = [vm(10, r, 128) for r in ROWS[1:]] + [vm(10, pairs + 2 * WB, 128) for pairs, _ in WHOLE]
    buffers = [
        vm(2, 3, 8, 128), vm(4, 8, 128), vm(2, 3, 8, 128), vm(4, 8, 128),
        vm(2, 32, 128), vm(2, 32, 128), vm(4, 24, 128),
        vm(8, 3, 8, 128), vm(8, 128), vm(NA - 1, 8, 128), vm(2, 4, 8, 128),
    ]
    dma = pltpu.SemaphoreType.DMA
    sems = [dma] * 11
    natural = [vm(1, 48, 128), vm(5, 96, 128), vm(9, 96, 128), vm(9, 96, 128), vm(9, 64, 128), vm(4, 64, 128)]
    held = (vm(3, 9, ROWS[0], 128), vm(10, ROWS[0], 128))
    inside = pl.BlockSpec(memory_space=pltpu.VMEM)
    outside = pl.BlockSpec(memory_space=pl.ANY)
    x0, c0 = pl.pallas_call(
        kernel,
        out_shape=held,
        in_specs=[outside] * 2,
        out_specs=(inside,) * 2,
        scratch_shapes=levels + natural + coefficients + buffers + sems,
        compiler_params=pltpu.CompilerParams(collective_id=0, has_side_effects=True),
    )(right_side, guess)
    x0, c0 = (pltpu.with_memory_space_constraint(x, pltpu.VMEM) for x in (x0, c0))
    block = jax.ShapeDtypeStruct(right_side.shape, F32)
    return pl.pallas_call(
        finish,
        out_shape=(block, block),
        in_specs=[inside] * 2,
        out_specs=(outside,) * 2,
        scratch_shapes=[vm(9, ROWS[0], 128)] * 4 + [vm(2, 8, 128, 128), dma],
    )(x0, c0)


def solution(mesh):
    placed = (P("rad", "ang"), P("rad", "ang"))
    return jax.shard_map(local, mesh=mesh, in_specs=placed, out_specs=placed, check_vma=False)
```

```python
import math

import jax
import jax.numpy as jnp
from jax import lax
from jax.experimental import pallas as pl
from jax.experimental.pallas import tpu as pltpu
from jax.sharding import PartitionSpec as P

MESH = pl.DeviceIdType.MESH
F32 = jnp.float32
NR, NT = 2048, 8192
NA, NB = 8, 16
OWN = ((64, 8), (32, 4), (16, 2), (8, 1))
BASE = (8, 24, 16, 16)
ROWS = tuple(o[0] + 2 * b for o, b in zip(OWN, BASE))
E0, E1 = 5, 18
WHOLE = ((64, 4), (32, 2), (16, 1), (8, 1))
WB = 8
DIRS = tuple((dr, da) for dr in (-1, 0, 1) for da in (-1, 0, 1) if dr or da)
CORNERS = tuple(d for d in DIRS if d[0] and d[1])
ORDER = tuple(sorted(DIRS, key=lambda d: (d[1] != 0, d[0] == 0)))
FB = 16


def grid_ids():
    sub = lax.broadcasted_iota(jnp.int32, (8, 128), 0)
    lane = lax.broadcasted_iota(jnp.int32, (8, 128), 1)
    return sub, lane


def ring_shift(tiles, lane):
    n = len(tiles)
    one = [pltpu.roll(x, 1, 1) for x in tiles]
    back = [pltpu.roll(x, 127, 1) for x in tiles]
    if n == 1:
        return one, back
    left = [jnp.where(lane == 0, one[t - 1], one[t]) for t in range(n)]
    right = [jnp.where(lane == 127, back[(t + 1) % n], back[t]) for t in range(n)]
    return left, right


def pick(x, index):
    return jnp.take_along_axis(x, index, axis=1, mode="promise_in_bounds")


def fill_coefficients(c_ref, count, base, first_row, total_rows, cells):
    h = 2.0 * math.pi / cells
    sub, lane = grid_ids()
    even = lane % 2 == 0

    def row_values(row):
        inside = jnp.logical_and(row >= 0, row < total_rows)
        r = 1.0 + (row.astype(F32) + 0.5) * h
        rr = r * r
        q = jnp.where(inside, 0.5 / (rr + 1.0), 0.0)
        half = (0.5 * h) * r
        return (rr + half) * q, (rr - half) * q, q, rr * q, 2.0 + 2.0 / rr

    for k in range(count):
        row = first_row + 2 * (8 * k - base + sub)
        o0, i0, a0, w0, c0 = row_values(row)
        o1, i1, a1, w1, c1 = row_values(row + 1)
        at = pl.ds(8 * k, 8)
        for j, (x, y) in enumerate(((o0, i1), (i0, o1), (a0, a1), (w0, w1), (c0, c1))):
            c_ref[j, at, :] = jnp.where(even, x, y)
            c_ref[5 + j, at, :] = jnp.where(even, y, x)


def relaxed(src, g, c_ref, colour, p, n, lane, tiles):
    at = pl.ds(p, 8)
    even = lane % 2 == 0
    first, second = (p - 1, p + 1) if colour == 0 else (p + 1, p - 1)
    x = {t: src[t, at, :] for t in sorted({(u + d) % n for u in tiles for d in (-1, 0, 1)})}
    one = {t: pltpu.roll(x[t], 1, 1) for t in sorted({(u + d) % n for u in tiles for d in (-1, 0)})}
    back = {t: pltpu.roll(x[t], 127, 1) for t in sorted({(u + d) % n for u in tiles for d in (0, 1)})}
    near, far, ang = (c_ref[5 * colour + k, at, :] for k in range(3))
    new = {}
    for t in tiles:
        left, right = one[t], back[t]
        if n > 1:
            left = jnp.where(lane == 0, one[(t - 1) % n], left)
            right = jnp.where(lane == 127, back[(t + 1) % n], right)
        other = jnp.where(even, src[t, pl.ds(first, 8), :], src[t, pl.ds(second, 8), :])
        new[t] = (g[t, at, :] + near * x[t]) + (far * other + ang * (left + right))
    return new


def half_sweep(dst, src, g, c_ref, colour, start, count, n, tiles=None):
    _, lane = grid_ids()
    for k in range(count):
        p = start + 8 * k
        for t, value in relaxed(src, g, c_ref, colour, p, n, lane, tiles or range(n)).items():
            dst[t, pl.ds(p, 8), :] = value


def residual_pass(dst, old, src, g, c_ref, colour, start, count, n, tiles=None):
    _, lane = grid_ids()
    for k in range(count):
        p = start + 8 * k
        c = c_ref[5 * colour + 4, pl.ds(p, 8), :]
        for t, value in relaxed(src, g, c_ref, colour, p, n, lane, tiles or range(n)).items():
            dst[t, pl.ds(p, 8), :] = c * (value - old[t, pl.ds(p, 8), :])


def fence(step):
    pl.when(lax.axis_index("rad") < NB)(step)


def mixed_block(s, p, n, lane):
    even = lane % 2 == 0
    r = [
        3.0 * s[t, pl.ds(p, 8), :] + jnp.where(even, s[t, pl.ds(p + 1, 8), :], s[t, pl.ds(p - 1, 8), :])
        for t in range(n)
    ]
    left, right = ring_shift(r, lane)
    return [3.0 * r[t] + jnp.where(even, left[t], right[t]) for t in range(n)]


def joined(a, b, lane):
    return jnp.where(lane % 2 == 0, a + pltpu.roll(a, 127, 1), b + pltpu.roll(b, 1, 1))


def gathered(x, lane):
    return pick(x, jnp.where(lane < 64, 2 * lane, 2 * lane - 127)) * 0.0625


def restrict_pass(s, fine_base, n, mix, nat, g, coarse_base, c_ref, start, count, pairs):
    _, lane = grid_ids()
    even = lane % 2 == 0
    for k in range(2 * count):
        for t, x in enumerate(mixed_block(s, fine_base + 2 * start + 8 * k, n, lane)):
            mix[t, pl.ds(8 * k, 8), :] = x

    def joins():
        for k in range(2 * count):
            at = pl.ds(8 * k, 8)
            for t, (a, b) in enumerate(pairs):
                nat[t, at, :] = joined(mix[a, at, :], mix[b, at, :], lane)

    fence(joins)

    def gathers():
        for k in range(2 * count):
            for t in range(len(pairs)):
                nat[t, pl.ds(8 * k, 8), :] = gathered(nat[t, pl.ds(8 * k, 8), :], lane)

    fence(gathers)
    for k in range(count):
        p = pl.ds(coarse_base + start + 8 * k, 8)
        red, black = c_ref[3, p, :], c_ref[8, p, :]
        for t in range(len(pairs)):
            x = nat[t, pl.ds(16 * k, 8, stride=2), :]
            y = nat[t, pl.ds(16 * k + 1, 8, stride=2), :]
            g[0, t, p, :] = jnp.where(even, x, y) * red
            g[1, t, p, :] = jnp.where(even, y, x) * black


def unpair(red, black, p, dst, q, n):
    _, lane = grid_ids()
    even = lane % 2 == 0
    for t in range(n):
        x, y = red[t, pl.ds(p, 8), :], black[t, pl.ds(p, 8), :]
        dst[t, pl.ds(q, 8, stride=2), :] = jnp.where(even, x, y)
        dst[t, pl.ds(q + 1, 8, stride=2), :] = jnp.where(even, y, x)


def prolong_pass(e, f, fa, fb, start, count, fine, fine_base, fine_start, fine_count, plan, sealed):
    _, lane = grid_ids()
    even = lane % 2 == 0
    half = lane // 2
    kinds = (half, half + 64, jnp.where(lane < 64, half, half + 64))
    nc = max(source for source, _ in plan) + 1
    for k in range(count):
        at = pl.ds(FB + start + 8 * k, 8)
        x = [e[t, at, :] for t in range(nc)]
        left, right = ring_shift(x, lane)
        for t in range(nc):
            fa[t, at, :] = 0.75 * x[t] + 0.25 * left[t]
            fb[t, at, :] = 0.75 * x[t] + 0.25 * right[t]

    for wanted, index in enumerate(kinds):
        tiles = [(t, source) for t, (source, kind) in enumerate(plan) if kind == wanted]

        def gathers(tiles=tiles, index=index):
            for k in range(count):
                at = pl.ds(FB + start + 8 * k, 8)
                for t, source in tiles:
                    f[t, at, :] = jnp.where(even, pick(fa[source, at, :], index), pick(fb[source, at, :], index))

        if tiles and wanted < 2:
            fence(gathers)
        elif tiles:
            gathers()
    if sealed:
        for t in range(len(plan)):
            f[t, pl.ds(FB - 8, 8), :] = jnp.zeros((8, 128), F32)
            f[t, pl.ds(FB + 8 * count, 8), :] = jnp.zeros((8, 128), F32)
    for k in range(fine_count):
        i = fine_start + 8 * k
        at = pl.ds(fine_base + i, 8)
        for t in range(len(plan)):
            other = jnp.where(even, f[t, pl.ds(FB + i + 1, 8), :], f[t, pl.ds(FB + i - 1, 8), :])
            fine[t, at, :] = fine[t, at, :] + (0.75 * f[t, pl.ds(FB + i, 8), :] + 0.25 * other)


def wait_bytes(ref, *sems):
    for sem in sems:
        pltpu.make_async_copy(ref, ref, sem).wait()


def zero_rows(ref, n, start, count):
    for t in range(n):
        for k in range(count):
            ref[t, pl.ds(start + 8 * k, 8), :] = jnp.zeros((8, 128), F32)


def down(r, k, g, s, c, start, count, n):
    half_sweep(k, g.at[0], g.at[1], c, 1, start, count, n)
    half_sweep(r, k, g.at[0], c, 0, start, count, n)
    half_sweep(k, r, g.at[1], c, 1, start, count, n)
    residual_pass(s, r, k, g.at[0], c, 0, start, count, n)


def post(r, k, g, c, start, count, n):
    for _ in range(2):
        half_sweep(r, k, g.at[0], c, 0, start, count, n)
        half_sweep(k, r, g.at[1], c, 1, start, count, n)


def spread(tiles, reach):
    _, lane = grid_ids()
    n = len(tiles)
    out = {0: tiles}
    for d in [k for k in range(-reach, reach + 1) if k]:
        turned = [[pltpu.roll(x, -d % 128, 1) for x in blocks] for blocks in tiles]
        if n > 1:
            own = lane < 128 - d if d > 0 else lane >= -d
            step = 1 if d > 0 else -1
            turned = [
                [jnp.where(own, x, y) for x, y in zip(turned[t], turned[(t + step) % n])] for t in range(n)
            ]
        out[d] = turned
    return out


def weights(c_ref, start, count):
    return [
        [tuple(c_ref[5 * colour + k, pl.ds(start + 8 * b, 8), :] for k in range(3)) for b in range(count)]
        for colour in range(2)
    ]


def relaxed_spread(src, g, w, colour, reach):
    sub, lane = grid_ids()
    even = lane % 2 == 0
    out = {}
    for d in range(-reach, reach + 1):
        kind = (colour + d) % 2
        out[d] = []
        for t, x in enumerate(src[d]):
            one = [pltpu.roll(y, 1, 0) for y in x]
            back = [pltpu.roll(y, 7, 0) for y in x]
            n = len(x)
            new = []
            for b in range(n):
                before = jnp.where(sub == 0, one[b - 1] if b else 0.0, one[b])
                after = jnp.where(sub == 7, back[b + 1] if b < n - 1 else 0.0, back[b])
                near, far, ang = w[kind][b]
                other = jnp.where(even, before, after) if kind == 0 else jnp.where(even, after, before)
                new.append((g[d][t][b] + near * x[b]) + (far * other + ang * (src[d - 1][t][b] + src[d + 1][t][b])))
            out[d].append(new)
    return out


def read(ref, start, count, n=1):
    return [[ref[t, pl.ds(start + 8 * b, 8), :] for b in range(count)] for t in range(n)]


def put(ref, start, tiles):
    for t, blocks in enumerate(tiles):
        for b, x in enumerate(blocks):
            ref[t, pl.ds(start + 8 * b, 8), :] = x


def spread_down(k, g, s, c_ref, start, count, n):
    w = weights(c_ref, start, count)
    gr, gk = spread(read(g.at[0], start, count, n), 4), spread(read(g.at[1], start, count, n), 3)
    black = relaxed_spread(gr, gk, w, 1, 3)
    red = relaxed_spread(black, gr, w, 0, 2)
    black = relaxed_spread(red, gk, w, 1, 1)
    put(k, start, black[0])
    new = relaxed_spread(black, gr, w, 0, 0)[0]
    for t in range(n):
        for b in range(count):
            at = pl.ds(start + 8 * b, 8)
            s[t, at, :] = c_ref[4, at, :] * (new[t][b] - red[0][t][b])


def spread_post(r, k, g, c_ref, start, count, n):
    w = weights(c_ref, start, count)
    gr, gk = spread(read(g.at[0], start, count, n), 3), spread(read(g.at[1], start, count, n), 2)
    red = relaxed_spread(spread(read(k, start, count, n), 4), gr, w, 0, 3)
    black = relaxed_spread(red, gk, w, 1, 2)
    red = relaxed_spread(black, gr, w, 0, 1)
    put(r, start, red[0])
    put(k, start, relaxed_spread(red, gk, w, 1, 0)[0])


def kernel(
    right_hbm, guess_hbm, x0, c0,
    raw, r0, s0, g1, r1, k1, s1, g2, r2, k2, s2, x3, r3, s3,
    g4, r4, k4, s4, g5, r5, k5, s5, g6, r6, k6, s6, g7, r7, k7,
    win, e_ref, f_ref, fa_ref, fb_ref, mix, nat, c1, c2, c3, c4, c5, c6, c7,
    pk0, pc0, rp0, rd0, pk1, rl1, rd1, bs3, own4, slots, strip,
    load_sem, send0, recv0, send1, recv1, sendc, recvc, senda, recva, sendg, recvg,
):
    me_a, me_r = lax.axis_index("ang"), lax.axis_index("rad")

    def device(dr, da):
        return {"ang": lax.rem(me_a + da + NA, NA), "rad": lax.rem(me_r + dr + NB, NB)}

    barrier = pltpu.get_barrier_semaphore()
    partners = list(DIRS) + [(0, d) for d in range(2, NA - 1)] + [(d, 0) for d in range(2, NB - 1)]
    for dr, da in partners:
        pl.semaphore_signal(barrier, inc=1, device_id=device(dr, da), device_id_type=MESH)

    loads = []
    for t in range(8):
        for k, src in ((0, guess_hbm), (1, right_hbm)):
            loads.append(pltpu.make_async_copy(
                src.at[:, pl.ds(128 * t, 128)], raw.at[k, t], load_sem))
    for copy in loads:
        copy.start()

    zero = jnp.zeros((8, 128), F32)
    k0, g0 = x0.at[0], x0.at[pl.ds(1, 2)]
    k3, g3 = x3.at[0], x3.at[pl.ds(1, 2)]
    edges = [(r, 0) for r in (r0, s0)] + [(r, 1) for r in (r1, k1, s1)]
    edges += [(r, 2) for r in (g2.at[0], g2.at[1], r2, k2, s2)]
    edges += [(r, 3) for r in (k3, x3.at[1], x3.at[2], r3, s3)]
    for ref, l in edges:
        depth = 1 if l < 2 else 2
        for t in range(OWN[l][1] + 1):
            for d in range(depth):
                ref[t, pl.ds(8 * d, 8), :] = zero
                ref[t, pl.ds(ROWS[l] - 8 - 8 * d, 8), :] = zero
    for l, refs in enumerate(((g4, r4, k4, s4), (g5, r5, k5, s5), (g6, r6, k6, s6), (g7, r7, k7))):
        for ref in refs:
            for x in ((ref.at[0], ref.at[1]) if len(ref.shape) == 4 else (ref,)):
                for t in range(WHOLE[l][1]):
                    x[t, pl.ds(0, 8), :] = zero
                    x[t, pl.ds(WB + WHOLE[l][0], 8), :] = zero
    zero_rows(win, 1, 0, 6)
    for t in range(9):
        for d in (0, 1, 10, 11):
            f_ref[t, pl.ds(8 * d, 8), :] = zero
    for l, c_ref in enumerate((c0, c1, c2, c3)):
        fill_coefficients(c_ref, ROWS[l] // 8, BASE[l], me_r * (2 * OWN[l][0]), NR >> l, NT >> l)
    for l, c_ref in enumerate((c4, c5, c6, c7)):
        fill_coefficients(c_ref, WHOLE[l][0] // 8 + 2, WB, 0, 2 * WHOLE[l][0], NT >> (l + 4))

    sub, lane = grid_ids()
    even = lane % 2 == 0

    def send(src, dst, send_sem, recv_sem, dr, da):
        pltpu.make_async_remote_copy(
            src_ref=src, dst_ref=dst, send_sem=send_sem, recv_sem=recv_sem,
            device_id=device(dr, da), device_id_type=MESH).start()

    def edge(l, dr, width):
        if dr < 0:
            return pl.ds(BASE[l], width), pl.ds(BASE[l] + OWN[l][0], width)
        return pl.ds(BASE[l] + OWN[l][0] - width, width), pl.ds(BASE[l] - width, width)

    wait_bytes(raw, load_sem)
    for k in range(8):
        at = pl.ds(BASE[0] + 8 * k, 8)
        red, black = c0[3, at, :], c0[8, at, :]
        for t in range(8):
            k0[t, at, :] = jnp.where(
                even, raw[0, t, pl.ds(16 * k + 1, 8, stride=2), :], raw[0, t, pl.ds(16 * k, 8, stride=2), :])
            x = raw[1, t, pl.ds(16 * k, 8, stride=2), :]
            y = raw[1, t, pl.ds(16 * k + 1, 8, stride=2), :]
            g0[0, t, at, :] = jnp.where(even, x, y) * red
            g0[1, t, at, :] = jnp.where(even, y, x) * black
    for q in range(3):
        for side, (tile, first) in enumerate(((0, 0), (7, 112))):
            total = None
            for b in range(8):
                x = x0[q, tile, pl.ds(BASE[0] + 8 * b, 8), :]
                shift = (16 * b - first) % 128
                x = pltpu.roll(x, shift, 1) if shift else x
                total = x if total is None else jnp.where(lane // 16 == b, x, total)
            pk0[side, q, :, :] = total
    for c, (dr, da) in enumerate(CORNERS):
        rows = pl.ds(BASE[0] if dr < 0 else BASE[0] + OWN[0][0] - 8, 8)
        tile, first = (0, 0) if da < 0 else (7, 112)
        total = None
        for q in range(3):
            x = x0[q, tile, rows, :]
            shift = (16 * q - first) % 128
            x = pltpu.roll(x, shift, 1) if shift else x
            total = x if total is None else jnp.where(lane // 16 == q, x, total)
        pc0[c, :, :] = total
    pl.semaphore_wait(barrier, len(partners))

    for dr, da in ORDER:
        mine, theirs = edge(0, dr, E0) if dr else (None, None)
        if da == 0:
            send(x0.at[0, pl.ds(0, 8), mine, :], x0.at[0, pl.ds(0, 8), theirs, :], send0, recv0, dr, da)
            mine, theirs = edge(0, dr, 4)
            send(x0.at[pl.ds(1, 2), pl.ds(0, 8), mine, :], x0.at[pl.ds(1, 2), pl.ds(0, 8), theirs, :],
                 send0, recv0, dr, da)
        elif dr == 0:
            side = 0 if da < 0 else 1
            send(pk0.at[side], rp0.at[side], send0, recv0, dr, da)
        else:
            c = CORNERS.index((dr, da))
            send(pc0.at[c, pl.ds(0 if dr < 0 else 8 - E0, E0), :], rd0.at[c, pl.ds(0, E0), :], send0, recv0, dr, da)
    wait_bytes(f_ref.at[pl.ds(0, 4), pl.ds(0, 69), :], send0, recv0)

    def clear_outside(refs, l, n, depth=1):
        @pl.when(me_r == 0)
        def _():
            for ref in refs:
                zero_rows(ref, n, BASE[l] - 8 * depth, depth)

        @pl.when(me_r == NB - 1)
        def _():
            for ref in refs:
                zero_rows(ref, n, BASE[l] + OWN[l][0], depth)

    for q in range(3):
        from_left, from_right = rp0[1, q], rp0[0, q]
        for b in range(8):
            shift_r, shift_l = (-16 * b) % 128, (112 - 16 * b) % 128
            x = pltpu.roll(from_right, shift_r, 1) if shift_r else from_right
            y = pltpu.roll(from_left, shift_l, 1) if shift_l else from_left
            x0[q, 8, pl.ds(BASE[0] + 8 * b, 8), :] = jnp.where(lane < 64, x, y)
        for dr in (-1, 1):
            start = BASE[0] - E0 if dr < 0 else BASE[0] + OWN[0][0]
            x = rd0[CORNERS.index((-dr, -1)), :, :]
            y = pltpu.roll(rd0[CORNERS.index((-dr, 1)), :, :], 112 - 16 * q, 1)
            x = pltpu.roll(x, 128 - 16 * q, 1) if q else x
            x0[q, 8, pl.ds(start, E0), :] = jnp.where(lane < 64, x, y)[:E0]
    clear_outside((k0, g0.at[0], g0.at[1]), 0, 9)

    for _ in range(2):
        half_sweep(r0, k0, g0.at[0], c0, 0, 4, 9, 9)
        half_sweep(k0, r0, g0.at[1], c0, 1, 4, 9, 9)
    residual_pass(s0, r0, k0, g0.at[0], c0, 0, 4, 9, 9)
    restrict_pass(s0, BASE[0], 9, mix, nat, g1, BASE[1], c1, 0, 4, ((0, 1), (2, 3), (4, 5), (6, 7)))

    for b in range(4):
        at, own = pl.ds(8 * b, 8), pl.ds(BASE[1] + 8 * b, 8)
        pk1[0, at, :] = jnp.where(lane < 64, g1[0, 0, own, :], pltpu.roll(g1[1, 0, own, :], 64, 1))
        pk1[1, at, :] = jnp.where(lane < 64, pltpu.roll(g1[0, 3, own, :], 64, 1), g1[1, 3, own, :])
    for dr, da in ORDER:
        side = 0 if da < 0 else 1
        if da == 0:
            mine, theirs = edge(1, dr, E1)
            send(g1.at[:, pl.ds(0, 4), mine, :], g1.at[:, pl.ds(0, 4), theirs, :], send1, recv1, dr, da)
        elif dr == 0:
            send(pk1.at[side], rl1.at[side], send1, recv1, dr, da)
        else:
            send(pk1.at[side, pl.ds(0 if dr < 0 else 32 - E1, E1), :],
                 rd1.at[CORNERS.index((dr, da)), pl.ds(0, E1), :], send1, recv1, dr, da)
    wait_bytes(f_ref.at[pl.ds(0, 8), pl.ds(0, 53), :], send1, recv1)

    def merge_edges(row, size, from_right, from_left):
        low = lane[:size] < 64
        g1[0, 4, pl.ds(row, size), :] = jnp.where(low, from_right, pltpu.roll(from_left, 64, 1))
        g1[1, 4, pl.ds(row, size), :] = jnp.where(low, pltpu.roll(from_right, 64, 1), from_left)

    for b in range(4):
        merge_edges(BASE[1] + 8 * b, 8, rl1[0, pl.ds(8 * b, 8), :], rl1[1, pl.ds(8 * b, 8), :])
    for dr in (-1, 1):
        start = BASE[1] - E1 if dr < 0 else BASE[1] + OWN[1][0]
        right, left = CORNERS.index((-dr, -1)), CORNERS.index((-dr, 1))
        for first in (0, 8, 16):
            size = 8 if first < 16 else 2
            merge_edges(start + first, size, rd1[right, pl.ds(first, size), :], rd1[left, pl.ds(first, size), :])
    for q in range(2):
        for dr in (-1, 1):
            rest = BASE[1] - E1 - 3 if dr < 0 else BASE[1] + OWN[1][0] + E1
            for t in range(5):
                g1[q, t, pl.ds(rest, 3), :] = jnp.zeros((3, 128), F32)
    clear_outside((g1.at[0], g1.at[1]), 1, 5, 3)

    down(r1, k1, g1, s1, c1, BASE[1] - 20, 9, 5)
    restrict_pass(s1, BASE[1], 5, mix, nat, g2, BASE[2], c2, -8, 4, ((0, 1), (2, 3), (4, 4)))
    down(r2, k2, g2, s2, c2, BASE[2] - 8, 4, 3)
    restrict_pass(s2, BASE[2], 3, mix, nat, g3, BASE[3], c3, -4, 2, ((0, 1), (2, 2)))
    spread_down(k3, g3, s3, c3, BASE[3] - 4, 2, 2)

    nat[0, pl.ds(0, 8), :] = gathered(joined(*mixed_block(s3, BASE[3], 2, lane)[:1] * 2, lane), lane)
    x, y = nat[0, pl.ds(0, 4, stride=2), :], nat[0, pl.ds(1, 4, stride=2), :]
    my_pairs = pl.ds(WB + 4 * me_r, 4)
    own4[pl.ds(0, 4), :] = jnp.where(even[:4], x, y) * c4[3, my_pairs, :]
    own4[pl.ds(4, 4), :] = jnp.where(even[:4], y, x) * c4[8, my_pairs, :]
    for d in range(1, NA):
        send(own4, slots.at[d - 1], senda, recva, 0, d)
    wait_bytes(slots, senda, recva)
    for t in range(4):
        total = own4[...]
        for d in range(1, NA):
            source = lax.rem(me_a - d + NA, NA)
            hit = jnp.logical_and(source // 2 == t, lane // 64 == source % 2)
            total = jnp.where(hit, slots[d - 1], total)
        for q in range(2):
            strip[q, t, pl.ds(0, 4), :] = total[4 * q:4 * q + 4]
            g4[q, t, my_pairs, :] = total[4 * q:4 * q + 4]
    for d in range(1, NB):
        send(strip.at[:, :, pl.ds(0, 4), :], g4.at[:, :, my_pairs, :], sendg, recvg, d, 0)
    for k, (dr, da) in enumerate(DIRS):
        send(x3.at[:, 0, pl.ds(BASE[3], 8), :], bs3.at[k], sendc, recvc, dr, da)
    wait_bytes(g4.at[:, :, pl.ds(WB, 60), :], sendg, recvg)

    down(r4, k4, g4, s4, c4, WB, 8, 4)
    restrict_pass(s4, WB, 4, mix, nat, g5, WB, c5, 0, 4, ((0, 1), (2, 3)))
    down(r5, k5, g5, s5, c5, WB, 4, 2)
    restrict_pass(s5, WB, 2, mix, nat, g6, WB, c6, 0, 2, ((0, 1),))
    spread_down(k6, g6, s6, c6, WB, 2, 1)
    restrict_pass(s6, WB, 1, mix, nat, g7, WB, c7, 0, 1, ((0, 0),))
    gr7, gk7, w7 = spread(read(g7.at[0], WB, 1), 4), spread(read(g7.at[1], WB, 1), 3), weights(c7, WB, 1)
    source = gr7
    for step in range(4):
        black = relaxed_spread(source, gk7, w7, 1, 3 if step < 3 else 2)
        red = relaxed_spread(black, gr7, w7, 0, 2 if step < 3 else 1)
        black = relaxed_spread(red, gk7, w7, 1, 1 if step < 3 else 0)
        if step < 3:
            source = spread(relaxed_spread(black, gr7, w7, 0, 0)[0], 4)
    put(r7, WB, red[0])
    put(k7, WB, black[0])

    def whole_up(rc, kc, blocks, nc, fine, plan):
        for k in range(blocks):
            unpair(rc, kc, WB + 8 * k, e_ref, FB + 16 * k, nc)
        prolong_pass(e_ref, f_ref, fa_ref, fb_ref, 0, 2 * blocks, fine, WB, 0, 2 * blocks, plan, True)

    whole_up(r7, k7, 1, 1, k6, ((0, 0),))
    spread_post(r6, k6, g6, c6, WB, 2, 1)
    whole_up(r6, k6, 2, 1, k5, ((0, 0), (0, 1)))
    post(r5, k5, g5, c5, WB, 4, 2)
    whole_up(r5, k5, 4, 2, k4, ((0, 0), (0, 1), (1, 0), (1, 1)))
    post(r4, k4, g4, c4, WB, 8, 4)

    def block(ref, da, wanted, at):
        b = lax.rem(me_a + da + NA, NA)
        x = ref[b // 2, at, :]
        return jnp.where(b % 2 == wanted, x, pltpu.roll(x, 64, 1))

    for k in range(2):
        at = pl.ds(WB - 4 + 4 * me_r + 8 * k, 8)
        seen = []
        for ref in (r4, k4):
            mine, rightward, leftward = block(ref, 0, 0, at), block(ref, 1, 1, at), block(ref, -1, 1, at)
            seen.append(jnp.where(lane < 64, mine, jnp.where(lane < 96, rightward, leftward)))
        q = FB - 8 + 16 * k
        win[0, pl.ds(q, 8, stride=2), :] = jnp.where(even, seen[0], seen[1])
        win[0, pl.ds(q + 1, 8, stride=2), :] = jnp.where(even, seen[1], seen[0])

    wait_bytes(bs3, sendc, recvc)
    for q in range(3):
        got = lambda dr, da: bs3[DIRS.index((-dr, -da)), q]
        x3[q, 0, pl.ds(BASE[3] - 8, 8), :] = got(-1, 0)
        x3[q, 0, pl.ds(BASE[3] + 8, 8), :] = got(1, 0)
        for dr in (-1, 0, 1):
            x3[q, 1, pl.ds(BASE[3] + 8 * dr, 8), :] = jnp.where(lane < 64, got(dr, 1), got(dr, -1))
    prolong_pass(win, f_ref, fa_ref, fb_ref, -8, 3, k3, BASE[3], -8, 3, ((0, 0), (0, 1)), False)
    clear_outside((k3, g3.at[0], g3.at[1]), 3, 2)
    spread_post(r3, k3, g3, c3, BASE[3] - 8, 3, 2)

    for k in range(2):
        unpair(r3, k3, BASE[3] - 4 + 8 * k, e_ref, FB - 8 + 16 * k, 2)
    prolong_pass(e_ref, f_ref, fa_ref, fb_ref, -8, 4, k2, BASE[2], -4, 3, ((0, 0), (0, 1), (1, 2)), False)
    clear_outside((k2,), 2, 3)
    post(r2, k2, g2, c2, BASE[2] - 4, 3, 3)

    for k in range(3):
        unpair(r2, k2, BASE[2] - 4 + 8 * k, e_ref, FB - 8 + 16 * k, 3)
    prolong_pass(e_ref, f_ref, fa_ref, fb_ref, -8, 6, k1, BASE[1], -4, 5, ((0, 0), (0, 1), (1, 0), (1, 1), (2, 2)), False)
    clear_outside((k1,), 1, 5)
    post(r1, k1, g1, c1, BASE[1] - 4, 5, 5)

    for k in range(5):
        unpair(r1, k1, BASE[1] - 4 + 8 * k, e_ref, FB - 8 + 16 * k, 5)
    plan = tuple((t // 2, t % 2) for t in range(8)) + ((4, 2),)
    prolong_pass(e_ref, f_ref, fa_ref, fb_ref, -8, 10, k0, BASE[0], -4, 9, plan, False)
    clear_outside((k0,), 0, 9)


def finish(x0, c0, sol_hbm, res_hbm, r, k, s, b, raw, out_sem):
    zero = jnp.zeros((8, 128), F32)
    for ref in (r, k):
        for t in range(9):
            ref[t, pl.ds(0, 8), :] = zero
            ref[t, pl.ds(ROWS[0] - 8, 8), :] = zero
    start, gr, gk = x0.at[0], x0.at[1], x0.at[2]
    half_sweep(r, start, gr, c0, 0, 4, 9, 9)
    half_sweep(k, r, gk, c0, 1, 4, 9, 9)
    half_sweep(r, k, gr, c0, 0, 4, 9, 9)
    half_sweep(k, r, gk, c0, 1, 4, 9, 9)

    def write(slot, red, black, hbm):
        for t in range(8):
            for q in range(8):
                unpair(red.at[pl.ds(t, 1)], black.at[pl.ds(t, 1)], BASE[0] + 8 * q, raw.at[slot, pl.ds(t, 1)], 16 * q, 1)
            copy = pltpu.make_async_copy(raw.at[slot, t], hbm.at[:, pl.ds(128 * t, 128)], out_sem)
            copy.start()

    write(0, r, k, sol_hbm)
    residual_pass(s, r, k, gr, c0, 0, BASE[0], 8, 9, tiles=range(8))
    residual_pass(b, k, r, gk, c0, 1, BASE[0], 8, 9, tiles=range(8))
    write(1, s, b, res_hbm)
    wait_bytes(raw, out_sem)


def local(right_side, guess):
    def vm(*shape):
        return pltpu.VMEM(shape, F32)

    levels = [vm(2, 8, 128, 128), vm(9, ROWS[0], 128), vm(9, ROWS[0], 128)]
    for l in (1, 2):
        n = OWN[l][1] + 1
        levels += [vm(2, n, ROWS[l], 128)] + [vm(n, ROWS[l], 128)] * 3
    levels += [vm(3, 2, ROWS[3], 128), vm(2, ROWS[3], 128), vm(2, ROWS[3], 128)]
    for l, (pairs, tiles) in enumerate(WHOLE):
        levels += [vm(2, tiles, pairs + 2 * WB, 128)] + [vm(tiles, pairs + 2 * WB, 128)] * (2 if l == 3 else 3)
    coefficients = [vm(10, r, 128) for r in ROWS[1:]] + [vm(10, pairs + 2 * WB, 128) for pairs, _ in WHOLE]
    buffers = [
        vm(2, 3, 8, 128), vm(4, 8, 128), vm(2, 3, 8, 128), vm(4, 8, 128),
        vm(2, 32, 128), vm(2, 32, 128), vm(4, 24, 128),
        vm(8, 3, 8, 128), vm(8, 128), vm(NA - 1, 8, 128), vm(2, 4, 8, 128),
    ]
    dma = pltpu.SemaphoreType.DMA
    sems = [dma] * 11
    natural = [vm(1, 48, 128), vm(5, 96, 128), vm(9, 96, 128), vm(5, 96, 128), vm(5, 96, 128), vm(9, 64, 128), vm(4, 64, 128)]
    held = (vm(3, 9, ROWS[0], 128), vm(10, ROWS[0], 128))
    inside = pl.BlockSpec(memory_space=pltpu.VMEM)
    outside = pl.BlockSpec(memory_space=pl.ANY)
    x0, c0 = pl.pallas_call(
        kernel,
        out_shape=held,
        in_specs=[outside] * 2,
        out_specs=(inside,) * 2,
        scratch_shapes=levels + natural + coefficients + buffers + sems,
        compiler_params=pltpu.CompilerParams(collective_id=0, has_side_effects=True),
    )(right_side, guess)
    x0, c0 = (pltpu.with_memory_space_constraint(x, pltpu.VMEM) for x in (x0, c0))
    block = jax.ShapeDtypeStruct(right_side.shape, F32)
    return pl.pallas_call(
        finish,
        out_shape=(block, block),
        in_specs=[inside] * 2,
        out_specs=(outside,) * 2,
        scratch_shapes=[vm(9, ROWS[0], 128)] * 4 + [vm(2, 8, 128, 128), dma],
    )(x0, c0)


def solution(mesh):
    placed = (P("rad", "ang"), P("rad", "ang"))
    return jax.shard_map(local, mesh=mesh, in_specs=placed, out_specs=placed, check_vma=False)
```

```python
import math

import jax
import jax.numpy as jnp
from jax import lax
from jax.experimental import pallas as pl
from jax.experimental.pallas import tpu as pltpu
from jax.sharding import PartitionSpec as P

MESH = pl.DeviceIdType.MESH
F32 = jnp.float32
NR, NT = 2048, 8192
NA, NB = 8, 16
OWN = ((64, 8), (32, 4), (16, 2), (8, 1))
BASE = (8, 24, 16, 16)
ROWS = tuple(o[0] + 2 * b for o, b in zip(OWN, BASE))
E0, E1 = 5, 18
WHOLE = ((64, 4), (32, 2), (16, 1), (8, 1))
WB = 8
DIRS = tuple((dr, da) for dr in (-1, 0, 1) for da in (-1, 0, 1) if dr or da)
CORNERS = tuple(d for d in DIRS if d[0] and d[1])
ORDER = tuple(sorted(DIRS, key=lambda d: (d[1] != 0, d[0] == 0)))
FB = 16


def grid_ids():
    sub = lax.broadcasted_iota(jnp.int32, (8, 128), 0)
    lane = lax.broadcasted_iota(jnp.int32, (8, 128), 1)
    return sub, lane


def ring_shift(tiles, lane):
    n = len(tiles)
    one = [pltpu.roll(x, 1, 1) for x in tiles]
    back = [pltpu.roll(x, 127, 1) for x in tiles]
    if n == 1:
        return one, back
    left = [jnp.where(lane == 0, one[t - 1], one[t]) for t in range(n)]
    right = [jnp.where(lane == 127, back[(t + 1) % n], back[t]) for t in range(n)]
    return left, right


def pick(x, index):
    return jnp.take_along_axis(x, index, axis=1, mode="promise_in_bounds")


def fill_coefficients(c_ref, count, base, first_row, total_rows, cells):
    h = 2.0 * math.pi / cells
    sub, lane = grid_ids()
    even = lane % 2 == 0

    def row_values(row):
        inside = jnp.logical_and(row >= 0, row < total_rows)
        r = 1.0 + (row.astype(F32) + 0.5) * h
        rr = r * r
        q = jnp.where(inside, 0.5 / (rr + 1.0), 0.0)
        half = (0.5 * h) * r
        return (rr + half) * q, (rr - half) * q, q, rr * q, 2.0 + 2.0 / rr

    for k in range(count):
        row = first_row + 2 * (8 * k - base + sub)
        o0, i0, a0, w0, c0 = row_values(row)
        o1, i1, a1, w1, c1 = row_values(row + 1)
        at = pl.ds(8 * k, 8)
        for j, (x, y) in enumerate(((o0, i1), (i0, o1), (a0, a1), (w0, w1), (c0, c1))):
            c_ref[j, at, :] = jnp.where(even, x, y)
            c_ref[5 + j, at, :] = jnp.where(even, y, x)


def relaxed(src, g, c_ref, colour, p, n, lane, tiles):
    at = pl.ds(p, 8)
    even = lane % 2 == 0
    first, second = (p - 1, p + 1) if colour == 0 else (p + 1, p - 1)
    x = {t: src[t, at, :] for t in sorted({(u + d) % n for u in tiles for d in (-1, 0, 1)})}
    one = {t: pltpu.roll(x[t], 1, 1) for t in sorted({(u + d) % n for u in tiles for d in (-1, 0)})}
    back = {t: pltpu.roll(x[t], 127, 1) for t in sorted({(u + d) % n for u in tiles for d in (0, 1)})}
    near, far, ang = (c_ref[5 * colour + k, at, :] for k in range(3))
    new = {}
    for t in tiles:
        left, right = one[t], back[t]
        if n > 1:
            left = jnp.where(lane == 0, one[(t - 1) % n], left)
            right = jnp.where(lane == 127, back[(t + 1) % n], right)
        other = jnp.where(even, src[t, pl.ds(first, 8), :], src[t, pl.ds(second, 8), :])
        new[t] = (g[t, at, :] + near * x[t]) + (far * other + ang * (left + right))
    return new


def half_sweep(dst, src, g, c_ref, colour, start, count, n, tiles=None):
    _, lane = grid_ids()
    for k in range(count):
        p = start + 8 * k
        for t, value in relaxed(src, g, c_ref, colour, p, n, lane, tiles or range(n)).items():
            dst[t, pl.ds(p, 8), :] = value


def residual_pass(dst, old, src, g, c_ref, colour, start, count, n, tiles=None):
    _, lane = grid_ids()
    for k in range(count):
        p = start + 8 * k
        c = c_ref[5 * colour + 4, pl.ds(p, 8), :]
        for t, value in relaxed(src, g, c_ref, colour, p, n, lane, tiles or range(n)).items():
            dst[t, pl.ds(p, 8), :] = c * (value - old[t, pl.ds(p, 8), :])


def fence(step):
    pl.when(lax.axis_index("rad") < NB)(step)


def mixed_block(s, p, n, lane):
    even = lane % 2 == 0
    r = [
        3.0 * s[t, pl.ds(p, 8), :] + jnp.where(even, s[t, pl.ds(p + 1, 8), :], s[t, pl.ds(p - 1, 8), :])
        for t in range(n)
    ]
    left, right = ring_shift(r, lane)
    return [3.0 * r[t] + jnp.where(even, left[t], right[t]) for t in range(n)]


def joined(a, b, lane):
    return jnp.where(lane % 2 == 0, a + pltpu.roll(a, 127, 1), b + pltpu.roll(b, 1, 1))


def gathered(x, lane):
    return pick(x, jnp.where(lane < 64, 2 * lane, 2 * lane - 127)) * 0.0625


def restrict_pass(s, fine_base, n, mix, nat, g, coarse_base, c_ref, start, count, pairs):
    _, lane = grid_ids()
    even = lane % 2 == 0
    for k in range(2 * count):
        for t, x in enumerate(mixed_block(s, fine_base + 2 * start + 8 * k, n, lane)):
            mix[t, pl.ds(8 * k, 8), :] = x

    def joins():
        for k in range(2 * count):
            at = pl.ds(8 * k, 8)
            for t, (a, b) in enumerate(pairs):
                nat[t, at, :] = joined(mix[a, at, :], mix[b, at, :], lane)

    fence(joins)

    def gathers():
        for k in range(2 * count):
            for t in range(len(pairs)):
                nat[t, pl.ds(8 * k, 8), :] = gathered(nat[t, pl.ds(8 * k, 8), :], lane)

    fence(gathers)
    for k in range(count):
        p = pl.ds(coarse_base + start + 8 * k, 8)
        red, black = c_ref[3, p, :], c_ref[8, p, :]
        for t in range(len(pairs)):
            x = nat[t, pl.ds(16 * k, 8, stride=2), :]
            y = nat[t, pl.ds(16 * k + 1, 8, stride=2), :]
            g[0, t, p, :] = jnp.where(even, x, y) * red
            g[1, t, p, :] = jnp.where(even, y, x) * black


def unpair(red, black, p, dst, q, n):
    _, lane = grid_ids()
    even = lane % 2 == 0
    for t in range(n):
        x, y = red[t, pl.ds(p, 8), :], black[t, pl.ds(p, 8), :]
        dst[t, pl.ds(q, 8, stride=2), :] = jnp.where(even, x, y)
        dst[t, pl.ds(q + 1, 8, stride=2), :] = jnp.where(even, y, x)


def prolong_pass(e, f, fa, fb, start, count, fine, fine_base, fine_start, fine_count, plan, sealed, own=0):
    sub, lane = grid_ids()
    me_r = lax.axis_index("rad")
    low = jnp.where(me_r == 0, 0, -64)
    high = jnp.where(me_r == NB - 1, own, 1024)
    even = lane % 2 == 0
    half = lane // 2
    kinds = (half, half + 64, jnp.where(lane < 64, half, half + 64))
    nc = max(source for source, _ in plan) + 1
    for k in range(count):
        at = pl.ds(FB + start + 8 * k, 8)
        x = [e[t, at, :] for t in range(nc)]
        left, right = ring_shift(x, lane)
        for t in range(nc):
            fa[t, at, :] = 0.75 * x[t] + 0.25 * left[t]
            fb[t, at, :] = 0.75 * x[t] + 0.25 * right[t]

    for wanted, index in enumerate(kinds):
        tiles = [(t, source) for t, (source, kind) in enumerate(plan) if kind == wanted]

        def gathers(tiles=tiles, index=index):
            for k in range(count):
                at = pl.ds(FB + start + 8 * k, 8)
                for t, source in tiles:
                    f[t, at, :] = jnp.where(even, pick(fa[source, at, :], index), pick(fb[source, at, :], index))

        if tiles and wanted < 2:
            fence(gathers)
        elif tiles:
            gathers()
    if sealed:
        for t in range(len(plan)):
            f[t, pl.ds(FB - 8, 8), :] = jnp.zeros((8, 128), F32)
            f[t, pl.ds(FB + 8 * count, 8), :] = jnp.zeros((8, 128), F32)
    for k in range(fine_count):
        i = fine_start + 8 * k
        at = pl.ds(fine_base + i, 8)
        for t in range(len(plan)):
            other = jnp.where(even, f[t, pl.ds(FB + i + 1, 8), :], f[t, pl.ds(FB + i - 1, 8), :])
            value = fine[t, at, :] + (0.75 * f[t, pl.ds(FB + i, 8), :] + 0.25 * other)
            if own and k in (0, fine_count - 1):
                value = jnp.where(jnp.logical_and(i + sub >= low, i + sub < high), value, 0.0)
            fine[t, at, :] = value


def wait_bytes(ref, *sems):
    for sem in sems:
        pltpu.make_async_copy(ref, ref, sem).wait()


def zero_rows(ref, n, start, count):
    for t in range(n):
        for k in range(count):
            ref[t, pl.ds(start + 8 * k, 8), :] = jnp.zeros((8, 128), F32)


def down(r, k, g, s, c, start, count, n):
    half_sweep(k, g.at[0], g.at[1], c, 1, start, count, n)
    half_sweep(r, k, g.at[0], c, 0, start, count, n)
    half_sweep(k, r, g.at[1], c, 1, start, count, n)
    residual_pass(s, r, k, g.at[0], c, 0, start, count, n)


def post(r, k, g, c, start, count, n):
    for _ in range(2):
        half_sweep(r, k, g.at[0], c, 0, start, count, n)
        half_sweep(k, r, g.at[1], c, 1, start, count, n)


def spread(tiles, reach):
    _, lane = grid_ids()
    n = len(tiles)
    out = {0: tiles}
    for d in [k for k in range(-reach, reach + 1) if k]:
        turned = [[pltpu.roll(x, -d % 128, 1) for x in blocks] for blocks in tiles]
        if n > 1:
            own = lane < 128 - d if d > 0 else lane >= -d
            step = 1 if d > 0 else -1
            turned = [
                [jnp.where(own, x, y) for x, y in zip(turned[t], turned[(t + step) % n])] for t in range(n)
            ]
        out[d] = turned
    return out


def weights(c_ref, start, count):
    return [
        [tuple(c_ref[5 * colour + k, pl.ds(start + 8 * b, 8), :] for k in range(3)) for b in range(count)]
        for colour in range(2)
    ]


def relaxed_spread(src, g, w, colour, reach):
    sub, lane = grid_ids()
    even = lane % 2 == 0
    out = {}
    for d in range(-reach, reach + 1):
        kind = (colour + d) % 2
        out[d] = []
        for t, x in enumerate(src[d]):
            one = [pltpu.roll(y, 1, 0) for y in x]
            back = [pltpu.roll(y, 7, 0) for y in x]
            n = len(x)
            new = []
            for b in range(n):
                before = jnp.where(sub == 0, one[b - 1] if b else 0.0, one[b])
                after = jnp.where(sub == 7, back[b + 1] if b < n - 1 else 0.0, back[b])
                near, far, ang = w[kind][b]
                other = jnp.where(even, before, after) if kind == 0 else jnp.where(even, after, before)
                new.append((g[d][t][b] + near * x[b]) + (far * other + ang * (src[d - 1][t][b] + src[d + 1][t][b])))
            out[d].append(new)
    return out


def read(ref, start, count, n=1):
    return [[ref[t, pl.ds(start + 8 * b, 8), :] for b in range(count)] for t in range(n)]


def put(ref, start, tiles):
    for t, blocks in enumerate(tiles):
        for b, x in enumerate(blocks):
            ref[t, pl.ds(start + 8 * b, 8), :] = x


def spread_down(k, g, s, c_ref, start, count, n):
    w = weights(c_ref, start, count)
    gr, gk = spread(read(g.at[0], start, count, n), 4), spread(read(g.at[1], start, count, n), 3)
    black = relaxed_spread(gr, gk, w, 1, 3)
    red = relaxed_spread(black, gr, w, 0, 2)
    black = relaxed_spread(red, gk, w, 1, 1)
    put(k, start, black[0])
    new = relaxed_spread(black, gr, w, 0, 0)[0]
    for t in range(n):
        for b in range(count):
            at = pl.ds(start + 8 * b, 8)
            s[t, at, :] = c_ref[4, at, :] * (new[t][b] - red[0][t][b])


def spread_post(r, k, g, c_ref, start, count, n):
    w = weights(c_ref, start, count)
    gr, gk = spread(read(g.at[0], start, count, n), 3), spread(read(g.at[1], start, count, n), 2)
    red = relaxed_spread(spread(read(k, start, count, n), 4), gr, w, 0, 3)
    black = relaxed_spread(red, gk, w, 1, 2)
    red = relaxed_spread(black, gr, w, 0, 1)
    put(r, start, red[0])
    put(k, start, relaxed_spread(red, gk, w, 1, 0)[0])


def kernel(
    right_hbm, guess_hbm, x0, c0,
    raw, r0, s0, g1, r1, k1, s1, g2, r2, k2, s2, x3, r3, s3,
    g4, r4, k4, s4, g5, r5, k5, s5, g6, r6, k6, s6, g7, r7, k7,
    win, e_ref, f_ref, fa_ref, fb_ref, mix, nat, c1, c2, c3, c4, c5, c6, c7,
    pk0, pc0, rp0, rd0, pk1, rl1, rd1, bs3, own4, slots, strip,
    load_sem, send0, recv0, send1, recv1, sendc, recvc, senda, recva, sendg, recvg,
):
    me_a, me_r = lax.axis_index("ang"), lax.axis_index("rad")

    def device(dr, da):
        return {"ang": lax.rem(me_a + da + NA, NA), "rad": lax.rem(me_r + dr + NB, NB)}

    barrier = pltpu.get_barrier_semaphore()
    partners = list(DIRS) + [(0, d) for d in range(2, NA - 1)] + [(d, 0) for d in range(2, NB - 1)]
    for dr, da in partners:
        pl.semaphore_signal(barrier, inc=1, device_id=device(dr, da), device_id_type=MESH)

    loads = []
    for t in range(8):
        for k, src in ((0, guess_hbm), (1, right_hbm)):
            loads.append(pltpu.make_async_copy(
                src.at[:, pl.ds(128 * t, 128)], raw.at[k, t], load_sem))
    for copy in loads:
        copy.start()

    zero = jnp.zeros((8, 128), F32)
    k0, g0 = x0.at[0], x0.at[pl.ds(1, 2)]
    k3, g3 = x3.at[0], x3.at[pl.ds(1, 2)]
    edges = [(r, 0) for r in (r0, s0)] + [(r, 1) for r in (r1, k1, s1)]
    edges += [(r, 2) for r in (g2.at[0], g2.at[1], r2, k2, s2)]
    edges += [(r, 3) for r in (k3, x3.at[1], x3.at[2], r3, s3)]
    for ref, l in edges:
        depth = 1 if l < 2 else 2
        for t in range(OWN[l][1] + 1):
            for d in range(depth):
                ref[t, pl.ds(8 * d, 8), :] = zero
                ref[t, pl.ds(ROWS[l] - 8 - 8 * d, 8), :] = zero
    for l, refs in enumerate(((g4, r4, k4, s4), (g5, r5, k5, s5), (g6, r6, k6, s6), (g7, r7, k7))):
        for ref in refs:
            for x in ((ref.at[0], ref.at[1]) if len(ref.shape) == 4 else (ref,)):
                for t in range(WHOLE[l][1]):
                    x[t, pl.ds(0, 8), :] = zero
                    x[t, pl.ds(WB + WHOLE[l][0], 8), :] = zero
    zero_rows(win, 1, 0, 6)
    for t in range(9):
        for d in (0, 1, 10, 11):
            f_ref[t, pl.ds(8 * d, 8), :] = zero
    for l, c_ref in enumerate((c0, c1, c2, c3)):
        fill_coefficients(c_ref, ROWS[l] // 8, BASE[l], me_r * (2 * OWN[l][0]), NR >> l, NT >> l)
    for l, c_ref in enumerate((c4, c5, c6, c7)):
        fill_coefficients(c_ref, WHOLE[l][0] // 8 + 2, WB, 0, 2 * WHOLE[l][0], NT >> (l + 4))

    sub, lane = grid_ids()
    even = lane % 2 == 0

    def send(src, dst, send_sem, recv_sem, dr, da):
        pltpu.make_async_remote_copy(
            src_ref=src, dst_ref=dst, send_sem=send_sem, recv_sem=recv_sem,
            device_id=device(dr, da), device_id_type=MESH).start()

    def edge(l, dr, width):
        if dr < 0:
            return pl.ds(BASE[l], width), pl.ds(BASE[l] + OWN[l][0], width)
        return pl.ds(BASE[l] + OWN[l][0] - width, width), pl.ds(BASE[l] - width, width)

    wait_bytes(raw, load_sem)
    for k in range(8):
        at = pl.ds(BASE[0] + 8 * k, 8)
        red, black = c0[3, at, :], c0[8, at, :]
        for t in range(8):
            k0[t, at, :] = jnp.where(
                even, raw[0, t, pl.ds(16 * k + 1, 8, stride=2), :], raw[0, t, pl.ds(16 * k, 8, stride=2), :])
            x = raw[1, t, pl.ds(16 * k, 8, stride=2), :]
            y = raw[1, t, pl.ds(16 * k + 1, 8, stride=2), :]
            g0[0, t, at, :] = jnp.where(even, x, y) * red
            g0[1, t, at, :] = jnp.where(even, y, x) * black
    for q in range(3):
        for side, (tile, first) in enumerate(((0, 0), (7, 112))):
            total = None
            for b in range(8):
                x = x0[q, tile, pl.ds(BASE[0] + 8 * b, 8), :]
                shift = (16 * b - first) % 128
                x = pltpu.roll(x, shift, 1) if shift else x
                total = x if total is None else jnp.where(lane // 16 == b, x, total)
            pk0[side, q, :, :] = total
    for c, (dr, da) in enumerate(CORNERS):
        rows = pl.ds(BASE[0] if dr < 0 else BASE[0] + OWN[0][0] - 8, 8)
        tile, first = (0, 0) if da < 0 else (7, 112)
        total = None
        for q in range(3):
            x = x0[q, tile, rows, :]
            shift = (16 * q - first) % 128
            x = pltpu.roll(x, shift, 1) if shift else x
            total = x if total is None else jnp.where(lane // 16 == q, x, total)
        pc0[c, :, :] = total
    pl.semaphore_wait(barrier, len(partners))

    for dr, da in ORDER:
        mine, theirs = edge(0, dr, E0) if dr else (None, None)
        if da == 0:
            send(x0.at[0, pl.ds(0, 8), mine, :], x0.at[0, pl.ds(0, 8), theirs, :], send0, recv0, dr, da)
            mine, theirs = edge(0, dr, 4)
            send(x0.at[pl.ds(1, 2), pl.ds(0, 8), mine, :], x0.at[pl.ds(1, 2), pl.ds(0, 8), theirs, :],
                 send0, recv0, dr, da)
        elif dr == 0:
            side = 0 if da < 0 else 1
            send(pk0.at[side], rp0.at[side], send0, recv0, dr, da)
        else:
            c = CORNERS.index((dr, da))
            send(pc0.at[c, pl.ds(0 if dr < 0 else 8 - E0, E0), :], rd0.at[c, pl.ds(0, E0), :], send0, recv0, dr, da)
    wait_bytes(f_ref.at[pl.ds(0, 4), pl.ds(0, 69), :], send0, recv0)

    def clear_outside(refs, l, n, depth=1):
        @pl.when(me_r == 0)
        def _():
            for ref in refs:
                zero_rows(ref, n, BASE[l] - 8 * depth, depth)

        @pl.when(me_r == NB - 1)
        def _():
            for ref in refs:
                zero_rows(ref, n, BASE[l] + OWN[l][0], depth)

    for q in range(3):
        from_left, from_right = rp0[1, q], rp0[0, q]
        for b in range(8):
            shift_r, shift_l = (-16 * b) % 128, (112 - 16 * b) % 128
            x = pltpu.roll(from_right, shift_r, 1) if shift_r else from_right
            y = pltpu.roll(from_left, shift_l, 1) if shift_l else from_left
            x0[q, 8, pl.ds(BASE[0] + 8 * b, 8), :] = jnp.where(lane < 64, x, y)
        for dr in (-1, 1):
            start = BASE[0] - E0 if dr < 0 else BASE[0] + OWN[0][0]
            x = rd0[CORNERS.index((-dr, -1)), :, :]
            y = pltpu.roll(rd0[CORNERS.index((-dr, 1)), :, :], 112 - 16 * q, 1)
            x = pltpu.roll(x, 128 - 16 * q, 1) if q else x
            x0[q, 8, pl.ds(start, E0), :] = jnp.where(lane < 64, x, y)[:E0]
    clear_outside((k0, g0.at[0], g0.at[1]), 0, 9)

    for _ in range(2):
        half_sweep(r0, k0, g0.at[0], c0, 0, 4, 9, 9)
        half_sweep(k0, r0, g0.at[1], c0, 1, 4, 9, 9)
    residual_pass(s0, r0, k0, g0.at[0], c0, 0, 4, 9, 9)
    restrict_pass(s0, BASE[0], 9, mix, nat, g1, BASE[1], c1, 0, 4, ((0, 1), (2, 3), (4, 5), (6, 7)))

    for b in range(4):
        at, own = pl.ds(8 * b, 8), pl.ds(BASE[1] + 8 * b, 8)
        pk1[0, at, :] = jnp.where(lane < 64, g1[0, 0, own, :], pltpu.roll(g1[1, 0, own, :], 64, 1))
        pk1[1, at, :] = jnp.where(lane < 64, pltpu.roll(g1[0, 3, own, :], 64, 1), g1[1, 3, own, :])
    for dr, da in ORDER:
        side = 0 if da < 0 else 1
        if da == 0:
            mine, theirs = edge(1, dr, E1)
            send(g1.at[:, pl.ds(0, 4), mine, :], g1.at[:, pl.ds(0, 4), theirs, :], send1, recv1, dr, da)
        elif dr == 0:
            send(pk1.at[side], rl1.at[side], send1, recv1, dr, da)
        else:
            send(pk1.at[side, pl.ds(0 if dr < 0 else 32 - E1, E1), :],
                 rd1.at[CORNERS.index((dr, da)), pl.ds(0, E1), :], send1, recv1, dr, da)
    wait_bytes(f_ref.at[pl.ds(0, 8), pl.ds(0, 53), :], send1, recv1)

    def merge_edges(row, size, from_right, from_left):
        low = lane[:size] < 64
        g1[0, 4, pl.ds(row, size), :] = jnp.where(low, from_right, pltpu.roll(from_left, 64, 1))
        g1[1, 4, pl.ds(row, size), :] = jnp.where(low, pltpu.roll(from_right, 64, 1), from_left)

    for b in range(4):
        merge_edges(BASE[1] + 8 * b, 8, rl1[0, pl.ds(8 * b, 8), :], rl1[1, pl.ds(8 * b, 8), :])
    for dr in (-1, 1):
        start = BASE[1] - E1 if dr < 0 else BASE[1] + OWN[1][0]
        right, left = CORNERS.index((-dr, -1)), CORNERS.index((-dr, 1))
        for first in (0, 8, 16):
            size = 8 if first < 16 else 2
            merge_edges(start + first, size, rd1[right, pl.ds(first, size), :], rd1[left, pl.ds(first, size), :])
    for q in range(2):
        for dr in (-1, 1):
            rest = BASE[1] - E1 - 3 if dr < 0 else BASE[1] + OWN[1][0] + E1
            for t in range(5):
                g1[q, t, pl.ds(rest, 3), :] = jnp.zeros((3, 128), F32)
    clear_outside((g1.at[0], g1.at[1]), 1, 5, 3)

    down(r1, k1, g1, s1, c1, BASE[1] - 20, 9, 5)
    restrict_pass(s1, BASE[1], 5, mix, nat, g2, BASE[2], c2, -8, 4, ((0, 1), (2, 3), (4, 4)))
    down(r2, k2, g2, s2, c2, BASE[2] - 8, 4, 3)
    restrict_pass(s2, BASE[2], 3, mix, nat, g3, BASE[3], c3, -4, 2, ((0, 1), (2, 2)))
    spread_down(k3, g3, s3, c3, BASE[3] - 4, 2, 2)

    nat[0, pl.ds(0, 8), :] = gathered(joined(*mixed_block(s3, BASE[3], 2, lane)[:1] * 2, lane), lane)
    x, y = nat[0, pl.ds(0, 4, stride=2), :], nat[0, pl.ds(1, 4, stride=2), :]
    my_pairs = pl.ds(WB + 4 * me_r, 4)
    own4[pl.ds(0, 4), :] = jnp.where(even[:4], x, y) * c4[3, my_pairs, :]
    own4[pl.ds(4, 4), :] = jnp.where(even[:4], y, x) * c4[8, my_pairs, :]
    for d in range(1, NA):
        send(own4, slots.at[d - 1], senda, recva, 0, d)
    wait_bytes(slots, senda, recva)
    for t in range(4):
        total = own4[...]
        for d in range(1, NA):
            source = lax.rem(me_a - d + NA, NA)
            hit = jnp.logical_and(source // 2 == t, lane // 64 == source % 2)
            total = jnp.where(hit, slots[d - 1], total)
        for q in range(2):
            strip[q, t, pl.ds(0, 4), :] = total[4 * q:4 * q + 4]
            g4[q, t, my_pairs, :] = total[4 * q:4 * q + 4]
    for d in range(1, NB):
        send(strip.at[:, :, pl.ds(0, 4), :], g4.at[:, :, my_pairs, :], sendg, recvg, d, 0)
    for k, (dr, da) in enumerate(DIRS):
        send(x3.at[:, 0, pl.ds(BASE[3], 8), :], bs3.at[k], sendc, recvc, dr, da)
    wait_bytes(g4.at[:, :, pl.ds(WB, 60), :], sendg, recvg)

    down(r4, k4, g4, s4, c4, WB, 8, 4)
    restrict_pass(s4, WB, 4, mix, nat, g5, WB, c5, 0, 4, ((0, 1), (2, 3)))
    down(r5, k5, g5, s5, c5, WB, 4, 2)
    restrict_pass(s5, WB, 2, mix, nat, g6, WB, c6, 0, 2, ((0, 1),))
    spread_down(k6, g6, s6, c6, WB, 2, 1)
    restrict_pass(s6, WB, 1, mix, nat, g7, WB, c7, 0, 1, ((0, 0),))
    gr7, gk7, w7 = spread(read(g7.at[0], WB, 1), 4), spread(read(g7.at[1], WB, 1), 3), weights(c7, WB, 1)
    source = gr7
    for step in range(4):
        black = relaxed_spread(source, gk7, w7, 1, 3 if step < 3 else 2)
        red = relaxed_spread(black, gr7, w7, 0, 2 if step < 3 else 1)
        black = relaxed_spread(red, gk7, w7, 1, 1 if step < 3 else 0)
        if step < 3:
            source = spread(relaxed_spread(black, gr7, w7, 0, 0)[0], 4)
    put(r7, WB, red[0])
    put(k7, WB, black[0])

    def whole_up(rc, kc, blocks, nc, fine, plan):
        for k in range(blocks):
            unpair(rc, kc, WB + 8 * k, e_ref, FB + 16 * k, nc)
        prolong_pass(e_ref, f_ref, fa_ref, fb_ref, 0, 2 * blocks, fine, WB, 0, 2 * blocks, plan, True)

    whole_up(r7, k7, 1, 1, k6, ((0, 0),))
    spread_post(r6, k6, g6, c6, WB, 2, 1)
    whole_up(r6, k6, 2, 1, k5, ((0, 0), (0, 1)))
    post(r5, k5, g5, c5, WB, 4, 2)
    whole_up(r5, k5, 4, 2, k4, ((0, 0), (0, 1), (1, 0), (1, 1)))
    post(r4, k4, g4, c4, WB, 8, 4)

    def block(ref, da, wanted, at):
        b = lax.rem(me_a + da + NA, NA)
        x = ref[b // 2, at, :]
        return jnp.where(b % 2 == wanted, x, pltpu.roll(x, 64, 1))

    for k in range(2):
        at = pl.ds(WB - 4 + 4 * me_r + 8 * k, 8)
        seen = []
        for ref in (r4, k4):
            mine, rightward, leftward = block(ref, 0, 0, at), block(ref, 1, 1, at), block(ref, -1, 1, at)
            seen.append(jnp.where(lane < 64, mine, jnp.where(lane < 96, rightward, leftward)))
        q = FB - 8 + 16 * k
        win[0, pl.ds(q, 8, stride=2), :] = jnp.where(even, seen[0], seen[1])
        win[0, pl.ds(q + 1, 8, stride=2), :] = jnp.where(even, seen[1], seen[0])

    wait_bytes(bs3, sendc, recvc)
    for q in range(3):
        keep = {-1: jnp.where(me_r == 0, 0.0, 1.0), 0: 1.0, 1: jnp.where(me_r == NB - 1, 0.0, 1.0)}
        got = lambda dr, da: bs3[DIRS.index((-dr, -da)), q] * keep[dr]
        x3[q, 0, pl.ds(BASE[3] - 8, 8), :] = got(-1, 0)
        x3[q, 0, pl.ds(BASE[3] + 8, 8), :] = got(1, 0)
        for dr in (-1, 0, 1):
            x3[q, 1, pl.ds(BASE[3] + 8 * dr, 8), :] = jnp.where(lane < 64, got(dr, 1), got(dr, -1))
    prolong_pass(win, f_ref, fa_ref, fb_ref, -8, 3, k3, BASE[3], -8, 3, ((0, 0), (0, 1)), False, OWN[3][0])
    spread_post(r3, k3, g3, c3, BASE[3] - 8, 3, 2)

    for k in range(2):
        unpair(r3, k3, BASE[3] - 4 + 8 * k, e_ref, FB - 8 + 16 * k, 2)
    prolong_pass(e_ref, f_ref, fa_ref, fb_ref, -8, 4, k2, BASE[2], -4, 3, ((0, 0), (0, 1), (1, 2)), False, OWN[2][0])
    post(r2, k2, g2, c2, BASE[2] - 4, 3, 3)

    for k in range(3):
        unpair(r2, k2, BASE[2] - 4 + 8 * k, e_ref, FB - 8 + 16 * k, 3)
    prolong_pass(e_ref, f_ref, fa_ref, fb_ref, -8, 6, k1, BASE[1], -4, 5, ((0, 0), (0, 1), (1, 0), (1, 1), (2, 2)), False, OWN[1][0])
    post(r1, k1, g1, c1, BASE[1] - 4, 5, 5)

    for k in range(5):
        unpair(r1, k1, BASE[1] - 4 + 8 * k, e_ref, FB - 8 + 16 * k, 5)
    plan = tuple((t // 2, t % 2) for t in range(8)) + ((4, 2),)
    prolong_pass(e_ref, f_ref, fa_ref, fb_ref, -8, 10, k0, BASE[0], -4, 9, plan, False, OWN[0][0])


def finish(x0, c0, sol_hbm, res_hbm, r, k, s, b, raw, out_sem):
    zero = jnp.zeros((8, 128), F32)
    for ref in (r, k):
        for t in range(9):
            ref[t, pl.ds(0, 8), :] = zero
            ref[t, pl.ds(ROWS[0] - 8, 8), :] = zero
    start, gr, gk = x0.at[0], x0.at[1], x0.at[2]
    half_sweep(r, start, gr, c0, 0, 4, 9, 9)
    half_sweep(k, r, gk, c0, 1, 4, 9, 9)
    half_sweep(r, k, gr, c0, 0, 4, 9, 9)
    half_sweep(k, r, gk, c0, 1, 4, 9, 9)

    def write(slot, red, black, hbm):
        for t in range(8):
            for q in range(8):
                unpair(red.at[pl.ds(t, 1)], black.at[pl.ds(t, 1)], BASE[0] + 8 * q, raw.at[slot, pl.ds(t, 1)], 16 * q, 1)
            copy = pltpu.make_async_copy(raw.at[slot, t], hbm.at[:, pl.ds(128 * t, 128)], out_sem)
            copy.start()

    write(0, r, k, sol_hbm)
    residual_pass(s, r, k, gr, c0, 0, BASE[0], 8, 9, tiles=range(8))
    residual_pass(b, k, r, gk, c0, 1, BASE[0], 8, 9, tiles=range(8))
    write(1, s, b, res_hbm)
    wait_bytes(raw, out_sem)


def local(right_side, guess):
    def vm(*shape):
        return pltpu.VMEM(shape, F32)

    levels = [vm(2, 8, 128, 128), vm(9, ROWS[0], 128), vm(9, ROWS[0], 128)]
    for l in (1, 2):
        n = OWN[l][1] + 1
        levels += [vm(2, n, ROWS[l], 128)] + [vm(n, ROWS[l], 128)] * 3
    levels += [vm(3, 2, ROWS[3], 128), vm(2, ROWS[3], 128), vm(2, ROWS[3], 128)]
    for l, (pairs, tiles) in enumerate(WHOLE):
        levels += [vm(2, tiles, pairs + 2 * WB, 128)] + [vm(tiles, pairs + 2 * WB, 128)] * (2 if l == 3 else 3)
    coefficients = [vm(10, r, 128) for r in ROWS[1:]] + [vm(10, pairs + 2 * WB, 128) for pairs, _ in WHOLE]
    buffers = [
        vm(2, 3, 8, 128), vm(4, 8, 128), vm(2, 3, 8, 128), vm(4, 8, 128),
        vm(2, 32, 128), vm(2, 32, 128), vm(4, 24, 128),
        vm(8, 3, 8, 128), vm(8, 128), vm(NA - 1, 8, 128), vm(2, 4, 8, 128),
    ]
    dma = pltpu.SemaphoreType.DMA
    sems = [dma] * 11
    natural = [vm(1, 48, 128), vm(5, 96, 128), vm(9, 96, 128), vm(5, 96, 128), vm(5, 96, 128), vm(9, 64, 128), vm(4, 64, 128)]
    held = (vm(3, 9, ROWS[0], 128), vm(10, ROWS[0], 128))
    inside = pl.BlockSpec(memory_space=pltpu.VMEM)
    outside = pl.BlockSpec(memory_space=pl.ANY)
    x0, c0 = pl.pallas_call(
        kernel,
        out_shape=held,
        in_specs=[outside] * 2,
        out_specs=(inside,) * 2,
        scratch_shapes=levels + natural + coefficients + buffers + sems,
        compiler_params=pltpu.CompilerParams(collective_id=0, has_side_effects=True),
    )(right_side, guess)
    x0, c0 = (pltpu.with_memory_space_constraint(x, pltpu.VMEM) for x in (x0, c0))
    block = jax.ShapeDtypeStruct(right_side.shape, F32)
    return pl.pallas_call(
        finish,
        out_shape=(block, block),
        in_specs=[inside] * 2,
        out_specs=(outside,) * 2,
        scratch_shapes=[vm(9, ROWS[0], 128)] * 4 + [vm(2, 8, 128, 128), dma],
    )(x0, c0)


def solution(mesh):
    placed = (P("rad", "ang"), P("rad", "ang"))
    return jax.shard_map(local, mesh=mesh, in_specs=placed, out_specs=placed, check_vma=False)
```

```python
import math

import jax
import jax.numpy as jnp
from jax import lax
from jax.experimental import pallas as pl
from jax.experimental.pallas import tpu as pltpu
from jax.sharding import PartitionSpec as P

MESH = pl.DeviceIdType.MESH
F32 = jnp.float32
NR, NT = 2048, 8192
NA, NB = 8, 16
OWN = ((64, 8), (32, 4), (16, 2), (8, 1))
BASE = (8, 24, 16, 16)
ROWS = tuple(o[0] + 2 * b for o, b in zip(OWN, BASE))
E0, E1 = 5, 18
WHOLE = ((64, 4), (32, 2), (16, 1), (8, 1))
WB = 8
DIRS = tuple((dr, da) for dr in (-1, 0, 1) for da in (-1, 0, 1) if dr or da)
CORNERS = tuple(d for d in DIRS if d[0] and d[1])
ORDER = tuple(sorted(DIRS, key=lambda d: (d[1] != 0, d[0] == 0)))
FB = 16


def grid_ids():
    sub = lax.broadcasted_iota(jnp.int32, (8, 128), 0)
    lane = lax.broadcasted_iota(jnp.int32, (8, 128), 1)
    return sub, lane


def ring_shift(tiles, lane):
    n = len(tiles)
    one = [pltpu.roll(x, 1, 1) for x in tiles]
    back = [pltpu.roll(x, 127, 1) for x in tiles]
    if n == 1:
        return one, back
    left = [jnp.where(lane == 0, one[t - 1], one[t]) for t in range(n)]
    right = [jnp.where(lane == 127, back[(t + 1) % n], back[t]) for t in range(n)]
    return left, right


def pick(x, index):
    return jnp.take_along_axis(x, index, axis=1, mode="promise_in_bounds")


def fill_coefficients(c_ref, count, base, first_row, total_rows, cells):
    h = 2.0 * math.pi / cells
    sub, lane = grid_ids()
    even = lane % 2 == 0

    def row_values(row):
        inside = jnp.logical_and(row >= 0, row < total_rows)
        r = 1.0 + (row.astype(F32) + 0.5) * h
        rr = r * r
        q = jnp.where(inside, 0.5 / (rr + 1.0), 0.0)
        half = (0.5 * h) * r
        return (rr + half) * q, (rr - half) * q, q, rr * q, 2.0 + 2.0 / rr

    for k in range(count):
        row = first_row + 2 * (8 * k - base + sub)
        o0, i0, a0, w0, c0 = row_values(row)
        o1, i1, a1, w1, c1 = row_values(row + 1)
        at = pl.ds(8 * k, 8)
        for j, (x, y) in enumerate(((o0, i1), (i0, o1), (a0, a1), (w0, w1), (c0, c1))):
            c_ref[j, at, :] = jnp.where(even, x, y)
            c_ref[5 + j, at, :] = jnp.where(even, y, x)


def relaxed(src, g, c_ref, colour, p, n, lane, tiles):
    at = pl.ds(p, 8)
    even = lane % 2 == 0
    first, second = (p - 1, p + 1) if colour == 0 else (p + 1, p - 1)
    x = {t: src[t, at, :] for t in sorted({(u + d) % n for u in tiles for d in (-1, 0, 1)})}
    one = {t: pltpu.roll(x[t], 1, 1) for t in sorted({(u + d) % n for u in tiles for d in (-1, 0)})}
    back = {t: pltpu.roll(x[t], 127, 1) for t in sorted({(u + d) % n for u in tiles for d in (0, 1)})}
    near, far, ang = (c_ref[5 * colour + k, at, :] for k in range(3))
    new = {}
    for t in tiles:
        left, right = one[t], back[t]
        if n > 1:
            left = jnp.where(lane == 0, one[(t - 1) % n], left)
            right = jnp.where(lane == 127, back[(t + 1) % n], right)
        other = jnp.where(even, src[t, pl.ds(first, 8), :], src[t, pl.ds(second, 8), :])
        new[t] = (g[t, at, :] + near * x[t]) + (far * other + ang * (left + right))
    return new


def half_sweep(dst, src, g, c_ref, colour, start, count, n, tiles=None):
    _, lane = grid_ids()
    for k in range(count):
        p = start + 8 * k
        for t, value in relaxed(src, g, c_ref, colour, p, n, lane, tiles or range(n)).items():
            dst[t, pl.ds(p, 8), :] = value


def residual_pass(dst, old, src, g, c_ref, colour, start, count, n, tiles=None):
    _, lane = grid_ids()
    for k in range(count):
        p = start + 8 * k
        c = c_ref[5 * colour + 4, pl.ds(p, 8), :]
        for t, value in relaxed(src, g, c_ref, colour, p, n, lane, tiles or range(n)).items():
            dst[t, pl.ds(p, 8), :] = c * (value - old[t, pl.ds(p, 8), :])


def fence(step):
    pl.when(lax.axis_index("rad") < NB)(step)


def mixed_block(s, p, n, lane):
    even = lane % 2 == 0
    r = [
        3.0 * s[t, pl.ds(p, 8), :] + jnp.where(even, s[t, pl.ds(p + 1, 8), :], s[t, pl.ds(p - 1, 8), :])
        for t in range(n)
    ]
    left, right = ring_shift(r, lane)
    return [3.0 * r[t] + jnp.where(even, left[t], right[t]) for t in range(n)]


def joined(a, b, lane):
    return jnp.where(lane % 2 == 0, a + pltpu.roll(a, 127, 1), b + pltpu.roll(b, 1, 1))


def gathered(x, lane):
    return pick(x, jnp.where(lane < 64, 2 * lane, 2 * lane - 127)) * 0.0625


def restrict_pass(s, fine_base, n, mix, nat, g, coarse_base, c_ref, start, count, pairs):
    _, lane = grid_ids()
    even = lane % 2 == 0
    for k in range(2 * count):
        for t, x in enumerate(mixed_block(s, fine_base + 2 * start + 8 * k, n, lane)):
            mix[t, pl.ds(8 * k, 8), :] = x

    def joins():
        for k in range(2 * count):
            at = pl.ds(8 * k, 8)
            for t, (a, b) in enumerate(pairs):
                nat[t, at, :] = joined(mix[a, at, :], mix[b, at, :], lane)

    fence(joins)

    def gathers():
        for k in range(2 * count):
            for t in range(len(pairs)):
                nat[t, pl.ds(8 * k, 8), :] = gathered(nat[t, pl.ds(8 * k, 8), :], lane)

    fence(gathers)
    for k in range(count):
        p = pl.ds(coarse_base + start + 8 * k, 8)
        red, black = c_ref[3, p, :], c_ref[8, p, :]
        for t in range(len(pairs)):
            x = nat[t, pl.ds(16 * k, 8, stride=2), :]
            y = nat[t, pl.ds(16 * k + 1, 8, stride=2), :]
            g[0, t, p, :] = jnp.where(even, x, y) * red
            g[1, t, p, :] = jnp.where(even, y, x) * black


def unpair(red, black, p, dst, q, n):
    _, lane = grid_ids()
    even = lane % 2 == 0
    for t in range(n):
        x, y = red[t, pl.ds(p, 8), :], black[t, pl.ds(p, 8), :]
        dst[t, pl.ds(q, 8, stride=2), :] = jnp.where(even, x, y)
        dst[t, pl.ds(q + 1, 8, stride=2), :] = jnp.where(even, y, x)


def prolong_pass(e, f, fa, fb, start, count, fine, fine_base, fine_start, fine_count, plan, sealed, own=0):
    sub, lane = grid_ids()
    me_r = lax.axis_index("rad")
    low = jnp.where(me_r == 0, 0, -64)
    high = jnp.where(me_r == NB - 1, own, 1024)
    even = lane % 2 == 0
    half = lane // 2
    kinds = (half, half + 64, jnp.where(lane < 64, half, half + 64))
    nc = max(source for source, _ in plan) + 1
    for k in range(count):
        at = pl.ds(FB + start + 8 * k, 8)
        x = [e[t, at, :] for t in range(nc)]
        left, right = ring_shift(x, lane)
        for t in range(nc):
            fa[t, at, :] = 0.75 * x[t] + 0.25 * left[t]
            fb[t, at, :] = 0.75 * x[t] + 0.25 * right[t]

    for wanted, index in enumerate(kinds):
        tiles = [(t, source) for t, (source, kind) in enumerate(plan) if kind == wanted]

        def gathers(tiles=tiles, index=index):
            for k in range(count):
                at = pl.ds(FB + start + 8 * k, 8)
                for t, source in tiles:
                    f[t, at, :] = jnp.where(even, pick(fa[source, at, :], index), pick(fb[source, at, :], index))

        if tiles and wanted < 2:
            fence(gathers)
        elif tiles:
            gathers()
    if sealed:
        for t in range(len(plan)):
            f[t, pl.ds(FB - 8, 8), :] = jnp.zeros((8, 128), F32)
            f[t, pl.ds(FB + 8 * count, 8), :] = jnp.zeros((8, 128), F32)
    for k in range(fine_count):
        i = fine_start + 8 * k
        at = pl.ds(fine_base + i, 8)
        for t in range(len(plan)):
            other = jnp.where(even, f[t, pl.ds(FB + i + 1, 8), :], f[t, pl.ds(FB + i - 1, 8), :])
            value = fine[t, at, :] + (0.75 * f[t, pl.ds(FB + i, 8), :] + 0.25 * other)
            if own and k in (0, fine_count - 1):
                value = jnp.where(jnp.logical_and(i + sub >= low, i + sub < high), value, 0.0)
            fine[t, at, :] = value


def wait_bytes(ref, *sems):
    for sem in sems:
        pltpu.make_async_copy(ref, ref, sem).wait()


def zero_rows(ref, n, start, count):
    for t in range(n):
        for k in range(count):
            ref[t, pl.ds(start + 8 * k, 8), :] = jnp.zeros((8, 128), F32)


def down(r, k, g, s, c, start, count, n):
    half_sweep(k, g.at[0], g.at[1], c, 1, start, count, n)
    half_sweep(r, k, g.at[0], c, 0, start, count, n)
    half_sweep(k, r, g.at[1], c, 1, start, count, n)
    residual_pass(s, r, k, g.at[0], c, 0, start, count, n)


def post(r, k, g, c, start, count, n):
    for _ in range(2):
        half_sweep(r, k, g.at[0], c, 0, start, count, n)
        half_sweep(k, r, g.at[1], c, 1, start, count, n)


def spread(tiles, reach):
    _, lane = grid_ids()
    n = len(tiles)
    out = {0: tiles}
    for d in [k for k in range(-reach, reach + 1) if k]:
        turned = [[pltpu.roll(x, -d % 128, 1) for x in blocks] for blocks in tiles]
        if n > 1:
            own = lane < 128 - d if d > 0 else lane >= -d
            step = 1 if d > 0 else -1
            turned = [
                [jnp.where(own, x, y) for x, y in zip(turned[t], turned[(t + step) % n])] for t in range(n)
            ]
        out[d] = turned
    return out


def weights(c_ref, start, count):
    return [
        [tuple(c_ref[5 * colour + k, pl.ds(start + 8 * b, 8), :] for k in range(3)) for b in range(count)]
        for colour in range(2)
    ]


def relaxed_spread(src, g, w, colour, reach):
    sub, lane = grid_ids()
    even = lane % 2 == 0
    out = {}
    for d in range(-reach, reach + 1):
        kind = (colour + d) % 2
        out[d] = []
        for t, x in enumerate(src[d]):
            one = [pltpu.roll(y, 1, 0) for y in x]
            back = [pltpu.roll(y, 7, 0) for y in x]
            n = len(x)
            new = []
            for b in range(n):
                before = jnp.where(sub == 0, one[b - 1] if b else 0.0, one[b])
                after = jnp.where(sub == 7, back[b + 1] if b < n - 1 else 0.0, back[b])
                near, far, ang = w[kind][b]
                other = jnp.where(even, before, after) if kind == 0 else jnp.where(even, after, before)
                new.append((g[d][t][b] + near * x[b]) + (far * other + ang * (src[d - 1][t][b] + src[d + 1][t][b])))
            out[d].append(new)
    return out


def read(ref, start, count, n=1):
    return [[ref[t, pl.ds(start + 8 * b, 8), :] for b in range(count)] for t in range(n)]


def put(ref, start, tiles):
    for t, blocks in enumerate(tiles):
        for b, x in enumerate(blocks):
            ref[t, pl.ds(start + 8 * b, 8), :] = x


def spread_down(k, g, s, c_ref, start, count, n):
    w = weights(c_ref, start, count)
    gr, gk = spread(read(g.at[0], start, count, n), 4), spread(read(g.at[1], start, count, n), 3)
    black = relaxed_spread(gr, gk, w, 1, 3)
    red = relaxed_spread(black, gr, w, 0, 2)
    black = relaxed_spread(red, gk, w, 1, 1)
    put(k, start, black[0])
    new = relaxed_spread(black, gr, w, 0, 0)[0]
    for t in range(n):
        for b in range(count):
            at = pl.ds(start + 8 * b, 8)
            s[t, at, :] = c_ref[4, at, :] * (new[t][b] - red[0][t][b])


def spread_post(r, k, g, c_ref, start, count, n):
    w = weights(c_ref, start, count)
    gr, gk = spread(read(g.at[0], start, count, n), 3), spread(read(g.at[1], start, count, n), 2)
    red = relaxed_spread(spread(read(k, start, count, n), 4), gr, w, 0, 3)
    black = relaxed_spread(red, gk, w, 1, 2)
    red = relaxed_spread(black, gr, w, 0, 1)
    put(r, start, red[0])
    put(k, start, relaxed_spread(red, gk, w, 1, 0)[0])


def kernel(
    right_hbm, guess_hbm, x0, c0,
    raw, r0, s0, g1, r1, k1, s1, g2, r2, k2, s2, x3, r3, s3,
    g4, r4, k4, s4, g5, r5, k5, s5, g6, r6, k6, s6, g7, r7, k7,
    win, e_ref, f_ref, fa_ref, fb_ref, mix, nat, c1, c2, c3, c4, c5, c6, c7,
    pk0, pc0, rp0, rd0, pk1, rl1, rd1, bs3, own4, slots, strip,
    load_sem, send0, recv0, send1, recv1, sendc, recvc, senda, recva, sendg, recvg,
):
    me_a, me_r = lax.axis_index("ang"), lax.axis_index("rad")

    def device(dr, da):
        return {"ang": lax.rem(me_a + da + NA, NA), "rad": lax.rem(me_r + dr + NB, NB)}

    barrier = pltpu.get_barrier_semaphore()
    partners = list(DIRS) + [(0, d) for d in range(2, NA - 1)] + [(d, 0) for d in range(2, NB - 1)]
    for dr, da in partners:
        pl.semaphore_signal(barrier, inc=1, device_id=device(dr, da), device_id_type=MESH)

    loads = []
    for t in range(8):
        for k, src in ((0, guess_hbm), (1, right_hbm)):
            loads.append(pltpu.make_async_copy(
                src.at[:, pl.ds(128 * t, 128)], raw.at[k, t], load_sem))
    for copy in loads:
        copy.start()

    zero = jnp.zeros((8, 128), F32)
    k0, g0 = x0.at[0], x0.at[pl.ds(1, 2)]
    k3, g3 = x3.at[0], x3.at[pl.ds(1, 2)]
    edges = [(r, 0) for r in (r0, s0)] + [(r, 1) for r in (r1, k1, s1)]
    edges += [(r, 2) for r in (g2.at[0], g2.at[1], r2, k2, s2)]
    edges += [(r, 3) for r in (k3, x3.at[1], x3.at[2], r3, s3)]
    for ref, l in edges:
        depth = 1 if l < 2 else 2
        for t in range(OWN[l][1] + 1):
            for d in range(depth):
                ref[t, pl.ds(8 * d, 8), :] = zero
                ref[t, pl.ds(ROWS[l] - 8 - 8 * d, 8), :] = zero
    for l, refs in enumerate(((g4, r4, k4, s4), (g5, r5, k5, s5), (g6, r6, k6, s6), (g7, r7, k7))):
        for ref in refs:
            for x in ((ref.at[0], ref.at[1]) if len(ref.shape) == 4 else (ref,)):
                for t in range(WHOLE[l][1]):
                    x[t, pl.ds(0, 8), :] = zero
                    x[t, pl.ds(WB + WHOLE[l][0], 8), :] = zero
    zero_rows(win, 1, 0, 6)
    for t in range(9):
        for d in (0, 1, 10, 11):
            f_ref[t, pl.ds(8 * d, 8), :] = zero
    for l, c_ref in enumerate((c0, c1, c2, c3)):
        fill_coefficients(c_ref, ROWS[l] // 8, BASE[l], me_r * (2 * OWN[l][0]), NR >> l, NT >> l)
    for l, c_ref in enumerate((c4, c5, c6, c7)):
        fill_coefficients(c_ref, WHOLE[l][0] // 8 + 2, WB, 0, 2 * WHOLE[l][0], NT >> (l + 4))

    sub, lane = grid_ids()
    even = lane % 2 == 0

    def send(src, dst, send_sem, recv_sem, dr, da):
        pltpu.make_async_remote_copy(
            src_ref=src, dst_ref=dst, send_sem=send_sem, recv_sem=recv_sem,
            device_id=device(dr, da), device_id_type=MESH).start()

    def edge(l, dr, width):
        if dr < 0:
            return pl.ds(BASE[l], width), pl.ds(BASE[l] + OWN[l][0], width)
        return pl.ds(BASE[l] + OWN[l][0] - width, width), pl.ds(BASE[l] - width, width)

    wait_bytes(raw, load_sem)
    for k in range(8):
        at = pl.ds(BASE[0] + 8 * k, 8)
        red, black = c0[3, at, :], c0[8, at, :]
        for t in range(8):
            k0[t, at, :] = jnp.where(
                even, raw[0, t, pl.ds(16 * k + 1, 8, stride=2), :], raw[0, t, pl.ds(16 * k, 8, stride=2), :])
            x = raw[1, t, pl.ds(16 * k, 8, stride=2), :]
            y = raw[1, t, pl.ds(16 * k + 1, 8, stride=2), :]
            g0[0, t, at, :] = jnp.where(even, x, y) * red
            g0[1, t, at, :] = jnp.where(even, y, x) * black
    for q in range(3):
        for side, (tile, first) in enumerate(((0, 0), (7, 112))):
            total = None
            for b in range(8):
                x = x0[q, tile, pl.ds(BASE[0] + 8 * b, 8), :]
                shift = (16 * b - first) % 128
                x = pltpu.roll(x, shift, 1) if shift else x
                total = x if total is None else jnp.where(lane // 16 == b, x, total)
            pk0[side, q, :, :] = total
    for c, (dr, da) in enumerate(CORNERS):
        rows = pl.ds(BASE[0] if dr < 0 else BASE[0] + OWN[0][0] - 8, 8)
        tile, first = (0, 0) if da < 0 else (7, 112)
        total = None
        for q in range(3):
            x = x0[q, tile, rows, :]
            shift = (16 * q - first) % 128
            x = pltpu.roll(x, shift, 1) if shift else x
            total = x if total is None else jnp.where(lane // 16 == q, x, total)
        pc0[c, :, :] = total
    pl.semaphore_wait(barrier, len(partners))

    for dr, da in ORDER:
        mine, theirs = edge(0, dr, E0) if dr else (None, None)
        if da == 0:
            send(x0.at[0, pl.ds(0, 8), mine, :], x0.at[0, pl.ds(0, 8), theirs, :], send0, recv0, dr, da)
            mine, theirs = edge(0, dr, 4)
            send(x0.at[pl.ds(1, 2), pl.ds(0, 8), mine, :], x0.at[pl.ds(1, 2), pl.ds(0, 8), theirs, :],
                 send0, recv0, dr, da)
        elif dr == 0:
            side = 0 if da < 0 else 1
            send(pk0.at[side], rp0.at[side], send0, recv0, dr, da)
        else:
            c = CORNERS.index((dr, da))
            send(pc0.at[c, pl.ds(0 if dr < 0 else 8 - E0, E0), :], rd0.at[c, pl.ds(0, E0), :], send0, recv0, dr, da)
    wait_bytes(f_ref.at[pl.ds(0, 4), pl.ds(0, 69), :], send0, recv0)

    keep_before = jnp.where(me_r == 0, 0.0, 1.0)
    keep_after = jnp.where(me_r == NB - 1, 0.0, 1.0)

    def clear_outside(refs, l, n, depth=1):
        for ref in refs:
            for t in range(n):
                for d in range(depth):
                    before, after = pl.ds(BASE[l] - 8 * (d + 1), 8), pl.ds(BASE[l] + OWN[l][0] + 8 * d, 8)
                    ref[t, before, :] = ref[t, before, :] * keep_before
                    ref[t, after, :] = ref[t, after, :] * keep_after

    for q in range(3):
        from_left, from_right = rp0[1, q], rp0[0, q]
        for b in range(8):
            shift_r, shift_l = (-16 * b) % 128, (112 - 16 * b) % 128
            x = pltpu.roll(from_right, shift_r, 1) if shift_r else from_right
            y = pltpu.roll(from_left, shift_l, 1) if shift_l else from_left
            x0[q, 8, pl.ds(BASE[0] + 8 * b, 8), :] = jnp.where(lane < 64, x, y)
        for dr in (-1, 1):
            start = BASE[0] - E0 if dr < 0 else BASE[0] + OWN[0][0]
            x = rd0[CORNERS.index((-dr, -1)), :, :]
            y = pltpu.roll(rd0[CORNERS.index((-dr, 1)), :, :], 112 - 16 * q, 1)
            x = pltpu.roll(x, 128 - 16 * q, 1) if q else x
            x0[q, 8, pl.ds(start, E0), :] = jnp.where(lane < 64, x, y)[:E0]
    clear_outside((k0, g0.at[0], g0.at[1]), 0, 9)

    for _ in range(2):
        half_sweep(r0, k0, g0.at[0], c0, 0, 4, 9, 9)
        half_sweep(k0, r0, g0.at[1], c0, 1, 4, 9, 9)
    residual_pass(s0, r0, k0, g0.at[0], c0, 0, 4, 9, 9)
    restrict_pass(s0, BASE[0], 9, mix, nat, g1, BASE[1], c1, 0, 4, ((0, 1), (2, 3), (4, 5), (6, 7)))

    for b in range(4):
        at, own = pl.ds(8 * b, 8), pl.ds(BASE[1] + 8 * b, 8)
        pk1[0, at, :] = jnp.where(lane < 64, g1[0, 0, own, :], pltpu.roll(g1[1, 0, own, :], 64, 1))
        pk1[1, at, :] = jnp.where(lane < 64, pltpu.roll(g1[0, 3, own, :], 64, 1), g1[1, 3, own, :])
    for dr, da in ORDER:
        side = 0 if da < 0 else 1
        if da == 0:
            mine, theirs = edge(1, dr, E1)
            send(g1.at[:, pl.ds(0, 4), mine, :], g1.at[:, pl.ds(0, 4), theirs, :], send1, recv1, dr, da)
        elif dr == 0:
            send(pk1.at[side], rl1.at[side], send1, recv1, dr, da)
        else:
            send(pk1.at[side, pl.ds(0 if dr < 0 else 32 - E1, E1), :],
                 rd1.at[CORNERS.index((dr, da)), pl.ds(0, E1), :], send1, recv1, dr, da)
    wait_bytes(f_ref.at[pl.ds(0, 8), pl.ds(0, 53), :], send1, recv1)

    def merge_edges(row, size, from_right, from_left):
        low = lane[:size] < 64
        g1[0, 4, pl.ds(row, size), :] = jnp.where(low, from_right, pltpu.roll(from_left, 64, 1))
        g1[1, 4, pl.ds(row, size), :] = jnp.where(low, pltpu.roll(from_right, 64, 1), from_left)

    for b in range(4):
        merge_edges(BASE[1] + 8 * b, 8, rl1[0, pl.ds(8 * b, 8), :], rl1[1, pl.ds(8 * b, 8), :])
    for dr in (-1, 1):
        start = BASE[1] - E1 if dr < 0 else BASE[1] + OWN[1][0]
        right, left = CORNERS.index((-dr, -1)), CORNERS.index((-dr, 1))
        for first in (0, 8, 16):
            size = 8 if first < 16 else 2
            merge_edges(start + first, size, rd1[right, pl.ds(first, size), :], rd1[left, pl.ds(first, size), :])
    for q in range(2):
        for dr in (-1, 1):
            rest = BASE[1] - E1 - 3 if dr < 0 else BASE[1] + OWN[1][0] + E1
            for t in range(5):
                g1[q, t, pl.ds(rest, 3), :] = jnp.zeros((3, 128), F32)
    clear_outside((g1.at[0], g1.at[1]), 1, 5, 3)

    down(r1, k1, g1, s1, c1, BASE[1] - 20, 9, 5)
    restrict_pass(s1, BASE[1], 5, mix, nat, g2, BASE[2], c2, -8, 4, ((0, 1), (2, 3), (4, 4)))
    down(r2, k2, g2, s2, c2, BASE[2] - 8, 4, 3)
    restrict_pass(s2, BASE[2], 3, mix, nat, g3, BASE[3], c3, -4, 2, ((0, 1), (2, 2)))
    spread_down(k3, g3, s3, c3, BASE[3] - 4, 2, 2)

    nat[0, pl.ds(0, 8), :] = gathered(joined(*mixed_block(s3, BASE[3], 2, lane)[:1] * 2, lane), lane)
    x, y = nat[0, pl.ds(0, 4, stride=2), :], nat[0, pl.ds(1, 4, stride=2), :]
    my_pairs = pl.ds(WB + 4 * me_r, 4)
    own4[pl.ds(0, 4), :] = jnp.where(even[:4], x, y) * c4[3, my_pairs, :]
    own4[pl.ds(4, 4), :] = jnp.where(even[:4], y, x) * c4[8, my_pairs, :]
    for d in range(1, NA):
        send(own4, slots.at[d - 1], senda, recva, 0, d)
    wait_bytes(slots, senda, recva)
    for t in range(4):
        total = own4[...]
        for d in range(1, NA):
            source = lax.rem(me_a - d + NA, NA)
            hit = jnp.logical_and(source // 2 == t, lane // 64 == source % 2)
            total = jnp.where(hit, slots[d - 1], total)
        for q in range(2):
            strip[q, t, pl.ds(0, 4), :] = total[4 * q:4 * q + 4]
            g4[q, t, my_pairs, :] = total[4 * q:4 * q + 4]
    for d in range(1, NB):
        send(strip.at[:, :, pl.ds(0, 4), :], g4.at[:, :, my_pairs, :], sendg, recvg, d, 0)
    for k, (dr, da) in enumerate(DIRS):
        send(x3.at[:, 0, pl.ds(BASE[3], 8), :], bs3.at[k], sendc, recvc, dr, da)
    wait_bytes(g4.at[:, :, pl.ds(WB, 60), :], sendg, recvg)

    down(r4, k4, g4, s4, c4, WB, 8, 4)
    restrict_pass(s4, WB, 4, mix, nat, g5, WB, c5, 0, 4, ((0, 1), (2, 3)))
    down(r5, k5, g5, s5, c5, WB, 4, 2)
    restrict_pass(s5, WB, 2, mix, nat, g6, WB, c6, 0, 2, ((0, 1),))
    spread_down(k6, g6, s6, c6, WB, 2, 1)
    restrict_pass(s6, WB, 1, mix, nat, g7, WB, c7, 0, 1, ((0, 0),))
    gr7, gk7, w7 = spread(read(g7.at[0], WB, 1), 4), spread(read(g7.at[1], WB, 1), 3), weights(c7, WB, 1)
    source = gr7
    for step in range(4):
        black = relaxed_spread(source, gk7, w7, 1, 3 if step < 3 else 2)
        red = relaxed_spread(black, gr7, w7, 0, 2 if step < 3 else 1)
        black = relaxed_spread(red, gk7, w7, 1, 1 if step < 3 else 0)
        if step < 3:
            source = spread(relaxed_spread(black, gr7, w7, 0, 0)[0], 4)
    put(r7, WB, red[0])
    put(k7, WB, black[0])

    def whole_up(rc, kc, blocks, nc, fine, plan):
        for k in range(blocks):
            unpair(rc, kc, WB + 8 * k, e_ref, FB + 16 * k, nc)
        prolong_pass(e_ref, f_ref, fa_ref, fb_ref, 0, 2 * blocks, fine, WB, 0, 2 * blocks, plan, True)

    whole_up(r7, k7, 1, 1, k6, ((0, 0),))
    spread_post(r6, k6, g6, c6, WB, 2, 1)
    whole_up(r6, k6, 2, 1, k5, ((0, 0), (0, 1)))
    post(r5, k5, g5, c5, WB, 4, 2)
    whole_up(r5, k5, 4, 2, k4, ((0, 0), (0, 1), (1, 0), (1, 1)))
    post(r4, k4, g4, c4, WB, 8, 4)

    def block(ref, da, wanted, at):
        b = lax.rem(me_a + da + NA, NA)
        x = ref[b // 2, at, :]
        return jnp.where(b % 2 == wanted, x, pltpu.roll(x, 64, 1))

    for k in range(2):
        at = pl.ds(WB - 4 + 4 * me_r + 8 * k, 8)
        seen = []
        for ref in (r4, k4):
            mine, rightward, leftward = block(ref, 0, 0, at), block(ref, 1, 1, at), block(ref, -1, 1, at)
            seen.append(jnp.where(lane < 64, mine, jnp.where(lane < 96, rightward, leftward)))
        q = FB - 8 + 16 * k
        win[0, pl.ds(q, 8, stride=2), :] = jnp.where(even, seen[0], seen[1])
        win[0, pl.ds(q + 1, 8, stride=2), :] = jnp.where(even, seen[1], seen[0])

    wait_bytes(bs3, sendc, recvc)
    for q in range(3):
        keep = {-1: jnp.where(me_r == 0, 0.0, 1.0), 0: 1.0, 1: jnp.where(me_r == NB - 1, 0.0, 1.0)}
        got = lambda dr, da: bs3[DIRS.index((-dr, -da)), q] * keep[dr]
        x3[q, 0, pl.ds(BASE[3] - 8, 8), :] = got(-1, 0)
        x3[q, 0, pl.ds(BASE[3] + 8, 8), :] = got(1, 0)
        for dr in (-1, 0, 1):
            x3[q, 1, pl.ds(BASE[3] + 8 * dr, 8), :] = jnp.where(lane < 64, got(dr, 1), got(dr, -1))
    prolong_pass(win, f_ref, fa_ref, fb_ref, -8, 3, k3, BASE[3], -8, 3, ((0, 0), (0, 1)), False, OWN[3][0])
    spread_post(r3, k3, g3, c3, BASE[3] - 8, 3, 2)

    for k in range(2):
        unpair(r3, k3, BASE[3] - 4 + 8 * k, e_ref, FB - 8 + 16 * k, 2)
    prolong_pass(e_ref, f_ref, fa_ref, fb_ref, -8, 4, k2, BASE[2], -4, 3, ((0, 0), (0, 1), (1, 2)), False, OWN[2][0])
    post(r2, k2, g2, c2, BASE[2] - 4, 3, 3)

    for k in range(3):
        unpair(r2, k2, BASE[2] - 4 + 8 * k, e_ref, FB - 8 + 16 * k, 3)
    prolong_pass(e_ref, f_ref, fa_ref, fb_ref, -8, 6, k1, BASE[1], -4, 5, ((0, 0), (0, 1), (1, 0), (1, 1), (2, 2)), False, OWN[1][0])
    post(r1, k1, g1, c1, BASE[1] - 4, 5, 5)

    for k in range(5):
        unpair(r1, k1, BASE[1] - 4 + 8 * k, e_ref, FB - 8 + 16 * k, 5)
    plan = tuple((t // 2, t % 2) for t in range(8)) + ((4, 2),)
    prolong_pass(e_ref, f_ref, fa_ref, fb_ref, -8, 10, k0, BASE[0], -4, 9, plan, False, OWN[0][0])


def finish(x0, c0, sol_hbm, res_hbm, r, k, s, b, raw, out_sem):
    zero = jnp.zeros((8, 128), F32)
    for ref in (r, k):
        for t in range(9):
            ref[t, pl.ds(0, 8), :] = zero
            ref[t, pl.ds(ROWS[0] - 8, 8), :] = zero
    start, gr, gk = x0.at[0], x0.at[1], x0.at[2]
    half_sweep(r, start, gr, c0, 0, 4, 9, 9)
    half_sweep(k, r, gk, c0, 1, 4, 9, 9)
    half_sweep(r, k, gr, c0, 0, 4, 9, 9)
    half_sweep(k, r, gk, c0, 1, 4, 9, 9)

    def write(slot, red, black, hbm):
        for t in range(8):
            for q in range(8):
                unpair(red.at[pl.ds(t, 1)], black.at[pl.ds(t, 1)], BASE[0] + 8 * q, raw.at[slot, pl.ds(t, 1)], 16 * q, 1)
            copy = pltpu.make_async_copy(raw.at[slot, t], hbm.at[:, pl.ds(128 * t, 128)], out_sem)
            copy.start()

    write(0, r, k, sol_hbm)
    residual_pass(s, r, k, gr, c0, 0, BASE[0], 8, 9, tiles=range(8))
    residual_pass(b, k, r, gk, c0, 1, BASE[0], 8, 9, tiles=range(8))
    write(1, s, b, res_hbm)
    wait_bytes(raw, out_sem)


def local(right_side, guess):
    def vm(*shape):
        return pltpu.VMEM(shape, F32)

    levels = [vm(2, 8, 128, 128), vm(9, ROWS[0], 128), vm(9, ROWS[0], 128)]
    for l in (1, 2):
        n = OWN[l][1] + 1
        levels += [vm(2, n, ROWS[l], 128)] + [vm(n, ROWS[l], 128)] * 3
    levels += [vm(3, 2, ROWS[3], 128), vm(2, ROWS[3], 128), vm(2, ROWS[3], 128)]
    for l, (pairs, tiles) in enumerate(WHOLE):
        levels += [vm(2, tiles, pairs + 2 * WB, 128)] + [vm(tiles, pairs + 2 * WB, 128)] * (2 if l == 3 else 3)
    coefficients = [vm(10, r, 128) for r in ROWS[1:]] + [vm(10, pairs + 2 * WB, 128) for pairs, _ in WHOLE]
    buffers = [
        vm(2, 3, 8, 128), vm(4, 8, 128), vm(2, 3, 8, 128), vm(4, 8, 128),
        vm(2, 32, 128), vm(2, 32, 128), vm(4, 24, 128),
        vm(8, 3, 8, 128), vm(8, 128), vm(NA - 1, 8, 128), vm(2, 4, 8, 128),
    ]
    dma = pltpu.SemaphoreType.DMA
    sems = [dma] * 11
    natural = [vm(1, 48, 128), vm(5, 96, 128), vm(9, 96, 128), vm(5, 96, 128), vm(5, 96, 128), vm(9, 64, 128), vm(4, 64, 128)]
    held = (vm(3, 9, ROWS[0], 128), vm(10, ROWS[0], 128))
    inside = pl.BlockSpec(memory_space=pltpu.VMEM)
    outside = pl.BlockSpec(memory_space=pl.ANY)
    x0, c0 = pl.pallas_call(
        kernel,
        out_shape=held,
        in_specs=[outside] * 2,
        out_specs=(inside,) * 2,
        scratch_shapes=levels + natural + coefficients + buffers + sems,
        compiler_params=pltpu.CompilerParams(collective_id=0, has_side_effects=True),
    )(right_side, guess)
    x0, c0 = (pltpu.with_memory_space_constraint(x, pltpu.VMEM) for x in (x0, c0))
    block = jax.ShapeDtypeStruct(right_side.shape, F32)
    return pl.pallas_call(
        finish,
        out_shape=(block, block),
        in_specs=[inside] * 2,
        out_specs=(outside,) * 2,
        scratch_shapes=[vm(9, ROWS[0], 128)] * 4 + [vm(2, 8, 128, 128), dma],
    )(x0, c0)


def solution(mesh):
    placed = (P("rad", "ang"), P("rad", "ang"))
    return jax.shard_map(local, mesh=mesh, in_specs=placed, out_specs=placed, check_vma=False)
```
